32 devices in a mesh: part: 1 (over z), tpa: 4 (over y), tpb: 8 (over x, core).
Axes of the slice: x: 4, y: 4, z: 1, core: 2. Of those that a mesh axis runs over, the one named last changes fastest.
The devices are a block of a 4x4x8 slice.
Arguments:
- x: bfloat16 [64, 1024, 2048], P(('part', 'tpb'))
- lengths: int32 [64], P(('part', 'tpb'))
- k_buf: bfloat16 [64, 1024, 4, 64], P(('part', 'tpb'), None, 'tpa')
- v_buf: bfloat16 [64, 1024, 4, 64], P(('part', 'tpb'), None, 'tpa')
- w_qkv: bfloat16 [2048, 2560], P('part', ('tpa', 'tpb'))
- w_o: bfloat16 [2048, 2048], P(('part', 'tpa', 'tpb'))
- w_gate_up: bfloat16 [2048, 11264], P('part', ('tpa', 'tpb'))
- w_down: bfloat16 [5632, 2048], P(('part', 'tpa', 'tpb'))
- g_attn: bfloat16 [2048], P('part')
- g_mlp: bfloat16 [2048], P('part')
Outputs:
- output 1: bfloat16 [64, 1024, 2048], P(('part', 'tpb'))
- output 2: bfloat16 [64, 1024, 4, 64], P(('part', 'tpb'), None, 'tpa')
- output 3: bfloat16 [64, 1024, 4, 64], P(('part', 'tpb'), None, 'tpa')
- output 4: bfloat16 [2048, 2048], P('part', 'tpa')
- output 5: bfloat16 [2048, 256], P('part', 'tpa')
- output 6: bfloat16 [2048, 256], P('part', 'tpa')
- output 7: bfloat16 [2048, 2048], P(('part', 'tpa'))
- output 8: bfloat16 [2048, 5632], P('part', 'tpa')
- output 9: bfloat16 [2048, 5632], P('part', 'tpa')
- output 10: bfloat16 [5632, 2048], P(('part', 'tpa'))
All inputs are finite; a program needn't handle non-finite values.
Results may differ from the reference program's by a relative error of at most 0.0142439.
Values are sent between devices in bfloat16 or wider.
A program may use at most 768 MiB of HBM per device.

```python
import math
import jax
import jax.numpy as jnp
from jax import lax

D = 2048
HEADS = 32
KV_HEADS = 4
HEAD = 64
FF = 5632
BATCH = 64
SEQ = 1024
TRAIN_TP = 32
GROUP = HEADS // KV_HEADS
QKV_COLS = KV_HEADS * (GROUP + 2) * HEAD
FF_BLOCK = FF // TRAIN_TP
ROPE_BASE = 500000.0
ROPE_FACTOR = 8.0
LOW_FREQ = 1.0
HIGH_FREQ = 4.0
ORIG_CONTEXT = 8192.0
NORM_EPS = 1e-5
MASK_VALUE = -1e30


def setup_inputs(seed: int = 0, part: int = 0) -> dict:
    part_key = jax.random.fold_in(jax.random.key(seed), part)
    sub_keys = jax.random.split(part_key, 10)
    x_in = jax.random.normal(sub_keys[0], (BATCH, SEQ, D), jnp.float32)
    drawn_len = jax.random.randint(sub_keys[1], (BATCH,), 1, SEQ + 1)
    lengths = jnp.where(jnp.arange(BATCH) == 0, SEQ, drawn_len).astype(jnp.int32)
    k_buf = jax.random.normal(sub_keys[2], (BATCH, SEQ, KV_HEADS, HEAD), jnp.float32)
    v_buf = jax.random.normal(sub_keys[3], (BATCH, SEQ, KV_HEADS, HEAD), jnp.float32)
    qk_scale = jnp.where(jnp.arange(GROUP + 2) <= GROUP, 1.5, 1.0)[:, None]
    w_qkv = (jax.random.normal(sub_keys[4], (D, KV_HEADS, GROUP + 2, HEAD), jnp.float32) * qk_scale * D ** -0.5).reshape(D, QKV_COLS)
    w_o = jax.random.normal(sub_keys[5], (HEADS * HEAD, D), jnp.float32) * (HEADS * HEAD) ** -0.5
    w_gate_up = jax.random.normal(sub_keys[6], (D, 2 * FF), jnp.float32) * D ** -0.5
    w_down = jax.random.normal(sub_keys[7], (FF, D), jnp.float32) * FF ** -0.5
    g_attn = 1.0 + 0.4 * jax.random.normal(sub_keys[8], (D,), jnp.float32)
    g_mlp = 1.0 + 0.4 * jax.random.normal(sub_keys[9], (D,), jnp.float32)
    return {'x': x_in.astype(jnp.bfloat16), 'lengths': lengths, 'k_buf': k_buf.astype(jnp.bfloat16), 'v_buf': v_buf.astype(jnp.bfloat16), 'w_qkv': w_qkv.astype(jnp.bfloat16), 'w_o': w_o.astype(jnp.bfloat16), 'w_gate_up': w_gate_up.astype(jnp.bfloat16), 'w_down': w_down.astype(jnp.bfloat16), 'g_attn': g_attn.astype(jnp.bfloat16), 'g_mlp': g_mlp.astype(jnp.bfloat16)}


def rms_norm(x_in, gain_vec):
    x_wide = x_in.astype(jnp.float32)
    mean_sq = jnp.mean(x_wide * x_wide, axis=-1, keepdims=True)
    return (x_wide * lax.rsqrt(mean_sq + NORM_EPS) * gain_vec.astype(jnp.float32)).astype(jnp.bfloat16)


def rope_tables():
    exponent = jnp.arange(HEAD // 2, dtype=jnp.float32) * (2.0 / HEAD)
    inv_freq = 1.0 / jnp.power(ROPE_BASE, exponent)
    wavelen = 2.0 * math.pi / inv_freq
    smooth = (ORIG_CONTEXT / wavelen - LOW_FREQ) / (HIGH_FREQ - LOW_FREQ)
    blended = (1.0 - smooth) * inv_freq / ROPE_FACTOR + smooth * inv_freq
    rope_freq = jnp.where(wavelen < ORIG_CONTEXT / HIGH_FREQ, inv_freq, jnp.where(wavelen > ORIG_CONTEXT / LOW_FREQ, inv_freq / ROPE_FACTOR, blended))
    angles = jnp.arange(SEQ, dtype=jnp.float32)[:, None] * rope_freq[None, :]
    return jnp.cos(angles), jnp.sin(angles)


def apply_rope(vec_in, cos_tab, sin_tab):
    half_dim = vec_in.shape[-1] // 2
    first_half = vec_in[..., :half_dim]
    second_half = vec_in[..., half_dim:]
    return jnp.concatenate([first_half * cos_tab - second_half * sin_tab, second_half * cos_tab + first_half * sin_tab], axis=-1)


def reference(x, lengths, k_buf, v_buf, w_qkv, w_o, w_gate_up, w_down, g_attn, g_mlp):
    packed = w_qkv.reshape(D, KV_HEADS, GROUP + 2, HEAD)
    w_q = packed[:, :, :GROUP, :].reshape(D, HEADS * HEAD)
    w_k = packed[:, :, GROUP, :].reshape(D, KV_HEADS * HEAD)
    w_v = packed[:, :, GROUP + 1, :].reshape(D, KV_HEADS * HEAD)
    gu_view = w_gate_up.reshape(D, TRAIN_TP, 2, FF_BLOCK)
    w_gate = gu_view[:, :, 0, :].reshape(D, FF)
    w_up = gu_view[:, :, 1, :].reshape(D, FF)
    cos_tab, sin_tab = rope_tables()
    positions = jnp.arange(SEQ)
    causal = positions[None, :] <= positions[:, None]

    def one_prompt(prompt_item):
        tokens, length = prompt_item
        x_normed = rms_norm(tokens, g_attn)
        queries = jnp.dot(x_normed, w_q, preferred_element_type=jnp.float32).astype(jnp.bfloat16).reshape(SEQ, KV_HEADS, GROUP, HEAD)
        keys_new = jnp.dot(x_normed, w_k, preferred_element_type=jnp.float32).astype(jnp.bfloat16).reshape(SEQ, KV_HEADS, HEAD)
        values = jnp.dot(x_normed, w_v, preferred_element_type=jnp.float32).astype(jnp.bfloat16).reshape(SEQ, KV_HEADS, HEAD)
        q_rot = apply_rope(queries.astype(jnp.float32), cos_tab[:, None, None, :], sin_tab[:, None, None, :]).astype(jnp.bfloat16)
        k_rot = apply_rope(keys_new.astype(jnp.float32), cos_tab[:, None, :], sin_tab[:, None, :]).astype(jnp.bfloat16)
        allowed = causal & (positions[None, :] < length)

        def one_group(kv_item):
            q_head, k_head, v_head = kv_item
            scores = jnp.einsum('qgd,sd->gqs', q_head.astype(jnp.float32), k_head.astype(jnp.float32)) * HEAD ** -0.5
            scores = jnp.where(allowed[None], scores, MASK_VALUE)
            attn_prob = jax.nn.softmax(scores, axis=-1).astype(jnp.bfloat16)
            return jnp.einsum('gqs,sd->qgd', attn_prob.astype(jnp.float32), v_head.astype(jnp.float32)).astype(jnp.bfloat16)

        per_group = lax.map(one_group, (q_rot.transpose(1, 0, 2, 3), k_rot.transpose(1, 0, 2), values.transpose(1, 0, 2)))
        attn_out = per_group.transpose(1, 0, 2, 3).reshape(SEQ, HEADS * HEAD)
        attn_proj = jnp.dot(attn_out, w_o, preferred_element_type=jnp.float32)
        hidden = (tokens.astype(jnp.float32) + attn_proj).astype(jnp.bfloat16)
        h_normed = rms_norm(hidden, g_mlp)
        gate_act = jnp.dot(h_normed, w_gate, preferred_element_type=jnp.float32).astype(jnp.bfloat16)
        up_act = jnp.dot(h_normed, w_up, preferred_element_type=jnp.float32).astype(jnp.bfloat16)
        mid_act = (jax.nn.silu(gate_act.astype(jnp.float32)) * up_act.astype(jnp.float32)).astype(jnp.bfloat16)
        layer_out = (hidden.astype(jnp.float32) + jnp.dot(mid_act, w_down, preferred_element_type=jnp.float32)).astype(jnp.bfloat16)
        return layer_out, k_rot, values

    layer_out, k_new, v_new = lax.map(one_prompt, (x, lengths))
    valid_pos = (positions[None, :] < lengths[:, None])[:, :, None, None]
    k_cache = jnp.where(valid_pos, k_new, k_buf)
    v_cache = jnp.where(valid_pos, v_new, v_buf)
    return (layer_out, k_cache, v_cache, w_q, w_k, w_v, w_o, w_gate, w_up, w_down)
```

```python
import functools
import math
import jax
import jax.numpy as jnp
from jax import lax
from jax.experimental import pallas as pl
from jax.experimental.pallas import tpu as pltpu
from jax.sharding import PartitionSpec as P

ROPE_BASE = 500000.0
ROPE_FACTOR = 8.0
LOW_FREQ = 1.0
HIGH_FREQ = 4.0
ORIG_CONTEXT = 8192.0
NORM_EPS = 1e-5
MASK_VALUE = -1e30
Q_TILE = 256
CHUNKS_PER_PROMPT = 2


def rms_norm(x_in, gain_vec):
    x_wide = x_in.astype(jnp.float32)
    mean_sq = jnp.mean(x_wide * x_wide, axis=-1, keepdims=True)
    return (x_wide * lax.rsqrt(mean_sq + NORM_EPS) * gain_vec.astype(jnp.float32)).astype(jnp.bfloat16)


def rope_tables(seq_len, head_dim):
    exponent = jnp.arange(head_dim // 2, dtype=jnp.float32) * (2.0 / head_dim)
    inv_freq = 1.0 / jnp.power(ROPE_BASE, exponent)
    wavelen = 2.0 * math.pi / inv_freq
    smooth = (ORIG_CONTEXT / wavelen - LOW_FREQ) / (HIGH_FREQ - LOW_FREQ)
    blended = (1.0 - smooth) * inv_freq / ROPE_FACTOR + smooth * inv_freq
    rope_freq = jnp.where(wavelen < ORIG_CONTEXT / HIGH_FREQ, inv_freq, jnp.where(wavelen > ORIG_CONTEXT / LOW_FREQ, inv_freq / ROPE_FACTOR, blended))
    angles = jnp.arange(seq_len, dtype=jnp.float32)[:, None] * rope_freq[None, :]
    return jnp.cos(angles), jnp.sin(angles)


def attention_kernel(head_dim, group_size, len_ref, qkv_ref, cos_ref, sin_ref, out_ref, k_scr, vl_scr, vr_scr):
    seq_len = qkv_ref.shape[1]
    pair = 2 * head_dim
    length = len_ref[pl.program_id(0)]
    lane = lax.broadcasted_iota(jnp.int32, (1, pair), 1)
    low_lane = lane < head_dim
    first_half = lax.rem(lane, head_dim) < head_dim // 2

    def rope(vec, rows):
        ahead = pltpu.roll(vec, pair - head_dim // 2, 1)
        behind = pltpu.roll(vec, head_dim // 2, 1)
        return vec * cos_ref[rows, :] + jnp.where(first_half, ahead, behind) * sin_ref[rows, :]

    q_cols = group_size * head_dim
    for start in range(0, seq_len, Q_TILE):
        rows = pl.ds(start, Q_TILE)
        kv = qkv_ref[0, rows, q_cols:q_cols + pair].astype(jnp.float32)
        k_rot = rope(kv, rows)
        k_scr[rows, :] = jnp.where(low_lane, k_rot, pltpu.roll(k_rot, head_dim, 1)).astype(jnp.bfloat16)
        vl_scr[rows, :] = jnp.where(low_lane, pltpu.roll(kv, head_dim, 1), 0.0).astype(jnp.bfloat16)
        vr_scr[rows, :] = jnp.where(low_lane, 0.0, kv).astype(jnp.bfloat16)

    for start in range(0, seq_len, Q_TILE):
        rows = pl.ds(start, Q_TILE)
        keys = start + Q_TILE
        row_id = start + lax.broadcasted_iota(jnp.int32, (Q_TILE, Q_TILE), 0)

        def weights(query):
            scores = lax.dot_general(query, k_scr[:keys, :], (((1,), (1,)), ((), ())), preferred_element_type=jnp.float32)
            parts = []
            for block in range(0, keys, Q_TILE):
                col_id = block + lax.broadcasted_iota(jnp.int32, (Q_TILE, Q_TILE), 1)
                allowed = col_id < length
                if block == start:
                    allowed = allowed & (col_id <= row_id)
                parts.append(jnp.where(allowed, scores[:, block:block + Q_TILE], MASK_VALUE))
            top = parts[0]
            for part in parts[1:]:
                top = jnp.maximum(top, part)
            top = jnp.max(top, axis=1, keepdims=True)
            parts = [jnp.exp(part - top) for part in parts]
            total = parts[0]
            for part in parts[1:]:
                total = total + part
            scale = 1.0 / jnp.sum(total, axis=1, keepdims=True)
            return jnp.concatenate([(part * scale).astype(jnp.bfloat16) for part in parts], axis=1)

        def head_pair(index, carry):
            cols = pl.ds(pl.multiple_of(index * pair, pair), pair)
            query = rope(qkv_ref[0, rows, cols].astype(jnp.float32), rows).astype(jnp.bfloat16).astype(jnp.float32) * head_dim ** -0.5
            left = weights(jnp.where(low_lane, query, 0.0).astype(jnp.bfloat16))
            right = weights(jnp.where(low_lane, 0.0, query).astype(jnp.bfloat16))
            acc = jnp.dot(left, vl_scr[:keys, :], preferred_element_type=jnp.float32)
            acc = acc + jnp.dot(right, vr_scr[:keys, :], preferred_element_type=jnp.float32)
            out_ref[0, rows, cols] = acc.astype(jnp.bfloat16)
            return carry

        lax.fori_loop(0, group_size // 2, head_pair, 0)


def attention(qkv_act, lengths, cos_tab, sin_tab, kv_heads, head_dim):
    batch, seq_len, qkv_cols = qkv_act.shape
    group_cols = qkv_cols // kv_heads
    group_size = group_cols // head_dim - 2
    out_cols = group_size * head_dim
    pair = 2 * head_dim
    cos_pair = jnp.tile(cos_tab, (1, 4))
    sin_pair = jnp.tile(jnp.concatenate([-sin_tab, sin_tab], axis=1), (1, 2))
    flops = 2 * 2 * batch * kv_heads * group_size * seq_len * seq_len * head_dim
    return pl.pallas_call(
        functools.partial(attention_kernel, head_dim, group_size),
        out_shape=jax.ShapeDtypeStruct((batch, seq_len, kv_heads * out_cols), jnp.bfloat16),
        grid_spec=pltpu.PrefetchScalarGridSpec(
            num_scalar_prefetch=1,
            grid=(batch, kv_heads),
            in_specs=[
                pl.BlockSpec((1, seq_len, group_cols), lambda b, g, _: (b, 0, g)),
                pl.BlockSpec((seq_len, pair), lambda b, g, _: (0, 0)),
                pl.BlockSpec((seq_len, pair), lambda b, g, _: (0, 0)),
            ],
            out_specs=pl.BlockSpec((1, seq_len, out_cols), lambda b, g, _: (b, 0, g)),
            scratch_shapes=[pltpu.VMEM((seq_len, pair), jnp.bfloat16)] * 3,
        ),
        compiler_params=pltpu.CompilerParams(dimension_semantics=('arbitrary', 'arbitrary'), vmem_limit_bytes=48 * 1024 * 1024),
        cost_estimate=pl.CostEstimate(flops=4 * flops, bytes_accessed=2 * batch * seq_len * (qkv_cols + kv_heads * out_cols), transcendentals=batch * kv_heads * group_size * seq_len * seq_len),
        name='prefill_attention',
    )(lengths, qkv_act, cos_pair, sin_pair)


def empty(shape, dtype):
    return pl.pallas_call(lambda out_ref: None, out_shape=jax.ShapeDtypeStruct(shape, dtype), out_specs=pl.BlockSpec(memory_space=pl.ANY), name='output_buffer')()


def matmul_t(lhs, rhs_t):
    return lax.dot_general(lhs, rhs_t, (((lhs.ndim - 1,), (1,)), ((), ())), preferred_element_type=jnp.float32)


def solution(mesh):
    n_tpa = mesh.shape['tpa']
    n_tpb = mesh.shape['tpb']
    up_ring = [(i, (i + 1) % n_tpa) for i in range(n_tpa)]
    down_ring = [(i, (i - 1) % n_tpa) for i in range(n_tpa)]
    both = ('tpa', 'tpb')

    def layer_step(x_loc, len_loc, k_buf, v_buf, w_qkv, w_o, w_gate_up, w_down, g_attn, g_mlp):
        row = lax.axis_index('tpa')
        batch_loc, seq_len, model_dim = x_loc.shape
        head_dim = k_buf.shape[3]
        own_batch = batch_loc // n_tpa
        ff_block = w_gate_up.shape[1] // 2
        qkv_row = w_qkv.shape[1] * n_tpb
        o_row = w_o.shape[0] * n_tpb
        ff_row = ff_block * n_tpb

        qkv_block = w_qkv.shape[1]
        qkvo = lax.all_gather(jnp.concatenate([w_qkv.T, w_o], axis=0), both, axis=0, tiled=False)
        qkv_t = qkvo[:, :qkv_block].reshape(-1, model_dim)
        o_full = qkvo[:, qkv_block:].reshape(-1, model_dim)
        gu_t = lax.all_gather(w_gate_up.T.reshape(2, ff_block, model_dim), both, axis=1, tiled=True)
        down_full = lax.all_gather(w_down, both, axis=0, tiled=True)

        cos_tab, sin_tab = rope_tables(seq_len, head_dim)
        x_own = lax.dynamic_index_in_dim(x_loc.reshape(own_batch, n_tpa, seq_len, model_dim), row, 1, keepdims=False)
        len_own = lax.dynamic_index_in_dim(len_loc.reshape(own_batch, n_tpa), row, 1, keepdims=False)

        qkv_act = matmul_t(rms_norm(x_own, g_attn), qkv_t).astype(jnp.bfloat16)
        attn_out = attention(qkv_act, len_own, cos_tab, sin_tab, n_tpa * k_buf.shape[2], head_dim)
        attn_proj = jnp.dot(attn_out, o_full, preferred_element_type=jnp.float32)
        hidden = (x_own.astype(jnp.float32) + attn_proj).astype(jnp.bfloat16)

        chunk = seq_len // CHUNKS_PER_PROMPT
        fars = []
        spots = [(slot, start) for slot in range(own_batch) for start in range(0, seq_len, chunk)]
        y_all = empty((own_batch, n_tpa, seq_len, model_dim), jnp.bfloat16)

        def put(y_buf, piece, slot, owner, start):
            return lax.dynamic_update_slice(y_buf, piece[None, None], (slot, lax.rem(owner + n_tpa, n_tpa), start, 0))

        mids = []
        ahead = 2
        for index, (slot, start) in enumerate(spots):
            h_normed = rms_norm(hidden[slot, start:start + chunk], g_mlp)
            gate_act = matmul_t(h_normed, gu_t[0]).astype(jnp.bfloat16)
            up_act = matmul_t(h_normed, gu_t[1]).astype(jnp.bfloat16)
            mids.append((jax.nn.silu(gate_act.astype(jnp.float32)) * up_act.astype(jnp.float32)).astype(jnp.bfloat16))
            if index == ahead - 1:
                down_use, *mids = lax.optimization_barrier((down_full, *mids))
        y_parts = []
        for mid_act, (slot, start) in zip(mids, spots):
            mlp_out = jnp.dot(mid_act, down_use, preferred_element_type=jnp.float32)
            y_parts.append((hidden[slot, start:start + chunk].astype(jnp.float32) + mlp_out).astype(jnp.bfloat16))
        near = []
        for part in y_parts:
            near.append((lax.ppermute(part, 'tpa', up_ring), lax.ppermute(part, 'tpa', down_ring)))
        for part, (slot, start) in zip(y_parts, spots):
            y_all = put(y_all, part, slot, row, start)

        qkv_own = lax.dynamic_slice_in_dim(qkv_t, row * qkv_row, qkv_row, 0)
        kv_cols = k_buf.shape[2] * head_dim
        q_cols = qkv_row - 2 * kv_cols
        w_query = qkv_own[:q_cols].T
        w_key = qkv_own[q_cols:q_cols + kv_cols].T
        w_value = qkv_own[q_cols + kv_cols:].T
        gu_own = lax.dynamic_slice_in_dim(gu_t, row * ff_row, ff_row, 1)
        w_gate = gu_own[0].T
        w_up = gu_own[1].T
        o_rows = lax.dynamic_slice_in_dim(o_full, row * o_row, o_row, 0)
        down_rows = lax.dynamic_slice_in_dim(down_full, row * ff_row, ff_row, 0)

        kv_new = matmul_t(rms_norm(x_loc, g_attn), qkv_own[q_cols:]).astype(jnp.bfloat16)
        half_dim = head_dim // 2
        k_first = kv_new[..., :half_dim].astype(jnp.float32)
        k_second = kv_new[..., half_dim:head_dim].astype(jnp.float32)
        k_rot = jnp.concatenate([k_first * cos_tab - k_second * sin_tab, k_second * cos_tab + k_first * sin_tab], axis=-1).astype(jnp.bfloat16)
        valid_pos = (jnp.arange(seq_len)[None, :] < len_loc[:, None])[:, :, None, None]
        k_cache = jnp.where(valid_pos, k_rot[:, :, None, :], k_buf)
        v_cache = jnp.where(valid_pos, kv_new[:, :, None, head_dim:], v_buf)
        fillers = (w_query, w_gate, w_up, down_rows, k_cache, v_cache)
        near[0], fillers, y_all = lax.optimization_barrier((near[0], fillers, y_all))
        w_query, w_gate, w_up, down_rows, k_cache, v_cache = fillers
        for index, ((from_below, from_above), (slot, start)) in enumerate(zip(near, spots)):
            if index % 2 == 0:
                far = lax.ppermute(from_below, 'tpa', up_ring)
            else:
                far = lax.ppermute(from_above, 'tpa', down_ring)
            y_all = put(y_all, from_below, slot, row - 1, start)
            y_all = put(y_all, from_above, slot, row + 1, start)
            fars.append(far)
        for far, (slot, start) in zip(fars, spots):
            y_all = put(y_all, far, slot, row - 2, start)
        layer_out = y_all.reshape(batch_loc, seq_len, model_dim)
        return (layer_out, k_cache, v_cache, w_query, w_key, w_value, o_rows, w_gate, w_up, down_rows)

    batch_spec = P(('part', 'tpb'), None, None)
    len_spec = P(('part', 'tpb'))
    cache_spec = P(('part', 'tpb'), None, 'tpa', None)
    train_cols = P('part', ('tpa', 'tpb'))
    train_rows = P(('part', 'tpa', 'tpb'), None)
    gain_spec = P('part')
    gen_cols = P('part', 'tpa')
    gen_rows = P(('part', 'tpa'), None)
    return jax.shard_map(layer_step, mesh=mesh, in_specs=(batch_spec, len_spec, cache_spec, cache_spec, train_cols, train_rows, train_cols, train_rows, gain_spec, gain_spec), out_specs=(batch_spec, cache_spec, cache_spec, gen_cols, gen_cols, gen_cols, gen_rows, gen_cols, gen_cols, gen_rows), check_vma=False)
```

```python
import functools
import math
import jax
import jax.numpy as jnp
from jax import lax
from jax.experimental import pallas as pl
from jax.experimental.pallas import tpu as pltpu
from jax.sharding import PartitionSpec as P

ROPE_BASE = 500000.0
ROPE_FACTOR = 8.0
LOW_FREQ = 1.0
HIGH_FREQ = 4.0
ORIG_CONTEXT = 8192.0
NORM_EPS = 1e-5
MASK_VALUE = -1e30
Q_TILE = 256
FF_TILE = 512
OUT_TILE = 512
ROW_TILE = 512
FIRST_SPLIT = (4, 4, 2)
LATER_SPLIT = (2, 2)


def inv_rms(x_in):
    x_wide = x_in.astype(jnp.float32)
    return lax.rsqrt(jnp.mean(x_wide * x_wide, axis=-1, keepdims=True) + NORM_EPS)


def scaled(x_in, inv_scale, gain_vec):
    return (x_in.astype(jnp.float32) * inv_scale * gain_vec.astype(jnp.float32)).astype(jnp.bfloat16)


def rope_tables(seq_len, head_dim):
    exponent = jnp.arange(head_dim // 2, dtype=jnp.float32) * (2.0 / head_dim)
    inv_freq = 1.0 / jnp.power(ROPE_BASE, exponent)
    wavelen = 2.0 * math.pi / inv_freq
    smooth = (ORIG_CONTEXT / wavelen - LOW_FREQ) / (HIGH_FREQ - LOW_FREQ)
    blended = (1.0 - smooth) * inv_freq / ROPE_FACTOR + smooth * inv_freq
    rope_freq = jnp.where(wavelen < ORIG_CONTEXT / HIGH_FREQ, inv_freq, jnp.where(wavelen > ORIG_CONTEXT / LOW_FREQ, inv_freq / ROPE_FACTOR, blended))
    angles = jnp.arange(seq_len, dtype=jnp.float32)[:, None] * rope_freq[None, :]
    return jnp.cos(angles), jnp.sin(angles)


def attention_kernel(head_dim, group_size, len_ref, qkv_ref, cos_ref, sin_ref, out_ref, kl_scr, kr_scr, vl_scr, vr_scr):
    seq_len = qkv_ref.shape[1]
    pair = 2 * head_dim
    length = len_ref[pl.program_id(0)]
    lane = lax.broadcasted_iota(jnp.int32, (1, pair), 1)
    low_lane = lane < head_dim
    first_half = lax.rem(lane, head_dim) < head_dim // 2
    one_low = jnp.where(lane == 0, 1.0, 0.0)
    one_high = jnp.where(lane == head_dim, 1.0, 0.0)

    def rope(vec, rows):
        ahead = pltpu.roll(vec, pair - head_dim // 2, 1)
        behind = pltpu.roll(vec, head_dim // 2, 1)
        return vec * cos_ref[rows, :] + jnp.where(first_half, ahead, behind) * sin_ref[rows, :]

    q_cols = group_size * head_dim
    for start in range(0, seq_len, Q_TILE):
        rows = pl.ds(start, Q_TILE)
        kv = qkv_ref[0, rows, q_cols:q_cols + pair].astype(jnp.float32)
        k_rot = rope(kv, rows)
        key_id = start + lax.broadcasted_iota(jnp.int32, (Q_TILE, pair), 0)
        bias = jnp.where(key_id < length, 0.0, MASK_VALUE)
        kl_scr[rows, :] = jnp.where(low_lane, k_rot, bias * one_high).astype(jnp.bfloat16)
        kr_scr[rows, :] = jnp.where(low_lane, bias * one_low, pltpu.roll(k_rot, head_dim, 1)).astype(jnp.bfloat16)
        vl_scr[rows, :] = jnp.where(low_lane, pltpu.roll(kv, head_dim, 1), 0.0).astype(jnp.bfloat16)
        vr_scr[rows, :] = jnp.where(low_lane, 0.0, kv).astype(jnp.bfloat16)

    for start in range(0, seq_len, Q_TILE):
        rows = pl.ds(start, Q_TILE)
        keys = start + Q_TILE
        causal = lax.broadcasted_iota(jnp.int32, (Q_TILE, Q_TILE), 1) <= lax.broadcasted_iota(jnp.int32, (Q_TILE, Q_TILE), 0)

        def weights(query, k_scr):
            scores = lax.dot_general(query, k_scr[:keys, :], (((1,), (1,)), ((), ())), preferred_element_type=jnp.float32)
            parts = [scores[:, block:block + Q_TILE] for block in range(0, keys, Q_TILE)]
            parts[-1] = jnp.where(causal, parts[-1], MASK_VALUE)
            top = parts[0]
            for part in parts[1:]:
                top = jnp.maximum(top, part)
            top = jnp.max(top, axis=1, keepdims=True)
            parts = [jnp.exp(part - top) for part in parts]
            total = parts[0]
            for part in parts[1:]:
                total = total + part
            scale = 1.0 / jnp.sum(total, axis=1, keepdims=True)
            return jnp.concatenate([(part * scale).astype(jnp.bfloat16) for part in parts], axis=1)

        def head_pair(index, carry):
            cols = pl.ds(pl.multiple_of(index * pair, pair), pair)
            query = rope(qkv_ref[0, rows, cols].astype(jnp.float32), rows).astype(jnp.bfloat16).astype(jnp.float32) * head_dim ** -0.5
            left = weights(jnp.where(low_lane, query, one_high).astype(jnp.bfloat16), kl_scr)
            right = weights(jnp.where(low_lane, one_low, query).astype(jnp.bfloat16), kr_scr)
            acc = jnp.dot(left, vl_scr[:keys, :], preferred_element_type=jnp.float32)
            acc = acc + jnp.dot(right, vr_scr[:keys, :], preferred_element_type=jnp.float32)
            out_ref[0, rows, cols] = acc.astype(jnp.bfloat16)
            return carry

        lax.fori_loop(0, group_size // 2, head_pair, 0, unroll=2)


def attention(qkv_act, lengths, cos_tab, sin_tab, kv_heads, head_dim):
    batch, seq_len, qkv_cols = qkv_act.shape
    group_cols = qkv_cols // kv_heads
    group_size = group_cols // head_dim - 2
    out_cols = group_size * head_dim
    pair = 2 * head_dim
    cos_pair = jnp.tile(cos_tab, (1, 4))
    sin_pair = jnp.tile(jnp.concatenate([-sin_tab, sin_tab], axis=1), (1, 2))
    flops = 2 * 2 * batch * kv_heads * group_size * seq_len * seq_len * head_dim
    return pl.pallas_call(
        functools.partial(attention_kernel, head_dim, group_size),
        out_shape=jax.ShapeDtypeStruct((batch, seq_len, kv_heads * out_cols), jnp.bfloat16),
        grid_spec=pltpu.PrefetchScalarGridSpec(
            num_scalar_prefetch=1,
            grid=(batch, kv_heads),
            in_specs=[
                pl.BlockSpec((1, seq_len, group_cols), lambda b, g, _: (b, 0, g)),
                pl.BlockSpec((seq_len, pair), lambda b, g, _: (0, 0)),
                pl.BlockSpec((seq_len, pair), lambda b, g, _: (0, 0)),
            ],
            out_specs=pl.BlockSpec((1, seq_len, out_cols), lambda b, g, _: (b, 0, g)),
            scratch_shapes=[pltpu.VMEM((seq_len, pair), jnp.bfloat16)] * 4,
        ),
        compiler_params=pltpu.CompilerParams(dimension_semantics=('arbitrary', 'arbitrary'), vmem_limit_bytes=48 * 1024 * 1024),
        cost_estimate=pl.CostEstimate(flops=4 * flops, bytes_accessed=2 * batch * seq_len * (qkv_cols + kv_heads * out_cols), transcendentals=batch * kv_heads * group_size * seq_len * seq_len),
        name='prefill_attention',
    )(lengths, qkv_act, cos_pair, sin_pair)


def empty(shape, dtype):
    return pl.pallas_call(lambda out_ref: None, out_shape=jax.ShapeDtypeStruct(shape, dtype), out_specs=pl.BlockSpec(memory_space=pl.ANY), name='output_buffer')()


def row_tiles(rows, body):
    tile = min(ROW_TILE, rows)

    def step(index, carry):
        body(pl.ds(pl.multiple_of(index * tile, tile), tile))
        return carry

    lax.fori_loop(0, rows // tile, step, 0)


def gate_up_kernel(h_ref, gain_ref, gate_ref, up_ref, mid_ref, norm_scr):
    rows = norm_scr.shape[0]
    contract = (((1,), (1,)), ((), ()))

    @pl.when(pl.program_id(0) == 0)
    def _():
        def step(index, carry):
            part = pl.ds(pl.multiple_of(index * 64, 64), 64)
            wide = h_ref[0, part, :].astype(jnp.float32)
            mean_sq = jnp.mean(wide * wide, axis=1, keepdims=True)
            norm_scr[part, :] = (wide * lax.rsqrt(mean_sq + NORM_EPS) * gain_ref[...].astype(jnp.float32)).astype(jnp.bfloat16)
            return carry

        lax.fori_loop(0, rows // 64, step, 0)

    def body(part):
        normed = norm_scr[part, :]
        gate = lax.dot_general(normed, gate_ref[0], contract, preferred_element_type=jnp.float32).astype(jnp.bfloat16).astype(jnp.float32)
        up = lax.dot_general(normed, up_ref[0], contract, preferred_element_type=jnp.float32).astype(jnp.bfloat16).astype(jnp.float32)
        mid_ref[part, :] = (jax.nn.silu(gate) * up).astype(jnp.bfloat16)

    row_tiles(rows, body)


def gate_up(hidden, gain, weights, slot, start, rows):
    dim = hidden.shape[2]
    ff = weights.shape[1]
    tile = min(FF_TILE, ff)
    return pl.pallas_call(
        gate_up_kernel,
        out_shape=jax.ShapeDtypeStruct((rows, ff), jnp.bfloat16),
        grid=(ff // tile,),
        in_specs=[
            pl.BlockSpec((1, rows, dim), lambda j: (slot, start // rows, 0)),
            pl.BlockSpec((1, dim), lambda j: (0, 0)),
            pl.BlockSpec((1, tile, dim), lambda j: (0, j, 0)),
            pl.BlockSpec((1, tile, dim), lambda j: (1, j, 0)),
        ],
        out_specs=pl.BlockSpec((rows, tile), lambda j: (0, j)),
        scratch_shapes=[pltpu.VMEM((rows, dim), jnp.bfloat16)],
        compiler_params=pltpu.CompilerParams(dimension_semantics=('arbitrary',), vmem_limit_bytes=56 * 1024 * 1024),
        cost_estimate=pl.CostEstimate(flops=4 * rows * dim * ff, bytes_accessed=4 * dim * ff + 2 * rows * (dim + ff), transcendentals=rows * ff),
        name='gate_up',
    )(hidden, gain[None, :], weights, weights)


def down_kernel(row_ref, h_ref, mid_ref, w_ref, y_in, y_ref, part_ref):
    def body(part):
        acc = jnp.dot(mid_ref[part, :], w_ref[0], preferred_element_type=jnp.float32)
        y_part = (h_ref[0, part, :].astype(jnp.float32) + acc).astype(jnp.bfloat16)
        part_ref[part, :] = y_part
        y_ref[0, 0, part, :] = y_part

    row_tiles(mid_ref.shape[0], body)


def down_proj(row, hidden, mid, weights, y_all, slot, start):
    rows, ff = mid.shape
    dim = hidden.shape[2]
    tile = min(OUT_TILE, dim)
    return pl.pallas_call(
        down_kernel,
        out_shape=(jax.ShapeDtypeStruct(y_all.shape, jnp.bfloat16), jax.ShapeDtypeStruct((rows, dim), jnp.bfloat16)),
        grid_spec=pltpu.PrefetchScalarGridSpec(
            num_scalar_prefetch=1,
            grid=(dim // tile,),
            in_specs=[
                pl.BlockSpec((1, rows, tile), lambda j, _: (slot, start // rows, j)),
                pl.BlockSpec((rows, ff), lambda j, _: (0, 0)),
                pl.BlockSpec((1, ff, tile), lambda j, _: (2, 0, j)),
                pl.BlockSpec(memory_space=pl.ANY),
            ],
            out_specs=(
                pl.BlockSpec((1, 1, rows, tile), lambda j, own: (slot, own[0], start // rows, j)),
                pl.BlockSpec((rows, tile), lambda j, _: (0, j)),
            ),
        ),
        input_output_aliases={4: 0},
        compiler_params=pltpu.CompilerParams(dimension_semantics=('arbitrary',), vmem_limit_bytes=56 * 1024 * 1024),
        cost_estimate=pl.CostEstimate(flops=2 * rows * dim * ff, bytes_accessed=2 * dim * ff + 2 * rows * (3 * dim + ff), transcendentals=0),
        name='down_proj',
    )(row, hidden, mid, weights, y_all)


def matmul_t(lhs, rhs_t):
    return lax.dot_general(lhs, rhs_t, (((lhs.ndim - 1,), (1,)), ((), ())), preferred_element_type=jnp.float32)


def solution(mesh):
    n_tpa = mesh.shape['tpa']
    n_tpb = mesh.shape['tpb']
    up_ring = [(i, (i + 1) % n_tpa) for i in range(n_tpa)]
    down_ring = [(i, (i - 1) % n_tpa) for i in range(n_tpa)]
    both = ('tpa', 'tpb')

    def layer_step(x_loc, len_loc, k_buf, v_buf, w_qkv, w_o, w_gate_up, w_down, g_attn, g_mlp):
        row = lax.axis_index('tpa')
        batch_loc, seq_len, model_dim = x_loc.shape
        head_dim = k_buf.shape[3]
        own_batch = batch_loc // n_tpa
        ff_block = w_gate_up.shape[1] // 2
        qkv_row = w_qkv.shape[1] * n_tpb
        o_row = w_o.shape[0] * n_tpb
        ff_row = ff_block * n_tpb

        qkv_block = w_qkv.shape[1]
        qkvo = lax.all_gather(jnp.concatenate([w_qkv.T, w_o], axis=0), both, axis=0, tiled=False)
        mlp_full = lax.all_gather(jnp.concatenate([w_gate_up.T.reshape(2, ff_block, model_dim), w_down[None]], axis=0), both, axis=1, tiled=True)
        qkv_t = qkvo[:, :qkv_block].reshape(-1, model_dim)

        cos_tab, sin_tab = rope_tables(seq_len, head_dim)
        x_own = lax.dynamic_index_in_dim(x_loc.reshape(own_batch, n_tpa, seq_len, model_dim), row, 1, keepdims=False)
        inv_all = inv_rms(x_loc)
        inv_own = lax.dynamic_index_in_dim(inv_all.reshape(own_batch, n_tpa, seq_len, 1), row, 1, keepdims=False)
        len_own = lax.dynamic_index_in_dim(len_loc.reshape(own_batch, n_tpa), row, 1, keepdims=False)

        qkv_act = matmul_t(scaled(x_own, inv_own, g_attn), qkv_t).astype(jnp.bfloat16)
        attn_out = attention(qkv_act, len_own, cos_tab, sin_tab, n_tpa * k_buf.shape[2], head_dim)
        attn_out, qkvo = lax.optimization_barrier((attn_out, qkvo))
        o_full = qkvo[:, qkv_block:].reshape(-1, model_dim)
        attn_proj = jnp.dot(attn_out, o_full, preferred_element_type=jnp.float32)
        hidden = (x_own.astype(jnp.float32) + attn_proj).astype(jnp.bfloat16)

        y_all = empty((own_batch, n_tpa, seq_len, model_dim), jnp.bfloat16)

        def put(y_buf, piece, slot, owner, start):
            return lax.dynamic_update_slice(y_buf, piece[None, None], (slot, lax.rem(owner + n_tpa, n_tpa), start, 0))

        spots = []
        for slot in range(own_batch):
            start = 0
            for share in FIRST_SPLIT if slot == 0 else LATER_SPLIT:
                spots.append((slot, start, seq_len // share))
                start += seq_len // share
        fars = []
        near = []
        upward = [0, 0]
        row_arg = row.astype(jnp.int32)[None]
        for slot, start, rows in spots:
            mid_act = gate_up(hidden, g_mlp, mlp_full, slot, start, rows)
            y_all, part = down_proj(row_arg, hidden, mid_act, mlp_full, y_all, slot, start)
            near.append((lax.ppermute(part, 'tpa', up_ring), lax.ppermute(part, 'tpa', down_ring)))

        y_all, x_late, qkvo_late, mlp_late = lax.optimization_barrier((y_all, x_loc, qkvo, mlp_full))
        kv_cols = k_buf.shape[2] * head_dim
        q_cols = qkv_row - 2 * kv_cols
        own_blocks = lax.dynamic_slice_in_dim(qkvo_late, row * n_tpb, n_tpb, 0)
        qkv_own = own_blocks[:, :qkv_block].reshape(qkv_row, model_dim)
        o_rows = own_blocks[:, qkv_block:].reshape(o_row, model_dim)
        w_query = qkv_own[:q_cols].T
        w_key = qkv_own[q_cols:q_cols + kv_cols].T
        w_value = qkv_own[q_cols + kv_cols:].T
        kv_new = matmul_t(scaled(x_late, inv_all, g_attn), qkv_own[q_cols:]).astype(jnp.bfloat16)
        half_dim = head_dim // 2
        k_first = kv_new[..., :half_dim].astype(jnp.float32)
        k_second = kv_new[..., half_dim:head_dim].astype(jnp.float32)
        k_rot = jnp.concatenate([k_first * cos_tab - k_second * sin_tab, k_second * cos_tab + k_first * sin_tab], axis=-1).astype(jnp.bfloat16)
        valid_pos = (jnp.arange(seq_len)[None, :] < len_loc[:, None])[:, :, None, None]
        k_cache = jnp.where(valid_pos, k_rot[:, :, None, :], k_buf)
        v_cache = jnp.where(valid_pos, kv_new[:, :, None, head_dim:], v_buf)
        mlp_own = lax.dynamic_slice_in_dim(mlp_late, row * ff_row, ff_row, 1)
        w_gate = mlp_own[0].T
        w_up = mlp_own[1].T
        down_rows = mlp_own[2]
        cache_outs = (k_cache, v_cache, w_query, w_key, w_value, o_rows)
        weight_outs = (w_gate, w_up, down_rows)
        near[-2], cache_outs = lax.optimization_barrier((near[-2], cache_outs))
        near[-1], weight_outs = lax.optimization_barrier((near[-1], weight_outs))
        k_cache, v_cache, w_query, w_key, w_value, o_rows = cache_outs
        w_gate, w_up, down_rows = weight_outs
        for (from_below, from_above), (slot, start, rows) in zip(near, spots):
            if upward[0] <= upward[1]:
                upward[0] += rows
                far = lax.ppermute(from_below, 'tpa', up_ring)
            else:
                upward[1] += rows
                far = lax.ppermute(from_above, 'tpa', down_ring)
            y_all = put(y_all, from_below, slot, row - 1, start)
            y_all = put(y_all, from_above, slot, row + 1, start)
            fars.append(far)
        for far, (slot, start, rows) in zip(fars, spots):
            y_all = put(y_all, far, slot, row - 2, start)
        layer_out = y_all.reshape(batch_loc, seq_len, model_dim)
        return (layer_out, k_cache, v_cache, w_query, w_key, w_value, o_rows, w_gate, w_up, down_rows)

    batch_spec = P(('part', 'tpb'), None, None)
    len_spec = P(('part', 'tpb'))
    cache_spec = P(('part', 'tpb'), None, 'tpa', None)
    train_cols = P('part', ('tpa', 'tpb'))
    train_rows = P(('part', 'tpa', 'tpb'), None)
    gain_spec = P('part')
    gen_cols = P('part', 'tpa')
    gen_rows = P(('part', 'tpa'), None)
    return jax.shard_map(layer_step, mesh=mesh, in_specs=(batch_spec, len_spec, cache_spec, cache_spec, train_cols, train_rows, train_cols, train_rows, gain_spec, gain_spec), out_specs=(batch_spec, cache_spec, cache_spec, gen_cols, gen_cols, gen_cols, gen_rows, gen_cols, gen_cols, gen_rows), check_vma=False)
```

```python
import functools
import math
import jax
import jax.numpy as jnp
from jax import lax
from jax.experimental import pallas as pl
from jax.experimental.pallas import tpu as pltpu
from jax.sharding import PartitionSpec as P

ROPE_BASE = 500000.0
ROPE_FACTOR = 8.0
LOW_FREQ = 1.0
HIGH_FREQ = 4.0
ORIG_CONTEXT = 8192.0
NORM_EPS = 1e-5
MASK_VALUE = -1e30
Q_TILE = 256
FF_TILE = 512
OUT_TILE = 512
NT_DIMS = (((1,), (1,)), ((), ()))
FIRST_SPLIT = (4, 4, 2)
LATER_SPLIT = (2, 2)


def inv_rms(x_in):
    x_wide = x_in.astype(jnp.float32)
    return lax.rsqrt(jnp.mean(x_wide * x_wide, axis=-1, keepdims=True) + NORM_EPS)


def scaled(x_in, inv_scale, gain_vec):
    return (x_in.astype(jnp.float32) * inv_scale * gain_vec.astype(jnp.float32)).astype(jnp.bfloat16)


def rope_tables(seq_len, head_dim):
    exponent = jnp.arange(head_dim // 2, dtype=jnp.float32) * (2.0 / head_dim)
    inv_freq = 1.0 / jnp.power(ROPE_BASE, exponent)
    wavelen = 2.0 * math.pi / inv_freq
    smooth = (ORIG_CONTEXT / wavelen - LOW_FREQ) / (HIGH_FREQ - LOW_FREQ)
    blended = (1.0 - smooth) * inv_freq / ROPE_FACTOR + smooth * inv_freq
    rope_freq = jnp.where(wavelen < ORIG_CONTEXT / HIGH_FREQ, inv_freq, jnp.where(wavelen > ORIG_CONTEXT / LOW_FREQ, inv_freq / ROPE_FACTOR, blended))
    angles = jnp.arange(seq_len, dtype=jnp.float32)[:, None] * rope_freq[None, :]
    return jnp.cos(angles), jnp.sin(angles)


def attention_kernel(head_dim, group_size, len_ref, qkv_ref, cos_ref, sin_ref, out_ref, kl_scr, kr_scr, vl_scr, vr_scr):
    seq_len = qkv_ref.shape[1]
    pair = 2 * head_dim
    length = len_ref[pl.program_id(0)]
    lane = lax.broadcasted_iota(jnp.int32, (1, pair), 1)
    low_lane = lane < head_dim
    first_half = lax.rem(lane, head_dim) < head_dim // 2
    one_low = jnp.where(lane == 0, 1.0, 0.0)
    one_high = jnp.where(lane == head_dim, 1.0, 0.0)

    def rope(vec, rows):
        ahead = pltpu.roll(vec, pair - head_dim // 2, 1)
        behind = pltpu.roll(vec, head_dim // 2, 1)
        return vec * cos_ref[rows, :] + jnp.where(first_half, ahead, behind) * sin_ref[rows, :]

    q_cols = group_size * head_dim
    for start in range(0, seq_len, Q_TILE):
        rows = pl.ds(start, Q_TILE)
        kv = qkv_ref[0, rows, q_cols:q_cols + pair].astype(jnp.float32)
        k_rot = rope(kv, rows)
        key_id = start + lax.broadcasted_iota(jnp.int32, (Q_TILE, pair), 0)
        bias = jnp.where(key_id < length, 0.0, MASK_VALUE)
        kl_scr[rows, :] = jnp.where(low_lane, k_rot, bias * one_high).astype(jnp.bfloat16)
        kr_scr[rows, :] = jnp.where(low_lane, bias * one_low, pltpu.roll(k_rot, head_dim, 1)).astype(jnp.bfloat16)
        vl_scr[rows, :] = jnp.where(low_lane, pltpu.roll(kv, head_dim, 1), 0.0).astype(jnp.bfloat16)
        vr_scr[rows, :] = jnp.where(low_lane, 0.0, kv).astype(jnp.bfloat16)

    for start in range(0, seq_len, Q_TILE):
        rows = pl.ds(start, Q_TILE)
        keys = start + Q_TILE
        causal = lax.broadcasted_iota(jnp.int32, (Q_TILE, Q_TILE), 1) <= lax.broadcasted_iota(jnp.int32, (Q_TILE, Q_TILE), 0)

        def weights(query, k_scr):
            scores = lax.dot_general(query, k_scr[:keys, :], (((1,), (1,)), ((), ())), preferred_element_type=jnp.float32)
            parts = [scores[:, block:block + Q_TILE] for block in range(0, keys, Q_TILE)]
            parts[-1] = jnp.where(causal, parts[-1], MASK_VALUE)
            top = parts[0]
            for part in parts[1:]:
                top = jnp.maximum(top, part)
            top = jnp.max(top, axis=1, keepdims=True)
            parts = [jnp.exp(part - top) for part in parts]
            total = parts[0]
            for part in parts[1:]:
                total = total + part
            scale = 1.0 / jnp.sum(total, axis=1, keepdims=True)
            return jnp.concatenate([(part * scale).astype(jnp.bfloat16) for part in parts], axis=1)

        def head_pair(index, carry):
            cols = pl.ds(pl.multiple_of(index * pair, pair), pair)
            query = rope(qkv_ref[0, rows, cols].astype(jnp.float32), rows).astype(jnp.bfloat16).astype(jnp.float32) * head_dim ** -0.5
            left = weights(jnp.where(low_lane, query, one_high).astype(jnp.bfloat16), kl_scr)
            right = weights(jnp.where(low_lane, one_low, query).astype(jnp.bfloat16), kr_scr)
            acc = jnp.dot(left, vl_scr[:keys, :], preferred_element_type=jnp.float32)
            acc = acc + jnp.dot(right, vr_scr[:keys, :], preferred_element_type=jnp.float32)
            out_ref[0, rows, cols] = acc.astype(jnp.bfloat16)
            return carry

        lax.fori_loop(0, group_size // 2, head_pair, 0, unroll=2)


def attention(qkv_act, lengths, cos_tab, sin_tab, kv_heads, head_dim):
    batch, seq_len, qkv_cols = qkv_act.shape
    group_cols = qkv_cols // kv_heads
    group_size = group_cols // head_dim - 2
    out_cols = group_size * head_dim
    pair = 2 * head_dim
    cos_pair = jnp.tile(cos_tab, (1, 4))
    sin_pair = jnp.tile(jnp.concatenate([-sin_tab, sin_tab], axis=1), (1, 2))
    flops = 2 * 2 * batch * kv_heads * group_size * seq_len * seq_len * head_dim
    return pl.pallas_call(
        functools.partial(attention_kernel, head_dim, group_size),
        out_shape=jax.ShapeDtypeStruct((batch, seq_len, kv_heads * out_cols), jnp.bfloat16),
        grid_spec=pltpu.PrefetchScalarGridSpec(
            num_scalar_prefetch=1,
            grid=(batch, kv_heads),
            in_specs=[
                pl.BlockSpec((1, seq_len, group_cols), lambda b, g, _: (b, 0, g)),
                pl.BlockSpec((seq_len, pair), lambda b, g, _: (0, 0)),
                pl.BlockSpec((seq_len, pair), lambda b, g, _: (0, 0)),
            ],
            out_specs=pl.BlockSpec((1, seq_len, out_cols), lambda b, g, _: (b, 0, g)),
            scratch_shapes=[pltpu.VMEM((seq_len, pair), jnp.bfloat16)] * 4,
        ),
        compiler_params=pltpu.CompilerParams(dimension_semantics=('arbitrary', 'arbitrary'), vmem_limit_bytes=48 * 1024 * 1024),
        cost_estimate=pl.CostEstimate(flops=4 * flops, bytes_accessed=2 * batch * seq_len * (qkv_cols + kv_heads * out_cols), transcendentals=batch * kv_heads * group_size * seq_len * seq_len),
        name='prefill_attention',
    )(lengths, qkv_act, cos_pair, sin_pair)


def empty(shape, dtype):
    return pl.pallas_call(lambda out_ref: None, out_shape=jax.ShapeDtypeStruct(shape, dtype), out_specs=pl.BlockSpec(memory_space=pl.ANY), name='output_buffer')()


def normalise(src, gain, dst, rows):
    def step(index, carry):
        part = pl.ds(pl.multiple_of(index * 64, 64), 64)
        wide = src[part, :].astype(jnp.float32)
        mean_sq = jnp.mean(wide * wide, axis=1, keepdims=True)
        dst[part, :] = (wide * lax.rsqrt(mean_sq + NORM_EPS) * gain).astype(jnp.bfloat16)
        return carry

    lax.fori_loop(0, rows // 64, step, 0)


def mlp_kernel(slot, start, row_ref, h_ref, gain_ref, w_ref, y_in, y_ref, part_ref, h_scr, u_scr, acc_scr, mid_scr, gu_buf, down_buf, gu_sem, down_sem, h_sem, out_sem):
    rows, dim = h_scr.shape
    depth, _, tile, _ = gu_buf.shape
    steps = w_ref.shape[1] // tile
    out_tile = min(OUT_TILE, dim)

    def gu_copy(step):
        return pltpu.make_async_copy(w_ref.at[0:2, pl.ds(pl.multiple_of(step * tile, tile), tile), :], gu_buf.at[lax.rem(step, depth)], gu_sem.at[lax.rem(step, depth)])

    def down_copy(step):
        return pltpu.make_async_copy(w_ref.at[2, pl.ds(pl.multiple_of(step * tile, tile), tile), :], down_buf.at[lax.rem(step, depth)], down_sem.at[lax.rem(step, depth)])

    h_copy = pltpu.make_async_copy(h_ref.at[slot, pl.ds(start, rows), :], h_scr, h_sem)
    h_copy.start()
    for step in range(min(depth - 1, steps)):
        gu_copy(step).start()
    for step in range(min(depth - 2, steps)):
        down_copy(step).start()
    mid_scr[...] = jnp.zeros_like(mid_scr)
    h_copy.wait()
    normalise(h_scr, gain_ref[...].astype(jnp.float32), u_scr, rows)

    def widen(index, carry):
        part = pl.ds(pl.multiple_of(index * 64, 64), 64)
        acc_scr[part, :] = h_scr[part, :].astype(jnp.float32)
        return carry

    lax.fori_loop(0, rows // 64, widen, 0)

    def add_down(index):
        for col in range(0, dim, out_tile):
            cols = slice(col, col + out_tile)
            acc_scr[:, cols] += jnp.dot(mid_scr[...], down_buf[index, :, cols], preferred_element_type=jnp.float32)

    def body(step, carry):
        @pl.when(step + depth - 1 < steps)
        def _():
            gu_copy(step + depth - 1).start()

        @pl.when(step + depth - 2 < steps)
        def _():
            down_copy(step + depth - 2).start()

        gu_copy(step).wait()
        before = jnp.maximum(step - 1, 0)

        @pl.when(step != 1)
        def _():
            down_copy(before).wait()

        index = lax.rem(step, depth)
        gate = lax.dot_general(u_scr[...], gu_buf[index, 0], NT_DIMS, preferred_element_type=jnp.float32)
        up = lax.dot_general(u_scr[...], gu_buf[index, 1], NT_DIMS, preferred_element_type=jnp.float32)
        add_down(lax.rem(before, depth))
        gate = gate.astype(jnp.bfloat16).astype(jnp.float32)
        up = up.astype(jnp.bfloat16).astype(jnp.float32)
        mid_scr[...] = (jax.nn.silu(gate) * up).astype(jnp.bfloat16)
        return carry

    lax.fori_loop(0, steps, body, 0)
    if steps > 1:
        down_copy(steps - 1).wait()
    add_down((steps - 1) % depth)

    def narrow(index, carry):
        part = pl.ds(pl.multiple_of(index * 64, 64), 64)
        h_scr[part, :] = acc_scr[part, :].astype(jnp.bfloat16)
        return carry

    lax.fori_loop(0, rows // 64, narrow, 0)
    part_out = pltpu.make_async_copy(h_scr, part_ref, out_sem.at[0])
    y_out = pltpu.make_async_copy(h_scr, y_ref.at[slot, row_ref[0], pl.ds(start, rows), :], out_sem.at[1])
    part_out.start()
    y_out.start()
    part_out.wait()
    y_out.wait()


def mlp(row, hidden, gain, weights, y_all, slot, start, rows):
    dim = hidden.shape[2]
    ff = weights.shape[1]
    tile = min(FF_TILE, ff)
    depth = 3
    anywhere = pl.BlockSpec(memory_space=pl.ANY)
    return pl.pallas_call(
        functools.partial(mlp_kernel, slot, start),
        out_shape=(jax.ShapeDtypeStruct(y_all.shape, jnp.bfloat16), jax.ShapeDtypeStruct((rows, dim), jnp.bfloat16)),
        in_specs=[pl.BlockSpec(memory_space=pltpu.SMEM), anywhere, pl.BlockSpec(memory_space=pltpu.VMEM), anywhere, anywhere],
        out_specs=(anywhere, anywhere),
        scratch_shapes=[
            pltpu.VMEM((rows, dim), jnp.bfloat16),
            pltpu.VMEM((rows, dim), jnp.bfloat16),
            pltpu.VMEM((rows, dim), jnp.float32),
            pltpu.VMEM((rows, tile), jnp.bfloat16),
            pltpu.VMEM((depth, 2, tile, dim), jnp.bfloat16),
            pltpu.VMEM((depth, tile, dim), jnp.bfloat16),
            pltpu.SemaphoreType.DMA((depth,)),
            pltpu.SemaphoreType.DMA((depth,)),
            pltpu.SemaphoreType.DMA,
            pltpu.SemaphoreType.DMA((2,)),
        ],
        input_output_aliases={4: 0},
        compiler_params=pltpu.CompilerParams(vmem_limit_bytes=58 * 1024 * 1024),
        cost_estimate=pl.CostEstimate(flops=6 * rows * dim * ff, bytes_accessed=6 * dim * ff + 8 * rows * dim, transcendentals=rows * ff),
        name='mlp_block',
    )(row, hidden, gain[None, :], weights, y_all)


def qkv_kernel(qkv_block, row_ref, x_ref, gain_ref, w_ref, out_ref, u_scr, w_scr):
    piece, tile = pl.program_id(0), pl.program_id(1)
    rows = x_ref.shape[2]

    @pl.when(tile == 0)
    def _():
        for block in range(w_ref.shape[0]):
            w_scr[block * qkv_block:(block + 1) * qkv_block, :] = w_ref[block, :qkv_block, :]

    @pl.when(piece == 0)
    def _():
        normalise(x_ref.at[0, 0], gain_ref[...].astype(jnp.float32), u_scr.at[tile], rows)

    out_ref[0] = lax.dot_general(u_scr[tile], w_scr[...], NT_DIMS, preferred_element_type=jnp.float32).astype(jnp.bfloat16)


def qkv_proj(row, x_rows, gain, qkvo, qkv_block, pieces):
    own_batch, _, seq_len, dim = x_rows.shape
    blocks = qkvo.shape[0] // pieces
    rows = min(512, seq_len)
    per = seq_len // rows
    tiles = own_batch * per
    cols = blocks * qkv_block

    def x_index(piece, tile, own):
        at = jnp.where(piece == 0, tile, tiles - 1)
        return (at // per, own[0], at % per, 0)

    return pl.pallas_call(
        functools.partial(qkv_kernel, qkv_block),
        out_shape=jax.ShapeDtypeStruct((own_batch, seq_len, pieces * cols), jnp.bfloat16),
        grid_spec=pltpu.PrefetchScalarGridSpec(
            num_scalar_prefetch=1,
            grid=(pieces, tiles),
            in_specs=[
                pl.BlockSpec((1, 1, rows, dim), x_index),
                pl.BlockSpec((1, dim), lambda p, t, _: (0, 0)),
                pl.BlockSpec((blocks,) + qkvo.shape[1:], lambda p, t, _: (p, 0, 0)),
            ],
            out_specs=pl.BlockSpec((1, rows, cols), lambda p, t, _: (t // per, t % per, p)),
            scratch_shapes=[pltpu.VMEM((tiles, rows, dim), jnp.bfloat16), pltpu.VMEM((cols, dim), jnp.bfloat16)],
        ),
        compiler_params=pltpu.CompilerParams(dimension_semantics=('arbitrary', 'arbitrary'), vmem_limit_bytes=60 * 1024 * 1024),
        cost_estimate=pl.CostEstimate(flops=2 * own_batch * seq_len * dim * pieces * cols, bytes_accessed=2 * dim * (pieces * cols + 2 * own_batch * seq_len), transcendentals=0),
        name='qkv_proj',
    )(row, x_rows, gain[None, :], qkvo)


def out_kernel(qkv_block, row_ref, a_ref, x_ref, w_ref, h_ref, w_scr, sem):
    @pl.when(pl.program_id(0) == 0)
    def _():
        copy = pltpu.make_async_copy(w_ref.at[:, pl.ds(qkv_block, w_scr.shape[1]), :], w_scr, sem)
        copy.start()
        copy.wait()

    dim = h_ref.shape[2]
    depth = w_scr.shape[0] * w_scr.shape[1]
    out_tile = min(OUT_TILE, dim)
    for col in range(0, dim, out_tile):
        cols = slice(col, col + out_tile)
        acc = jnp.dot(a_ref[0], w_scr[:, :, cols].reshape(depth, out_tile), preferred_element_type=jnp.float32)
        h_ref[0, :, cols] = (x_ref[0, 0, :, cols].astype(jnp.float32) + acc).astype(jnp.bfloat16)


def out_proj(row, attn, x_rows, qkvo, qkv_block):
    own_batch, seq_len, depth = attn.shape
    dim = x_rows.shape[3]
    rows = min(512, seq_len)
    per = seq_len // rows
    return pl.pallas_call(
        functools.partial(out_kernel, qkv_block),
        out_shape=jax.ShapeDtypeStruct((own_batch, seq_len, dim), jnp.bfloat16),
        grid_spec=pltpu.PrefetchScalarGridSpec(
            num_scalar_prefetch=1,
            grid=(own_batch * per,),
            in_specs=[
                pl.BlockSpec((1, rows, depth), lambda t, _: (t // per, t % per, 0)),
                pl.BlockSpec((1, 1, rows, dim), lambda t, own: (t // per, own[0], t % per, 0)),
                pl.BlockSpec(memory_space=pl.ANY),
            ],
            out_specs=pl.BlockSpec((1, rows, dim), lambda t, _: (t // per, t % per, 0)),
            scratch_shapes=[pltpu.VMEM((qkvo.shape[0], qkvo.shape[1] - qkv_block, dim), jnp.bfloat16), pltpu.SemaphoreType.DMA],
        ),
        compiler_params=pltpu.CompilerParams(dimension_semantics=('arbitrary',), vmem_limit_bytes=56 * 1024 * 1024),
        cost_estimate=pl.CostEstimate(flops=2 * own_batch * seq_len * dim * depth, bytes_accessed=2 * dim * (depth + 3 * own_batch * seq_len), transcendentals=0),
        name='out_proj',
    )(row, attn, x_rows, qkvo)


def matmul_t(lhs, rhs_t):
    return lax.dot_general(lhs, rhs_t, (((lhs.ndim - 1,), (1,)), ((), ())), preferred_element_type=jnp.float32)


def solution(mesh):
    n_tpa = mesh.shape['tpa']
    n_tpb = mesh.shape['tpb']
    up_ring = [(i, (i + 1) % n_tpa) for i in range(n_tpa)]
    down_ring = [(i, (i - 1) % n_tpa) for i in range(n_tpa)]
    both = ('tpa', 'tpb')

    def layer_step(x_loc, len_loc, k_buf, v_buf, w_qkv, w_o, w_gate_up, w_down, g_attn, g_mlp):
        row = lax.axis_index('tpa')
        batch_loc, seq_len, model_dim = x_loc.shape
        head_dim = k_buf.shape[3]
        own_batch = batch_loc // n_tpa
        ff_block = w_gate_up.shape[1] // 2
        qkv_row = w_qkv.shape[1] * n_tpb
        o_row = w_o.shape[0] * n_tpb
        ff_row = ff_block * n_tpb

        qkv_block = w_qkv.shape[1]
        qkvo = lax.all_gather(jnp.concatenate([w_qkv.T, w_o], axis=0), both, axis=0, tiled=False)
        mlp_full = lax.all_gather(jnp.concatenate([w_gate_up.T.reshape(2, ff_block, model_dim), w_down[None]], axis=0), both, axis=1, tiled=True)
        row_arg = row.astype(jnp.int32)[None]
        cos_tab, sin_tab = rope_tables(seq_len, head_dim)
        x_rows = x_loc.reshape(own_batch, n_tpa, seq_len, model_dim)
        inv_all = inv_rms(x_loc)
        len_own = lax.dynamic_index_in_dim(len_loc.reshape(own_batch, n_tpa), row, 1, keepdims=False)

        qkv_act = qkv_proj(row_arg, x_rows, g_attn, qkvo, qkv_block, 2)
        attn_out = attention(qkv_act, len_own, cos_tab, sin_tab, n_tpa * k_buf.shape[2], head_dim)
        hidden = out_proj(row_arg, attn_out, x_rows, qkvo, qkv_block)

        hidden, x_late, qkvo_late = lax.optimization_barrier((hidden, x_loc, qkvo))
        kv_cols = k_buf.shape[2] * head_dim
        q_cols = qkv_row - 2 * kv_cols
        own_blocks = lax.dynamic_slice_in_dim(qkvo_late, row * n_tpb, n_tpb, 0)
        qkv_own = own_blocks[:, :qkv_block].reshape(qkv_row, model_dim)
        o_rows = own_blocks[:, qkv_block:].reshape(o_row, model_dim)
        w_query = qkv_own[:q_cols].T
        w_key = qkv_own[q_cols:q_cols + kv_cols].T
        w_value = qkv_own[q_cols + kv_cols:].T
        kv_new = matmul_t(scaled(x_late, inv_all, g_attn), qkv_own[q_cols:]).astype(jnp.bfloat16)
        half_dim = head_dim // 2
        k_first = kv_new[..., :half_dim].astype(jnp.float32)
        k_second = kv_new[..., half_dim:head_dim].astype(jnp.float32)
        k_rot = jnp.concatenate([k_first * cos_tab - k_second * sin_tab, k_second * cos_tab + k_first * sin_tab], axis=-1).astype(jnp.bfloat16)
        valid_pos = (jnp.arange(seq_len)[None, :] < len_loc[:, None])[:, :, None, None]
        k_cache = jnp.where(valid_pos, k_rot[:, :, None, :], k_buf)
        v_cache = jnp.where(valid_pos, kv_new[:, :, None, head_dim:], v_buf)
        cache_outs = (k_cache, v_cache, w_query, w_key, w_value, o_rows)
        mlp_full, cache_outs = lax.optimization_barrier((mlp_full, cache_outs))
        k_cache, v_cache, w_query, w_key, w_value, o_rows = cache_outs

        y_all = empty((own_batch, n_tpa, seq_len, model_dim), jnp.bfloat16)

        def put(y_buf, piece, slot, owner, start):
            return lax.dynamic_update_slice(y_buf, piece[None, None], (slot, lax.rem(owner + n_tpa, n_tpa), start, 0))

        spots = []
        for slot in range(own_batch):
            start = 0
            for share in FIRST_SPLIT if slot == 0 else LATER_SPLIT:
                spots.append((slot, start, seq_len // share))
                start += seq_len // share
        fars = []
        near = []
        upward = [0, 0]
        for slot, start, rows in spots:
            y_all, part = mlp(row_arg, hidden, g_mlp, mlp_full, y_all, slot, start, rows)
            near.append((lax.ppermute(part, 'tpa', up_ring), lax.ppermute(part, 'tpa', down_ring)))

        y_all, mlp_late = lax.optimization_barrier((y_all, mlp_full))
        mlp_own = lax.dynamic_slice_in_dim(mlp_late, row * ff_row, ff_row, 1)
        w_gate = mlp_own[0].T
        w_up = mlp_own[1].T
        down_rows = mlp_own[2]
        near[-1], (w_gate, w_up, down_rows) = lax.optimization_barrier((near[-1], (w_gate, w_up, down_rows)))
        for (from_below, from_above), (slot, start, rows) in zip(near, spots):
            if upward[0] <= upward[1]:
                upward[0] += rows
                far = lax.ppermute(from_below, 'tpa', up_ring)
            else:
                upward[1] += rows
                far = lax.ppermute(from_above, 'tpa', down_ring)
            y_all = put(y_all, from_below, slot, row - 1, start)
            y_all = put(y_all, from_above, slot, row + 1, start)
            fars.append(far)
        for far, (slot, start, rows) in zip(fars, spots):
            y_all = put(y_all, far, slot, row - 2, start)
        layer_out = y_all.reshape(batch_loc, seq_len, model_dim)
        return (layer_out, k_cache, v_cache, w_query, w_key, w_value, o_rows, w_gate, w_up, down_rows)

    batch_spec = P(('part', 'tpb'), None, None)
    len_spec = P(('part', 'tpb'))
    cache_spec = P(('part', 'tpb'), None, 'tpa', None)
    train_cols = P('part', ('tpa', 'tpb'))
    train_rows = P(('part', 'tpa', 'tpb'), None)
    gain_spec = P('part')
    gen_cols = P('part', 'tpa')
    gen_rows = P(('part', 'tpa'), None)
    return jax.shard_map(layer_step, mesh=mesh, in_specs=(batch_spec, len_spec, cache_spec, cache_spec, train_cols, train_rows, train_cols, train_rows, gain_spec, gain_spec), out_specs=(batch_spec, cache_spec, cache_spec, gen_cols, gen_cols, gen_cols, gen_rows, gen_cols, gen_cols, gen_rows), check_vma=False)
```

```python
import functools
import math
import jax
import jax.numpy as jnp
from jax import lax
from jax.experimental import pallas as pl
from jax.experimental.pallas import tpu as pltpu
from jax.sharding import PartitionSpec as P

ROPE_BASE = 500000.0
ROPE_FACTOR = 8.0
LOW_FREQ = 1.0
HIGH_FREQ = 4.0
ORIG_CONTEXT = 8192.0
NORM_EPS = 1e-5
MASK_VALUE = -1e30
Q_TILE = 256
FF_TILE = 512
OUT_TILE = 512
NT_DIMS = (((1,), (1,)), ((), ()))
FIRST_SPLIT = (4, 4, 2)
LATER_SPLIT = (2, 4, 4)


def inv_rms(x_in):
    x_wide = x_in.astype(jnp.float32)
    return lax.rsqrt(jnp.mean(x_wide * x_wide, axis=-1, keepdims=True) + NORM_EPS)


def scaled(x_in, inv_scale, gain_vec):
    return (x_in.astype(jnp.float32) * inv_scale * gain_vec.astype(jnp.float32)).astype(jnp.bfloat16)


def rope_tables(seq_len, head_dim):
    exponent = jnp.arange(head_dim // 2, dtype=jnp.float32) * (2.0 / head_dim)
    inv_freq = 1.0 / jnp.power(ROPE_BASE, exponent)
    wavelen = 2.0 * math.pi / inv_freq
    smooth = (ORIG_CONTEXT / wavelen - LOW_FREQ) / (HIGH_FREQ - LOW_FREQ)
    blended = (1.0 - smooth) * inv_freq / ROPE_FACTOR + smooth * inv_freq
    rope_freq = jnp.where(wavelen < ORIG_CONTEXT / HIGH_FREQ, inv_freq, jnp.where(wavelen > ORIG_CONTEXT / LOW_FREQ, inv_freq / ROPE_FACTOR, blended))
    angles = jnp.arange(seq_len, dtype=jnp.float32)[:, None] * rope_freq[None, :]
    return jnp.cos(angles), jnp.sin(angles)


def attention_kernel(head_dim, group_size, len_ref, qkv_ref, cos_ref, sin_ref, out_ref, kl_scr, kr_scr, vl_scr, vr_scr):
    seq_len = qkv_ref.shape[1]
    pair = 2 * head_dim
    length = len_ref[pl.program_id(0)]
    lane = lax.broadcasted_iota(jnp.int32, (1, pair), 1)
    low_lane = lane < head_dim
    first_half = lax.rem(lane, head_dim) < head_dim // 2
    one_low = jnp.where(lane == 0, 1.0, 0.0)
    one_high = jnp.where(lane == head_dim, 1.0, 0.0)

    def rope(vec, rows):
        ahead = pltpu.roll(vec, pair - head_dim // 2, 1)
        behind = pltpu.roll(vec, head_dim // 2, 1)
        return vec * cos_ref[rows, :] + jnp.where(first_half, ahead, behind) * sin_ref[rows, :]

    q_cols = group_size * head_dim
    for start in range(0, seq_len, Q_TILE):
        rows = pl.ds(start, Q_TILE)
        kv = qkv_ref[0, rows, q_cols:q_cols + pair].astype(jnp.float32)
        k_rot = rope(kv, rows)
        key_id = start + lax.broadcasted_iota(jnp.int32, (Q_TILE, pair), 0)
        bias = jnp.where(key_id < length, 0.0, MASK_VALUE)
        kl_scr[rows, :] = jnp.where(low_lane, k_rot, bias * one_high).astype(jnp.bfloat16)
        kr_scr[rows, :] = jnp.where(low_lane, bias * one_low, pltpu.roll(k_rot, head_dim, 1)).astype(jnp.bfloat16)
        vl_scr[rows, :] = jnp.where(low_lane, pltpu.roll(kv, head_dim, 1), 0.0).astype(jnp.bfloat16)
        vr_scr[rows, :] = jnp.where(low_lane, 0.0, kv).astype(jnp.bfloat16)

    for start in range(0, seq_len, Q_TILE):
        rows = pl.ds(start, Q_TILE)
        keys = start + Q_TILE
        causal = lax.broadcasted_iota(jnp.int32, (Q_TILE, Q_TILE), 1) <= lax.broadcasted_iota(jnp.int32, (Q_TILE, Q_TILE), 0)

        def weights(query, k_scr):
            scores = lax.dot_general(query, k_scr[:keys, :], (((1,), (1,)), ((), ())), preferred_element_type=jnp.float32)
            parts = [scores[:, block:block + Q_TILE] for block in range(0, keys, Q_TILE)]
            parts[-1] = jnp.where(causal, parts[-1], MASK_VALUE)
            top = parts[0]
            for part in parts[1:]:
                top = jnp.maximum(top, part)
            top = jnp.max(top, axis=1, keepdims=True)
            parts = [jnp.exp(part - top) for part in parts]
            total = parts[0]
            for part in parts[1:]:
                total = total + part
            scale = 1.0 / jnp.sum(total, axis=1, keepdims=True)
            return jnp.concatenate([(part * scale).astype(jnp.bfloat16) for part in parts], axis=1)

        def head_pair(index, carry):
            cols = pl.ds(pl.multiple_of(index * pair, pair), pair)
            query = rope(qkv_ref[0, rows, cols].astype(jnp.float32), rows).astype(jnp.bfloat16).astype(jnp.float32) * head_dim ** -0.5
            left = weights(jnp.where(low_lane, query, one_high).astype(jnp.bfloat16), kl_scr)
            right = weights(jnp.where(low_lane, one_low, query).astype(jnp.bfloat16), kr_scr)
            acc = jnp.dot(left, vl_scr[:keys, :], preferred_element_type=jnp.float32)
            acc = acc + jnp.dot(right, vr_scr[:keys, :], preferred_element_type=jnp.float32)
            out_ref[0, rows, cols] = acc.astype(jnp.bfloat16)
            return carry

        lax.fori_loop(0, group_size // 2, head_pair, 0, unroll=2)


def attention(qkv_act, lengths, cos_tab, sin_tab, kv_heads, head_dim):
    batch, seq_len, qkv_cols = qkv_act.shape
    group_cols = qkv_cols // kv_heads
    group_size = group_cols // head_dim - 2
    out_cols = group_size * head_dim
    pair = 2 * head_dim
    cos_pair = jnp.tile(cos_tab, (1, 4))
    sin_pair = jnp.tile(jnp.concatenate([-sin_tab, sin_tab], axis=1), (1, 2))
    flops = 2 * 2 * batch * kv_heads * group_size * seq_len * seq_len * head_dim
    return pl.pallas_call(
        functools.partial(attention_kernel, head_dim, group_size),
        out_shape=jax.ShapeDtypeStruct((batch, seq_len, kv_heads * out_cols), jnp.bfloat16),
        grid_spec=pltpu.PrefetchScalarGridSpec(
            num_scalar_prefetch=1,
            grid=(batch, kv_heads),
            in_specs=[
                pl.BlockSpec((1, seq_len, group_cols), lambda b, g, _: (b, 0, g)),
                pl.BlockSpec((seq_len, pair), lambda b, g, _: (0, 0)),
                pl.BlockSpec((seq_len, pair), lambda b, g, _: (0, 0)),
            ],
            out_specs=pl.BlockSpec((1, seq_len, out_cols), lambda b, g, _: (b, 0, g)),
            scratch_shapes=[pltpu.VMEM((seq_len, pair), jnp.bfloat16)] * 4,
        ),
        compiler_params=pltpu.CompilerParams(dimension_semantics=('arbitrary', 'arbitrary'), vmem_limit_bytes=48 * 1024 * 1024),
        cost_estimate=pl.CostEstimate(flops=4 * flops, bytes_accessed=2 * batch * seq_len * (qkv_cols + kv_heads * out_cols), transcendentals=batch * kv_heads * group_size * seq_len * seq_len),
        name='prefill_attention',
    )(lengths, qkv_act, cos_pair, sin_pair)


def empty(shape, dtype):
    return pl.pallas_call(lambda out_ref: None, out_shape=jax.ShapeDtypeStruct(shape, dtype), out_specs=pl.BlockSpec(memory_space=pl.ANY), name='output_buffer')()


def normalise(src, gain, dst, rows):
    def step(index, carry):
        part = pl.ds(pl.multiple_of(index * 64, 64), 64)
        wide = src[part, :].astype(jnp.float32)
        mean_sq = jnp.mean(wide * wide, axis=1, keepdims=True)
        dst[part, :] = (wide * lax.rsqrt(mean_sq + NORM_EPS) * gain).astype(jnp.bfloat16)
        return carry

    lax.fori_loop(0, rows // 64, step, 0)


def gate_up_kernel(slot, start, h_ref, gain_ref, w_ref, mid_ref, h_scr, u_scr, act_scr, mid_scr, w_buf, w_sem, h_sem, out_sem):
    rows, _ = h_scr.shape
    depth, _, tile, _ = w_buf.shape
    steps = w_ref.shape[1] // tile

    def w_copy(step):
        return pltpu.make_async_copy(w_ref.at[:, pl.ds(pl.multiple_of(step * tile, tile), tile), :], w_buf.at[lax.rem(step, depth)], w_sem.at[lax.rem(step, depth)])

    def out_copy(step):
        return pltpu.make_async_copy(mid_scr.at[lax.rem(step, 2)], mid_ref.at[:, pl.ds(pl.multiple_of(step * tile, tile), tile)], out_sem.at[lax.rem(step, 2)])

    h_copy = pltpu.make_async_copy(h_ref.at[slot, pl.ds(start, rows), :], h_scr, h_sem)
    h_copy.start()
    for step in range(min(depth - 1, steps)):
        w_copy(step).start()
    h_copy.wait()
    normalise(h_scr, gain_ref[...].astype(jnp.float32), u_scr, rows)

    def finish(step):
        gate = act_scr[0].astype(jnp.float32)
        up = act_scr[1].astype(jnp.float32)
        mid_scr[lax.rem(step, 2)] = (jax.nn.silu(gate) * up).astype(jnp.bfloat16)

    def body(step, carry):
        @pl.when(step + depth - 1 < steps)
        def _():
            w_copy(step + depth - 1).start()

        @pl.when(step >= 3)
        def _():
            out_copy(step - 3).wait()

        w_copy(step).wait()
        index = lax.rem(step, depth)
        gate = lax.dot_general(u_scr[...], w_buf[index, 0], NT_DIMS, preferred_element_type=jnp.float32)
        up = lax.dot_general(u_scr[...], w_buf[index, 1], NT_DIMS, preferred_element_type=jnp.float32)
        finish(step + 1)
        act_scr[0] = gate.astype(jnp.bfloat16)
        act_scr[1] = up.astype(jnp.bfloat16)

        @pl.when(step >= 1)
        def _():
            out_copy(step - 1).start()

        return carry

    act_scr[...] = jnp.zeros_like(act_scr)
    lax.fori_loop(0, steps, body, 0)
    if steps >= 3:
        out_copy(steps - 3).wait()
    finish(steps - 1)
    out_copy(steps - 1).start()
    if steps >= 2:
        out_copy(steps - 2).wait()
    out_copy(steps - 1).wait()


def gate_up(hidden, gain, weights, slot, start, rows):
    dim = hidden.shape[2]
    ff = weights.shape[1]
    tile = min(FF_TILE, ff)
    depth = 3
    anywhere = pl.BlockSpec(memory_space=pl.ANY)
    return pl.pallas_call(
        functools.partial(gate_up_kernel, slot, start),
        out_shape=jax.ShapeDtypeStruct((rows, ff), jnp.bfloat16),
        in_specs=[anywhere, pl.BlockSpec(memory_space=pltpu.VMEM), anywhere],
        out_specs=anywhere,
        scratch_shapes=[
            pltpu.VMEM((rows, dim), jnp.bfloat16),
            pltpu.VMEM((rows, dim), jnp.bfloat16),
            pltpu.VMEM((2, rows, tile), jnp.bfloat16),
            pltpu.VMEM((2, rows, tile), jnp.bfloat16),
            pltpu.VMEM((depth, 2, tile, dim), jnp.bfloat16),
            pltpu.SemaphoreType.DMA((depth,)),
            pltpu.SemaphoreType.DMA,
            pltpu.SemaphoreType.DMA((2,)),
        ],
        compiler_params=pltpu.CompilerParams(vmem_limit_bytes=58 * 1024 * 1024),
        cost_estimate=pl.CostEstimate(flops=4 * rows * dim * ff, bytes_accessed=4 * dim * ff + 2 * rows * (dim + ff), transcendentals=rows * ff),
        name='gate_up',
    )(hidden, gain[None, :], weights)


def down_kernel(slot, start, first, row_ref, h_ref, mid_ref, w_ref, y_in, y_ref, part_ref, h_scr, mid_scr, acc_scr, w_buf, w_sem, in_sem, out_sem):
    rows, dim = h_scr.shape
    depth, tile, _ = w_buf.shape
    steps = w_ref.shape[0] // tile
    out_tile = min(OUT_TILE, dim)

    def w_copy(step):
        return pltpu.make_async_copy(w_ref.at[pl.ds(pl.multiple_of(step * tile, tile), tile), :], w_buf.at[lax.rem(step, depth)], w_sem.at[lax.rem(step, depth)])

    h_copy = pltpu.make_async_copy(h_ref.at[slot, pl.ds(start, rows), :], h_scr, in_sem.at[0])
    mid_copy = pltpu.make_async_copy(mid_ref.at[pl.ds(first, rows), :], mid_scr, in_sem.at[1])
    h_copy.start()
    mid_copy.start()
    for step in range(min(depth - 1, steps)):
        w_copy(step).start()
    h_copy.wait()

    def widen(index, carry):
        part = pl.ds(pl.multiple_of(index * 64, 64), 64)
        acc_scr[part, :] = h_scr[part, :].astype(jnp.float32)
        return carry

    lax.fori_loop(0, rows // 64, widen, 0)
    mid_copy.wait()

    def body(step, carry):
        @pl.when(step + depth - 1 < steps)
        def _():
            w_copy(step + depth - 1).start()

        w_copy(step).wait()
        index = lax.rem(step, depth)
        mid = mid_scr[:, pl.ds(pl.multiple_of(step * tile, tile), tile)]
        for col in range(0, dim, out_tile):
            cols = slice(col, col + out_tile)
            acc_scr[:, cols] += jnp.dot(mid, w_buf[index, :, cols], preferred_element_type=jnp.float32)
        return carry

    lax.fori_loop(0, steps, body, 0)

    def narrow(index, carry):
        part = pl.ds(pl.multiple_of(index * 64, 64), 64)
        h_scr[part, :] = acc_scr[part, :].astype(jnp.bfloat16)
        return carry

    lax.fori_loop(0, rows // 64, narrow, 0)
    part_out = pltpu.make_async_copy(h_scr, part_ref, out_sem.at[0])
    y_out = pltpu.make_async_copy(h_scr, y_ref.at[slot, row_ref[0], pl.ds(start, rows), :], out_sem.at[1])
    part_out.start()
    y_out.start()
    part_out.wait()
    y_out.wait()


def down_proj(row, hidden, mid, weights, y_all, slot, start, first, rows):
    dim = hidden.shape[2]
    ff = mid.shape[1]
    tile = min(FF_TILE, ff)
    depth = 4
    anywhere = pl.BlockSpec(memory_space=pl.ANY)
    return pl.pallas_call(
        functools.partial(down_kernel, slot, start, first),
        out_shape=(jax.ShapeDtypeStruct(y_all.shape, jnp.bfloat16), jax.ShapeDtypeStruct((rows, dim), jnp.bfloat16)),
        in_specs=[pl.BlockSpec(memory_space=pltpu.SMEM), anywhere, anywhere, anywhere, anywhere],
        out_specs=(anywhere, anywhere),
        scratch_shapes=[
            pltpu.VMEM((rows, dim), jnp.bfloat16),
            pltpu.VMEM((rows, ff), jnp.bfloat16),
            pltpu.VMEM((rows, dim), jnp.float32),
            pltpu.VMEM((depth, tile, dim), jnp.bfloat16),
            pltpu.SemaphoreType.DMA((depth,)),
            pltpu.SemaphoreType.DMA((2,)),
            pltpu.SemaphoreType.DMA((2,)),
        ],
        input_output_aliases={4: 0},
        compiler_params=pltpu.CompilerParams(vmem_limit_bytes=58 * 1024 * 1024),
        cost_estimate=pl.CostEstimate(flops=2 * rows * dim * ff, bytes_accessed=2 * dim * ff + 2 * rows * (4 * dim + ff), transcendentals=0),
        name='down_proj',
    )(row, hidden, mid, weights, y_all)


def qkv_kernel(qkv_block, row_ref, x_ref, gain_ref, w_ref, out_ref, u_scr, w_scr):
    piece, tile = pl.program_id(0), pl.program_id(1)
    rows = x_ref.shape[2]

    @pl.when(tile == 0)
    def _():
        for block in range(w_ref.shape[0]):
            w_scr[block * qkv_block:(block + 1) * qkv_block, :] = w_ref[block, :qkv_block, :]

    @pl.when(piece == 0)
    def _():
        normalise(x_ref.at[0, 0], gain_ref[...].astype(jnp.float32), u_scr.at[tile], rows)

    out_ref[0] = lax.dot_general(u_scr[tile], w_scr[...], NT_DIMS, preferred_element_type=jnp.float32).astype(jnp.bfloat16)


def qkv_proj(row, x_rows, gain, qkvo, qkv_block, pieces):
    own_batch, _, seq_len, dim = x_rows.shape
    blocks = qkvo.shape[0] // pieces
    rows = min(512, seq_len)
    per = seq_len // rows
    tiles = own_batch * per
    cols = blocks * qkv_block

    def x_index(piece, tile, own):
        at = jnp.where(piece == 0, tile, tiles - 1)
        return (at // per, own[0], at % per, 0)

    return pl.pallas_call(
        functools.partial(qkv_kernel, qkv_block),
        out_shape=jax.ShapeDtypeStruct((own_batch, seq_len, pieces * cols), jnp.bfloat16),
        grid_spec=pltpu.PrefetchScalarGridSpec(
            num_scalar_prefetch=1,
            grid=(pieces, tiles),
            in_specs=[
                pl.BlockSpec((1, 1, rows, dim), x_index),
                pl.BlockSpec((1, dim), lambda p, t, _: (0, 0)),
                pl.BlockSpec((blocks,) + qkvo.shape[1:], lambda p, t, _: (p, 0, 0)),
            ],
            out_specs=pl.BlockSpec((1, rows, cols), lambda p, t, _: (t // per, t % per, p)),
            scratch_shapes=[pltpu.VMEM((tiles, rows, dim), jnp.bfloat16), pltpu.VMEM((cols, dim), jnp.bfloat16)],
        ),
        compiler_params=pltpu.CompilerParams(dimension_semantics=('arbitrary', 'arbitrary'), vmem_limit_bytes=60 * 1024 * 1024),
        cost_estimate=pl.CostEstimate(flops=2 * own_batch * seq_len * dim * pieces * cols, bytes_accessed=2 * dim * (pieces * cols + 2 * own_batch * seq_len), transcendentals=0),
        name='qkv_proj',
    )(row, x_rows, gain[None, :], qkvo)


def out_kernel(qkv_block, row_ref, a_ref, x_ref, w_ref, h_ref, w_scr, sem):
    @pl.when(pl.program_id(0) == 0)
    def _():
        copy = pltpu.make_async_copy(w_ref.at[:, pl.ds(qkv_block, w_scr.shape[1]), :], w_scr, sem)
        copy.start()
        copy.wait()

    dim = h_ref.shape[2]
    depth = w_scr.shape[0] * w_scr.shape[1]
    out_tile = min(OUT_TILE, dim)
    for col in range(0, dim, out_tile):
        cols = slice(col, col + out_tile)
        acc = jnp.dot(a_ref[0], w_scr[:, :, cols].reshape(depth, out_tile), preferred_element_type=jnp.float32)
        h_ref[0, :, cols] = (x_ref[0, 0, :, cols].astype(jnp.float32) + acc).astype(jnp.bfloat16)


def out_proj(row, attn, x_rows, qkvo, qkv_block):
    own_batch, seq_len, depth = attn.shape
    dim = x_rows.shape[3]
    rows = min(512, seq_len)
    per = seq_len // rows
    return pl.pallas_call(
        functools.partial(out_kernel, qkv_block),
        out_shape=jax.ShapeDtypeStruct((own_batch, seq_len, dim), jnp.bfloat16),
        grid_spec=pltpu.PrefetchScalarGridSpec(
            num_scalar_prefetch=1,
            grid=(own_batch * per,),
            in_specs=[
                pl.BlockSpec((1, rows, depth), lambda t, _: (t // per, t % per, 0)),
                pl.BlockSpec((1, 1, rows, dim), lambda t, own: (t // per, own[0], t % per, 0)),
                pl.BlockSpec(memory_space=pl.ANY),
            ],
            out_specs=pl.BlockSpec((1, rows, dim), lambda t, _: (t // per, t % per, 0)),
            scratch_shapes=[pltpu.VMEM((qkvo.shape[0], qkvo.shape[1] - qkv_block, dim), jnp.bfloat16), pltpu.SemaphoreType.DMA],
        ),
        compiler_params=pltpu.CompilerParams(dimension_semantics=('arbitrary',), vmem_limit_bytes=56 * 1024 * 1024),
        cost_estimate=pl.CostEstimate(flops=2 * own_batch * seq_len * dim * depth, bytes_accessed=2 * dim * (depth + 3 * own_batch * seq_len), transcendentals=0),
        name='out_proj',
    )(row, attn, x_rows, qkvo)


def matmul_t(lhs, rhs_t):
    return lax.dot_general(lhs, rhs_t, (((lhs.ndim - 1,), (1,)), ((), ())), preferred_element_type=jnp.float32)


def solution(mesh):
    n_tpa = mesh.shape['tpa']
    n_tpb = mesh.shape['tpb']
    up_ring = [(i, (i + 1) % n_tpa) for i in range(n_tpa)]
    down_ring = [(i, (i - 1) % n_tpa) for i in range(n_tpa)]
    both = ('tpa', 'tpb')

    def layer_step(x_loc, len_loc, k_buf, v_buf, w_qkv, w_o, w_gate_up, w_down, g_attn, g_mlp):
        row = lax.axis_index('tpa')
        batch_loc, seq_len, model_dim = x_loc.shape
        head_dim = k_buf.shape[3]
        own_batch = batch_loc // n_tpa
        ff_block = w_gate_up.shape[1] // 2
        qkv_row = w_qkv.shape[1] * n_tpb
        o_row = w_o.shape[0] * n_tpb
        ff_row = ff_block * n_tpb

        qkv_block = w_qkv.shape[1]
        qkvo = lax.all_gather(jnp.concatenate([w_qkv.T, w_o], axis=0), both, axis=0, tiled=False)
        gu_full = lax.all_gather(w_gate_up.T.reshape(2, ff_block, model_dim), both, axis=1, tiled=True)
        down_full = lax.all_gather(w_down, both, axis=0, tiled=True)
        row_arg = row.astype(jnp.int32)[None]
        cos_tab, sin_tab = rope_tables(seq_len, head_dim)
        x_rows = x_loc.reshape(own_batch, n_tpa, seq_len, model_dim)
        inv_all = inv_rms(x_loc)
        len_own = lax.dynamic_index_in_dim(len_loc.reshape(own_batch, n_tpa), row, 1, keepdims=False)

        qkv_act = qkv_proj(row_arg, x_rows, g_attn, qkvo, qkv_block, 2)
        attn_out = attention(qkv_act, len_own, cos_tab, sin_tab, n_tpa * k_buf.shape[2], head_dim)
        hidden = out_proj(row_arg, attn_out, x_rows, qkvo, qkv_block)

        y_all = empty((own_batch, n_tpa, seq_len, model_dim), jnp.bfloat16)

        def put(y_buf, piece, slot, owner, start):
            return lax.dynamic_update_slice(y_buf, piece[None, None], (slot, lax.rem(owner + n_tpa, n_tpa), start, 0))

        spots = []
        for slot in range(own_batch):
            start = 0
            for share in FIRST_SPLIT if slot == 0 else LATER_SPLIT:
                spots.append((slot, start, seq_len // share))
                start += seq_len // share
        mids = []
        fars = []
        near = []
        for slot, start, rows in spots:
            if start == 0:
                mids.append(gate_up(hidden, g_mlp, gu_full, slot, 0, seq_len))
            y_all, part = down_proj(row_arg, hidden, mids[slot], down_full, y_all, slot, start, start, rows)
            near.append((lax.ppermute(part, 'tpa', up_ring), lax.ppermute(part, 'tpa', down_ring)))

        y_all, x_late, qkvo_late, gu_late, down_late = lax.optimization_barrier((y_all, x_loc, qkvo, gu_full, down_full))
        kv_cols = k_buf.shape[2] * head_dim
        q_cols = qkv_row - 2 * kv_cols
        own_blocks = lax.dynamic_slice_in_dim(qkvo_late, row * n_tpb, n_tpb, 0)
        qkv_own = own_blocks[:, :qkv_block].reshape(qkv_row, model_dim)
        o_rows = own_blocks[:, qkv_block:].reshape(o_row, model_dim)
        w_query = qkv_own[:q_cols].T
        w_key = qkv_own[q_cols:q_cols + kv_cols].T
        w_value = qkv_own[q_cols + kv_cols:].T
        kv_new = matmul_t(scaled(x_late, inv_all, g_attn), qkv_own[q_cols:]).astype(jnp.bfloat16)
        half_dim = head_dim // 2
        k_first = kv_new[..., :half_dim].astype(jnp.float32)
        k_second = kv_new[..., half_dim:head_dim].astype(jnp.float32)
        k_rot = jnp.concatenate([k_first * cos_tab - k_second * sin_tab, k_second * cos_tab + k_first * sin_tab], axis=-1).astype(jnp.bfloat16)
        valid_pos = (jnp.arange(seq_len)[None, :] < len_loc[:, None])[:, :, None, None]
        k_cache = jnp.where(valid_pos, k_rot[:, :, None, :], k_buf)
        v_cache = jnp.where(valid_pos, kv_new[:, :, None, head_dim:], v_buf)
        gu_own = lax.dynamic_slice_in_dim(gu_late, row * ff_row, ff_row, 1)
        w_gate = gu_own[0].T
        w_up = gu_own[1].T
        down_rows = lax.dynamic_slice_in_dim(down_late, row * ff_row, ff_row, 0)
        cache_outs = (k_cache, v_cache, w_query, w_key, w_value, o_rows)
        near[-3], cache_outs = lax.optimization_barrier((near[-3], cache_outs))
        k_cache, v_cache, w_query, w_key, w_value, o_rows = cache_outs
        near[-2], (w_gate, w_up, down_rows) = lax.optimization_barrier((near[-2], (w_gate, w_up, down_rows)))
        for index, ((from_below, from_above), (slot, start, rows)) in enumerate(zip(near, spots)):
            if index % 2 == 0:
                far = lax.ppermute(from_below, 'tpa', up_ring)
            else:
                far = lax.ppermute(from_above, 'tpa', down_ring)
            y_all = put(y_all, from_below, slot, row - 1, start)
            y_all = put(y_all, from_above, slot, row + 1, start)
            fars.append(far)
        for far, (slot, start, rows) in zip(fars, spots):
            y_all = put(y_all, far, slot, row - 2, start)
        layer_out = y_all.reshape(batch_loc, seq_len, model_dim)
        return (layer_out, k_cache, v_cache, w_query, w_key, w_value, o_rows, w_gate, w_up, down_rows)

    batch_spec = P(('part', 'tpb'), None, None)
    len_spec = P(('part', 'tpb'))
    cache_spec = P(('part', 'tpb'), None, 'tpa', None)
    train_cols = P('part', ('tpa', 'tpb'))
    train_rows = P(('part', 'tpa', 'tpb'), None)
    gain_spec = P('part')
    gen_cols = P('part', 'tpa')
    gen_rows = P(('part', 'tpa'), None)
    return jax.shard_map(layer_step, mesh=mesh, in_specs=(batch_spec, len_spec, cache_spec, cache_spec, train_cols, train_rows, train_cols, train_rows, gain_spec, gain_spec), out_specs=(batch_spec, cache_spec, cache_spec, gen_cols, gen_cols, gen_cols, gen_rows, gen_cols, gen_cols, gen_rows), check_vma=False)
```

```python
import functools
import math
import jax
import jax.numpy as jnp
from jax import lax
from jax.experimental import pallas as pl
from jax.experimental.pallas import tpu as pltpu
from jax.sharding import PartitionSpec as P

ROPE_BASE = 500000.0
ROPE_FACTOR = 8.0
LOW_FREQ = 1.0
HIGH_FREQ = 4.0
ORIG_CONTEXT = 8192.0
NORM_EPS = 1e-5
MASK_VALUE = -1e30
Q_TILE = 256
SCORE_LIMIT = 64.0
FF_TILE = 512
OUT_TILE = 512
NT_DIMS = (((1,), (1,)), ((), ()))
FIRST_SPLIT = (4, 4, 2)
LATER_SPLIT = (2, 4, 4)


def inv_rms(x_in):
    x_wide = x_in.astype(jnp.float32)
    return lax.rsqrt(jnp.mean(x_wide * x_wide, axis=-1, keepdims=True) + NORM_EPS)


def scaled(x_in, inv_scale, gain_vec):
    return (x_in.astype(jnp.float32) * inv_scale * gain_vec.astype(jnp.float32)).astype(jnp.bfloat16)


def rope_tables(seq_len, head_dim):
    exponent = jnp.arange(head_dim // 2, dtype=jnp.float32) * (2.0 / head_dim)
    inv_freq = 1.0 / jnp.power(ROPE_BASE, exponent)
    wavelen = 2.0 * math.pi / inv_freq
    smooth = (ORIG_CONTEXT / wavelen - LOW_FREQ) / (HIGH_FREQ - LOW_FREQ)
    blended = (1.0 - smooth) * inv_freq / ROPE_FACTOR + smooth * inv_freq
    rope_freq = jnp.where(wavelen < ORIG_CONTEXT / HIGH_FREQ, inv_freq, jnp.where(wavelen > ORIG_CONTEXT / LOW_FREQ, inv_freq / ROPE_FACTOR, blended))
    angles = jnp.arange(seq_len, dtype=jnp.float32)[:, None] * rope_freq[None, :]
    return jnp.cos(angles), jnp.sin(angles)


def attention_kernel(head_dim, group_size, len_ref, qkv_ref, cos_ref, sin_ref, out_ref, kl_scr, kr_scr, vl_scr, vr_scr):
    seq_len = qkv_ref.shape[1]
    pair = 2 * head_dim
    length = len_ref[pl.program_id(0)]
    lane = lax.broadcasted_iota(jnp.int32, (1, pair), 1)
    low_lane = lane < head_dim
    first_half = lax.rem(lane, head_dim) < head_dim // 2
    one_low = jnp.where(lane == 0, 1.0, 0.0)
    one_high = jnp.where(lane == head_dim, 1.0, 0.0)

    def rope(vec, rows):
        ahead = pltpu.roll(vec, pair - head_dim // 2, 1)
        behind = pltpu.roll(vec, head_dim // 2, 1)
        return vec * cos_ref[rows, :] + jnp.where(first_half, ahead, behind) * sin_ref[rows, :]

    q_cols = group_size * head_dim
    q_top = jnp.zeros((Q_TILE, 1), jnp.float32)
    k_top = jnp.zeros((Q_TILE, 1), jnp.float32)
    for start in range(0, seq_len, Q_TILE):
        rows = pl.ds(start, Q_TILE)
        kv = qkv_ref[0, rows, q_cols:q_cols + pair].astype(jnp.float32)
        k_rot = rope(kv, rows)
        key_id = start + lax.broadcasted_iota(jnp.int32, (Q_TILE, pair), 0)
        bias = jnp.where(key_id < length, 0.0, MASK_VALUE)
        kl_scr[rows, :] = jnp.where(low_lane, k_rot, bias * one_high).astype(jnp.bfloat16)
        kr_scr[rows, :] = jnp.where(low_lane, bias * one_low, pltpu.roll(k_rot, head_dim, 1)).astype(jnp.bfloat16)
        vl_scr[rows, :] = jnp.where(low_lane, pltpu.roll(kv, head_dim, 1), 0.0).astype(jnp.bfloat16)
        vr_scr[rows, :] = jnp.where(low_lane, 0.0, kv).astype(jnp.bfloat16)
        k_top = jnp.maximum(k_top, jnp.sum(jnp.where(low_lane, k_rot * k_rot, 0.0), axis=1, keepdims=True))
        for col in range(0, q_cols, pair):
            query = qkv_ref[0, rows, col:col + pair].astype(jnp.float32)
            q_top = jnp.maximum(q_top, jnp.sum(query * query, axis=1, keepdims=True))
    small = jnp.max(q_top) * jnp.max(k_top) < head_dim * SCORE_LIMIT ** 2

    def attend(keep_top, unroll):
        for start in range(0, seq_len, Q_TILE):
            rows = pl.ds(start, Q_TILE)
            keys = start + Q_TILE
            causal = lax.broadcasted_iota(jnp.int32, (Q_TILE, Q_TILE), 1) <= lax.broadcasted_iota(jnp.int32, (Q_TILE, Q_TILE), 0)

            def weights(query, k_scr):
                scores = lax.dot_general(query, k_scr[:keys, :], NT_DIMS, preferred_element_type=jnp.float32)
                parts = [scores[:, block:block + Q_TILE] for block in range(0, keys, Q_TILE)]
                parts[-1] = jnp.where(causal, parts[-1], MASK_VALUE)
                if keep_top:
                    top = parts[0]
                    for part in parts[1:]:
                        top = jnp.maximum(top, part)
                    top = jnp.max(top, axis=1, keepdims=True)
                    parts = [part - top for part in parts]
                parts = [jnp.exp(part) for part in parts]
                total = parts[0]
                for part in parts[1:]:
                    total = total + part
                scale = 1.0 / jnp.sum(total, axis=1, keepdims=True)
                return jnp.concatenate([(part * scale).astype(jnp.bfloat16) for part in parts], axis=1)

            def head_pair(index, carry):
                cols = pl.ds(pl.multiple_of(index * pair, pair), pair)
                query = rope(qkv_ref[0, rows, cols].astype(jnp.float32), rows).astype(jnp.bfloat16).astype(jnp.float32) * head_dim ** -0.5
                left = weights(jnp.where(low_lane, query, one_high).astype(jnp.bfloat16), kl_scr)
                right = weights(jnp.where(low_lane, one_low, query).astype(jnp.bfloat16), kr_scr)
                acc = jnp.dot(left, vl_scr[:keys, :], preferred_element_type=jnp.float32)
                acc = acc + jnp.dot(right, vr_scr[:keys, :], preferred_element_type=jnp.float32)
                out_ref[0, rows, cols] = acc.astype(jnp.bfloat16)
                return carry

            lax.fori_loop(0, group_size // 2, head_pair, 0, unroll=unroll)

    @pl.when(small)
    def _():
        attend(False, 2)

    @pl.when(jnp.logical_not(small))
    def _():
        attend(True, 1)


def attention(qkv_act, lengths, cos_tab, sin_tab, kv_heads, head_dim):
    batch, seq_len, qkv_cols = qkv_act.shape
    group_cols = qkv_cols // kv_heads
    group_size = group_cols // head_dim - 2
    out_cols = group_size * head_dim
    pair = 2 * head_dim
    cos_pair = jnp.tile(cos_tab, (1, 4))
    sin_pair = jnp.tile(jnp.concatenate([-sin_tab, sin_tab], axis=1), (1, 2))
    flops = 2 * 2 * batch * kv_heads * group_size * seq_len * seq_len * head_dim
    return pl.pallas_call(
        functools.partial(attention_kernel, head_dim, group_size),
        out_shape=jax.ShapeDtypeStruct((batch, seq_len, kv_heads * out_cols), jnp.bfloat16),
        grid_spec=pltpu.PrefetchScalarGridSpec(
            num_scalar_prefetch=1,
            grid=(batch, kv_heads),
            in_specs=[
                pl.BlockSpec((1, seq_len, group_cols), lambda b, g, _: (b, 0, g)),
                pl.BlockSpec((seq_len, pair), lambda b, g, _: (0, 0)),
                pl.BlockSpec((seq_len, pair), lambda b, g, _: (0, 0)),
            ],
            out_specs=pl.BlockSpec((1, seq_len, out_cols), lambda b, g, _: (b, 0, g)),
            scratch_shapes=[pltpu.VMEM((seq_len, pair), jnp.bfloat16)] * 4,
        ),
        compiler_params=pltpu.CompilerParams(dimension_semantics=('arbitrary', 'arbitrary'), vmem_limit_bytes=48 * 1024 * 1024),
        cost_estimate=pl.CostEstimate(flops=4 * flops, bytes_accessed=2 * batch * seq_len * (qkv_cols + kv_heads * out_cols), transcendentals=batch * kv_heads * group_size * seq_len * seq_len),
        name='prefill_attention',
    )(lengths, qkv_act, cos_pair, sin_pair)


def empty(shape, dtype):
    return pl.pallas_call(lambda out_ref: None, out_shape=jax.ShapeDtypeStruct(shape, dtype), out_specs=pl.BlockSpec(memory_space=pl.ANY), name='output_buffer')()


def normalise(src, gain, dst, rows):
    def step(index, carry):
        part = pl.ds(pl.multiple_of(index * 64, 64), 64)
        wide = src[part, :].astype(jnp.float32)
        mean_sq = jnp.mean(wide * wide, axis=1, keepdims=True)
        dst[part, :] = (wide * lax.rsqrt(mean_sq + NORM_EPS) * gain).astype(jnp.bfloat16)
        return carry

    lax.fori_loop(0, rows // 64, step, 0)


def gate_up_kernel(slot, start, h_ref, gain_ref, w_ref, mid_ref, h_scr, u_scr, act_scr, mid_scr, w_buf, w_sem, h_sem, out_sem):
    rows, _ = h_scr.shape
    depth, _, tile, _ = w_buf.shape
    steps = w_ref.shape[1] // tile

    def w_copy(step):
        return pltpu.make_async_copy(w_ref.at[:, pl.ds(pl.multiple_of(step * tile, tile), tile), :], w_buf.at[lax.rem(step, depth)], w_sem.at[lax.rem(step, depth)])

    def out_copy(step):
        return pltpu.make_async_copy(mid_scr.at[lax.rem(step, 2)], mid_ref.at[:, pl.ds(pl.multiple_of(step * tile, tile), tile)], out_sem.at[lax.rem(step, 2)])

    h_copy = pltpu.make_async_copy(h_ref.at[slot, pl.ds(start, rows), :], h_scr, h_sem)
    h_copy.start()
    for step in range(min(depth - 1, steps)):
        w_copy(step).start()
    h_copy.wait()
    normalise(h_scr, gain_ref[...].astype(jnp.float32), u_scr, rows)

    def finish(step):
        gate = act_scr[0].astype(jnp.float32)
        up = act_scr[1].astype(jnp.float32)
        mid_scr[lax.rem(step, 2)] = (jax.nn.silu(gate) * up).astype(jnp.bfloat16)

    def body(step, carry):
        @pl.when(step + depth - 1 < steps)
        def _():
            w_copy(step + depth - 1).start()

        @pl.when(step >= 3)
        def _():
            out_copy(step - 3).wait()

        w_copy(step).wait()
        index = lax.rem(step, depth)
        gate = lax.dot_general(u_scr[...], w_buf[index, 0], NT_DIMS, preferred_element_type=jnp.float32)
        up = lax.dot_general(u_scr[...], w_buf[index, 1], NT_DIMS, preferred_element_type=jnp.float32)
        finish(step + 1)
        act_scr[0] = gate.astype(jnp.bfloat16)
        act_scr[1] = up.astype(jnp.bfloat16)

        @pl.when(step >= 1)
        def _():
            out_copy(step - 1).start()

        return carry

    act_scr[...] = jnp.zeros_like(act_scr)
    lax.fori_loop(0, steps, body, 0)
    if steps >= 3:
        out_copy(steps - 3).wait()
    finish(steps - 1)
    out_copy(steps - 1).start()
    if steps >= 2:
        out_copy(steps - 2).wait()
    out_copy(steps - 1).wait()


def gate_up(hidden, gain, weights, slot, start, rows):
    dim = hidden.shape[2]
    ff = weights.shape[1]
    tile = min(FF_TILE, ff)
    depth = 3
    anywhere = pl.BlockSpec(memory_space=pl.ANY)
    return pl.pallas_call(
        functools.partial(gate_up_kernel, slot, start),
        out_shape=jax.ShapeDtypeStruct((rows, ff), jnp.bfloat16),
        in_specs=[anywhere, pl.BlockSpec(memory_space=pltpu.VMEM), anywhere],
        out_specs=anywhere,
        scratch_shapes=[
            pltpu.VMEM((rows, dim), jnp.bfloat16),
            pltpu.VMEM((rows, dim), jnp.bfloat16),
            pltpu.VMEM((2, rows, tile), jnp.bfloat16),
            pltpu.VMEM((2, rows, tile), jnp.bfloat16),
            pltpu.VMEM((depth, 2, tile, dim), jnp.bfloat16),
            pltpu.SemaphoreType.DMA((depth,)),
            pltpu.SemaphoreType.DMA,
            pltpu.SemaphoreType.DMA((2,)),
        ],
        compiler_params=pltpu.CompilerParams(vmem_limit_bytes=58 * 1024 * 1024),
        cost_estimate=pl.CostEstimate(flops=4 * rows * dim * ff, bytes_accessed=4 * dim * ff + 2 * rows * (dim + ff), transcendentals=rows * ff),
        name='gate_up',
    )(hidden, gain[None, :], weights)


def down_kernel(slot, start, first, row_ref, h_ref, mid_ref, w_ref, y_in, y_ref, part_ref, h_scr, mid_scr, acc_scr, w_buf, w_sem, mid_sem, h_sem, out_sem):
    rows, dim = h_scr.shape
    depth, tile, _ = w_buf.shape
    steps = w_ref.shape[0] // tile
    out_tile = min(OUT_TILE, dim)

    def w_copy(step):
        return pltpu.make_async_copy(w_ref.at[pl.ds(pl.multiple_of(step * tile, tile), tile), :], w_buf.at[lax.rem(step, depth)], w_sem.at[lax.rem(step, depth)])

    def mid_copy(step):
        return pltpu.make_async_copy(mid_ref.at[pl.ds(first, rows), pl.ds(pl.multiple_of(step * tile, tile), tile)], mid_scr.at[lax.rem(step, depth)], mid_sem.at[lax.rem(step, depth)])

    h_copy = pltpu.make_async_copy(h_ref.at[slot, pl.ds(start, rows), :], h_scr, h_sem)
    h_copy.start()
    for step in range(min(depth - 1, steps)):
        w_copy(step).start()
        mid_copy(step).start()
    h_copy.wait()

    def widen(index, carry):
        part = pl.ds(pl.multiple_of(index * 64, 64), 64)
        acc_scr[part, :] = h_scr[part, :].astype(jnp.float32)
        return carry

    lax.fori_loop(0, rows // 64, widen, 0)

    def body(step, carry):
        @pl.when(step + depth - 1 < steps)
        def _():
            w_copy(step + depth - 1).start()
            mid_copy(step + depth - 1).start()

        w_copy(step).wait()
        mid_copy(step).wait()
        index = lax.rem(step, depth)
        mid = mid_scr[index]
        for col in range(0, dim, out_tile):
            cols = slice(col, col + out_tile)
            acc_scr[:, cols] += jnp.dot(mid, w_buf[index, :, cols], preferred_element_type=jnp.float32)
        return carry

    lax.fori_loop(0, steps, body, 0)

    def narrow(index, carry):
        part = pl.ds(pl.multiple_of(index * 64, 64), 64)
        h_scr[part, :] = acc_scr[part, :].astype(jnp.bfloat16)
        return carry

    lax.fori_loop(0, rows // 64, narrow, 0)
    part_out = pltpu.make_async_copy(h_scr, part_ref, out_sem.at[0])
    y_out = pltpu.make_async_copy(h_scr, y_ref.at[slot, row_ref[0], pl.ds(start, rows), :], out_sem.at[1])
    part_out.start()
    y_out.start()
    part_out.wait()
    y_out.wait()


def down_proj(row, hidden, mid, weights, y_all, slot, start, first, rows):
    dim = hidden.shape[2]
    ff = mid.shape[1]
    tile = min(FF_TILE, ff)
    depth = 4
    anywhere = pl.BlockSpec(memory_space=pl.ANY)
    return pl.pallas_call(
        functools.partial(down_kernel, slot, start, first),
        out_shape=(jax.ShapeDtypeStruct(y_all.shape, jnp.bfloat16), jax.ShapeDtypeStruct((rows, dim), jnp.bfloat16)),
        in_specs=[pl.BlockSpec(memory_space=pltpu.SMEM), anywhere, anywhere, anywhere, anywhere],
        out_specs=(anywhere, anywhere),
        scratch_shapes=[
            pltpu.VMEM((rows, dim), jnp.bfloat16),
            pltpu.VMEM((depth, rows, tile), jnp.bfloat16),
            pltpu.VMEM((rows, dim), jnp.float32),
            pltpu.VMEM((depth, tile, dim), jnp.bfloat16),
            pltpu.SemaphoreType.DMA((depth,)),
            pltpu.SemaphoreType.DMA((depth,)),
            pltpu.SemaphoreType.DMA,
            pltpu.SemaphoreType.DMA((2,)),
        ],
        input_output_aliases={4: 0},
        compiler_params=pltpu.CompilerParams(vmem_limit_bytes=58 * 1024 * 1024),
        cost_estimate=pl.CostEstimate(flops=2 * rows * dim * ff, bytes_accessed=2 * dim * ff + 2 * rows * (4 * dim + ff), transcendentals=0),
        name='down_proj',
    )(row, hidden, mid, weights, y_all)


def place_kernel(spots, n_rows, row_ref, y_in, *refs):
    pieces, (y_ref, buf, in_sem, out_sem) = refs[:len(spots)], refs[len(spots):]
    block = buf.shape[1]
    loads, stores = [], []
    for piece, (slot, offset, start, rows) in zip(pieces, spots):
        owner = lax.rem(row_ref[0] + offset, n_rows)
        for first in range(0, rows, block):
            at = len(loads)
            loads.append(pltpu.make_async_copy(piece.at[pl.ds(first, block), :], buf.at[at], in_sem.at[at]))
            stores.append(pltpu.make_async_copy(buf.at[at], y_ref.at[slot, owner, pl.ds(start + first, block), :], out_sem.at[at]))
    for load in loads:
        load.start()
    for load, store in zip(loads, stores):
        load.wait()
        store.start()
    for store in stores:
        store.wait()


def place(row, y_all, pieces):
    arrays = [piece for piece, _ in pieces]
    spots = [spot for _, spot in pieces]
    block = min(256, *(spot[3] for spot in spots))
    count = sum(spot[3] for spot in spots) // block
    dim = y_all.shape[3]
    anywhere = pl.BlockSpec(memory_space=pl.ANY)
    moved = 2 * dim * sum(spot[3] for spot in spots)
    return pl.pallas_call(
        functools.partial(place_kernel, spots, y_all.shape[1]),
        out_shape=jax.ShapeDtypeStruct(y_all.shape, y_all.dtype),
        in_specs=[pl.BlockSpec(memory_space=pltpu.SMEM)] + [anywhere] * (1 + len(arrays)),
        out_specs=anywhere,
        scratch_shapes=[pltpu.VMEM((count, block, dim), jnp.bfloat16), pltpu.SemaphoreType.DMA((count,)), pltpu.SemaphoreType.DMA((count,))],
        input_output_aliases={1: 0},
        compiler_params=pltpu.CompilerParams(vmem_limit_bytes=40 * 1024 * 1024),
        cost_estimate=pl.CostEstimate(flops=moved * 100, bytes_accessed=2 * moved, transcendentals=0),
        name='place_rows',
    )(row, y_all, *arrays)


def relayout_kernel(row_ref, gu_ref, d_ref, gate_ref, up_ref, down_ref):
    gate_ref[...] = jnp.transpose(gu_ref[0].astype(jnp.float32)).astype(jnp.bfloat16)
    up_ref[...] = jnp.transpose(gu_ref[1].astype(jnp.float32)).astype(jnp.bfloat16)
    down_ref[...] = d_ref[...]


def relayout(row, gu_full, down_full, n_rows):
    _, ff, dim = gu_full.shape
    own = ff // n_rows
    tile = min(128, own)
    steps = own // tile
    column = pl.BlockSpec((dim, tile), lambda j, _: (0, j))
    return pl.pallas_call(
        relayout_kernel,
        out_shape=(jax.ShapeDtypeStruct((dim, own), jnp.bfloat16), jax.ShapeDtypeStruct((dim, own), jnp.bfloat16), jax.ShapeDtypeStruct((own, dim), jnp.bfloat16)),
        grid_spec=pltpu.PrefetchScalarGridSpec(
            num_scalar_prefetch=1,
            grid=(steps,),
            in_specs=[
                pl.BlockSpec((2, tile, dim), lambda j, at: (0, at[0] * steps + j, 0)),
                pl.BlockSpec((tile, dim), lambda j, at: (at[0] * steps + j, 0)),
            ],
            out_specs=(column, column, pl.BlockSpec((tile, dim), lambda j, _: (j, 0))),
        ),
        compiler_params=pltpu.CompilerParams(dimension_semantics=('arbitrary',), vmem_limit_bytes=40 * 1024 * 1024),
        cost_estimate=pl.CostEstimate(flops=600 * own * dim, bytes_accessed=12 * own * dim, transcendentals=0),
        name='relayout',
    )(row, gu_full, down_full)


def qkv_kernel(qkv_block, row_ref, x_ref, gain_ref, w_ref, out_ref, u_scr, w_scr):
    piece, tile = pl.program_id(0), pl.program_id(1)
    rows = x_ref.shape[2]

    @pl.when(tile == 0)
    def _():
        for block in range(w_ref.shape[0]):
            w_scr[block * qkv_block:(block + 1) * qkv_block, :] = w_ref[block, :qkv_block, :]

    @pl.when(piece == 0)
    def _():
        normalise(x_ref.at[0, 0], gain_ref[...].astype(jnp.float32), u_scr.at[tile], rows)

    out_ref[0] = lax.dot_general(u_scr[tile], w_scr[...], NT_DIMS, preferred_element_type=jnp.float32).astype(jnp.bfloat16)


def qkv_proj(row, x_rows, gain, qkvo, qkv_block, pieces):
    own_batch, _, seq_len, dim = x_rows.shape
    blocks = qkvo.shape[0] // pieces
    rows = min(512, seq_len)
    per = seq_len // rows
    tiles = own_batch * per
    cols = blocks * qkv_block

    def x_index(piece, tile, own):
        at = jnp.where(piece == 0, tile, tiles - 1)
        return (at // per, own[0], at % per, 0)

    return pl.pallas_call(
        functools.partial(qkv_kernel, qkv_block),
        out_shape=jax.ShapeDtypeStruct((own_batch, seq_len, pieces * cols), jnp.bfloat16),
        grid_spec=pltpu.PrefetchScalarGridSpec(
            num_scalar_prefetch=1,
            grid=(pieces, tiles),
            in_specs=[
                pl.BlockSpec((1, 1, rows, dim), x_index),
                pl.BlockSpec((1, dim), lambda p, t, _: (0, 0)),
                pl.BlockSpec((blocks,) + qkvo.shape[1:], lambda p, t, _: (p, 0, 0)),
            ],
            out_specs=pl.BlockSpec((1, rows, cols), lambda p, t, _: (t // per, t % per, p)),
            scratch_shapes=[pltpu.VMEM((tiles, rows, dim), jnp.bfloat16), pltpu.VMEM((cols, dim), jnp.bfloat16)],
        ),
        compiler_params=pltpu.CompilerParams(dimension_semantics=('arbitrary', 'arbitrary'), vmem_limit_bytes=60 * 1024 * 1024),
        cost_estimate=pl.CostEstimate(flops=2 * own_batch * seq_len * dim * pieces * cols, bytes_accessed=2 * dim * (pieces * cols + 2 * own_batch * seq_len), transcendentals=0),
        name='qkv_proj',
    )(row, x_rows, gain[None, :], qkvo)


def out_kernel(qkv_block, row_ref, a_ref, x_ref, w_ref, h_ref, w_scr, sem):
    @pl.when(pl.program_id(0) == 0)
    def _():
        copy = pltpu.make_async_copy(w_ref.at[:, pl.ds(qkv_block, w_scr.shape[1]), :], w_scr, sem)
        copy.start()
        copy.wait()

    dim = h_ref.shape[2]
    depth = w_scr.shape[0] * w_scr.shape[1]
    out_tile = min(OUT_TILE, dim)
    for col in range(0, dim, out_tile):
        cols = slice(col, col + out_tile)
        acc = jnp.dot(a_ref[0], w_scr[:, :, cols].reshape(depth, out_tile), preferred_element_type=jnp.float32)
        h_ref[0, :, cols] = (x_ref[0, 0, :, cols].astype(jnp.float32) + acc).astype(jnp.bfloat16)


def out_proj(row, attn, x_rows, qkvo, qkv_block):
    own_batch, seq_len, depth = attn.shape
    dim = x_rows.shape[3]
    rows = min(512, seq_len)
    per = seq_len // rows
    return pl.pallas_call(
        functools.partial(out_kernel, qkv_block),
        out_shape=jax.ShapeDtypeStruct((own_batch, seq_len, dim), jnp.bfloat16),
        grid_spec=pltpu.PrefetchScalarGridSpec(
            num_scalar_prefetch=1,
            grid=(own_batch * per,),
            in_specs=[
                pl.BlockSpec((1, rows, depth), lambda t, _: (t // per, t % per, 0)),
                pl.BlockSpec((1, 1, rows, dim), lambda t, own: (t // per, own[0], t % per, 0)),
                pl.BlockSpec(memory_space=pl.ANY),
            ],
            out_specs=pl.BlockSpec((1, rows, dim), lambda t, _: (t // per, t % per, 0)),
            scratch_shapes=[pltpu.VMEM((qkvo.shape[0], qkvo.shape[1] - qkv_block, dim), jnp.bfloat16), pltpu.SemaphoreType.DMA],
        ),
        compiler_params=pltpu.CompilerParams(dimension_semantics=('arbitrary',), vmem_limit_bytes=56 * 1024 * 1024),
        cost_estimate=pl.CostEstimate(flops=2 * own_batch * seq_len * dim * depth, bytes_accessed=2 * dim * (depth + 3 * own_batch * seq_len), transcendentals=0),
        name='out_proj',
    )(row, attn, x_rows, qkvo)


def matmul_t(lhs, rhs_t):
    return lax.dot_general(lhs, rhs_t, (((lhs.ndim - 1,), (1,)), ((), ())), preferred_element_type=jnp.float32)


def solution(mesh):
    n_tpa = mesh.shape['tpa']
    n_tpb = mesh.shape['tpb']
    up_ring = [(i, (i + 1) % n_tpa) for i in range(n_tpa)]
    down_ring = [(i, (i - 1) % n_tpa) for i in range(n_tpa)]
    both = ('tpa', 'tpb')

    def layer_step(x_loc, len_loc, k_buf, v_buf, w_qkv, w_o, w_gate_up, w_down, g_attn, g_mlp):
        row = lax.axis_index('tpa')
        batch_loc, seq_len, model_dim = x_loc.shape
        head_dim = k_buf.shape[3]
        own_batch = batch_loc // n_tpa
        ff_block = w_gate_up.shape[1] // 2
        qkv_row = w_qkv.shape[1] * n_tpb
        o_row = w_o.shape[0] * n_tpb

        qkv_block = w_qkv.shape[1]
        qkvo = lax.all_gather(jnp.concatenate([w_qkv.T, w_o], axis=0), both, axis=0, tiled=False)
        gu_full = lax.all_gather(w_gate_up.T.reshape(2, ff_block, model_dim), both, axis=1, tiled=True)
        down_full = lax.all_gather(w_down, both, axis=0, tiled=True)
        row_arg = row.astype(jnp.int32)[None]
        cos_tab, sin_tab = rope_tables(seq_len, head_dim)
        x_rows = x_loc.reshape(own_batch, n_tpa, seq_len, model_dim)
        inv_all = inv_rms(x_loc)
        len_own = lax.dynamic_index_in_dim(len_loc.reshape(own_batch, n_tpa), row, 1, keepdims=False)

        qkv_act = qkv_proj(row_arg, x_rows, g_attn, qkvo, qkv_block, 2)
        attn_out = attention(qkv_act, len_own, cos_tab, sin_tab, n_tpa * k_buf.shape[2], head_dim)
        hidden = out_proj(row_arg, attn_out, x_rows, qkvo, qkv_block)

        y_all = empty((own_batch, n_tpa, seq_len, model_dim), jnp.bfloat16)

        spots = []
        for slot in range(own_batch):
            start = 0
            for share in FIRST_SPLIT if slot == 0 else LATER_SPLIT:
                spots.append((slot, start, seq_len // share))
                start += seq_len // share
        mids = []
        fars = []
        near = []
        for slot, start, rows in spots:
            if start == 0:
                mids.append(gate_up(hidden, g_mlp, gu_full, slot, 0, seq_len))
            y_all, part = down_proj(row_arg, hidden, mids[slot], down_full, y_all, slot, start, start, rows)
            near.append((lax.ppermute(part, 'tpa', up_ring), lax.ppermute(part, 'tpa', down_ring)))

        y_all, x_late, qkvo_late, gu_late, down_late = lax.optimization_barrier((y_all, x_loc, qkvo, gu_full, down_full))
        kv_cols = k_buf.shape[2] * head_dim
        q_cols = qkv_row - 2 * kv_cols
        own_blocks = lax.dynamic_slice_in_dim(qkvo_late, row * n_tpb, n_tpb, 0)
        qkv_own = own_blocks[:, :qkv_block].reshape(qkv_row, model_dim)
        o_rows = own_blocks[:, qkv_block:].reshape(o_row, model_dim)
        w_query = qkv_own[:q_cols].T
        w_key = qkv_own[q_cols:q_cols + kv_cols].T
        w_value = qkv_own[q_cols + kv_cols:].T
        kv_new = matmul_t(scaled(x_late, inv_all, g_attn), qkv_own[q_cols:]).astype(jnp.bfloat16)
        half_dim = head_dim // 2
        k_first = kv_new[..., :half_dim].astype(jnp.float32)
        k_second = kv_new[..., half_dim:head_dim].astype(jnp.float32)
        k_rot = jnp.concatenate([k_first * cos_tab - k_second * sin_tab, k_second * cos_tab + k_first * sin_tab], axis=-1).astype(jnp.bfloat16)
        valid_pos = (jnp.arange(seq_len)[None, :] < len_loc[:, None])[:, :, None, None]
        k_cache = jnp.where(valid_pos, k_rot[:, :, None, :], k_buf)
        v_cache = jnp.where(valid_pos, kv_new[:, :, None, head_dim:], v_buf)
        w_gate, w_up, down_rows = relayout(row_arg, gu_late, down_late, n_tpa)
        cache_outs = (k_cache, v_cache, w_query, w_key, w_value, o_rows)
        near[-3], cache_outs = lax.optimization_barrier((near[-3], cache_outs))
        k_cache, v_cache, w_query, w_key, w_value, o_rows = cache_outs
        near[-2], (w_gate, w_up, down_rows) = lax.optimization_barrier((near[-2], (w_gate, w_up, down_rows)))
        for index, ((from_below, from_above), (slot, start, rows)) in enumerate(zip(near, spots)):
            if index % 2 == 0:
                far = lax.ppermute(from_below, 'tpa', up_ring)
            else:
                far = lax.ppermute(from_above, 'tpa', down_ring)
            fars.append(far)

        def near_pieces(first, last):
            for (from_below, from_above), (slot, start, rows) in list(zip(near, spots))[first:last]:
                yield from_below, (slot, n_tpa - 1, start, rows)
                yield from_above, (slot, 1, start, rows)

        def far_pieces(first, last):
            for far, (slot, start, rows) in list(zip(fars, spots))[first:last]:
                yield far, (slot, n_tpa - 2, start, rows)

        n_first = len(FIRST_SPLIT)
        y_all = place(row_arg, y_all, [*near_pieces(0, n_first), *far_pieces(0, 2)])
        y_all = place(row_arg, y_all, [*near_pieces(n_first, len(spots)), *far_pieces(2, n_first)])
        for index in range(n_first, len(spots)):
            y_all = place(row_arg, y_all, [*far_pieces(index, index + 1)])
        layer_out = y_all.reshape(batch_loc, seq_len, model_dim)
        return (layer_out, k_cache, v_cache, w_query, w_key, w_value, o_rows, w_gate, w_up, down_rows)

    batch_spec = P(('part', 'tpb'), None, None)
    len_spec = P(('part', 'tpb'))
    cache_spec = P(('part', 'tpb'), None, 'tpa', None)
    train_cols = P('part', ('tpa', 'tpb'))
    train_rows = P(('part', 'tpa', 'tpb'), None)
    gain_spec = P('part')
    gen_cols = P('part', 'tpa')
    gen_rows = P(('part', 'tpa'), None)
    return jax.shard_map(layer_step, mesh=mesh, in_specs=(batch_spec, len_spec, cache_spec, cache_spec, train_cols, train_rows, train_cols, train_rows, gain_spec, gain_spec), out_specs=(batch_spec, cache_spec, cache_spec, gen_cols, gen_cols, gen_cols, gen_rows, gen_cols, gen_cols, gen_rows), check_vma=False)
```

```python
import functools
import math
import jax
import jax.numpy as jnp
from jax import lax
from jax.experimental import pallas as pl
from jax.experimental.pallas import tpu as pltpu
from jax.sharding import PartitionSpec as P

ROPE_BASE = 500000.0
ROPE_FACTOR = 8.0
LOW_FREQ = 1.0
HIGH_FREQ = 4.0
ORIG_CONTEXT = 8192.0
NORM_EPS = 1e-5
MASK_VALUE = -1e30
Q_TILE = 256
SCORE_LIMIT = 64.0
FF_TILE = 512
OUT_TILE = 512
NT_DIMS = (((1,), (1,)), ((), ()))
MESH = pl.DeviceIdType.MESH
GATES_PER_PROMPT = 2


def rope_tables(seq_len, head_dim):
    exponent = jnp.arange(head_dim // 2, dtype=jnp.float32) * (2.0 / head_dim)
    inv_freq = 1.0 / jnp.power(ROPE_BASE, exponent)
    wavelen = 2.0 * math.pi / inv_freq
    smooth = (ORIG_CONTEXT / wavelen - LOW_FREQ) / (HIGH_FREQ - LOW_FREQ)
    blended = (1.0 - smooth) * inv_freq / ROPE_FACTOR + smooth * inv_freq
    rope_freq = jnp.where(wavelen < ORIG_CONTEXT / HIGH_FREQ, inv_freq, jnp.where(wavelen > ORIG_CONTEXT / LOW_FREQ, inv_freq / ROPE_FACTOR, blended))
    angles = jnp.arange(seq_len, dtype=jnp.float32)[:, None] * rope_freq[None, :]
    return jnp.cos(angles), jnp.sin(angles)


def attention_kernel(head_dim, group_size, len_ref, qkv_ref, cos_ref, sin_ref, out_ref, kl_scr, kr_scr, vl_scr, vr_scr):
    seq_len = qkv_ref.shape[1]
    pair = 2 * head_dim
    length = len_ref[pl.program_id(0)]
    lane = lax.broadcasted_iota(jnp.int32, (1, pair), 1)
    low_lane = lane < head_dim
    first_half = lax.rem(lane, head_dim) < head_dim // 2
    one_low = jnp.where(lane == 0, 1.0, 0.0)
    one_high = jnp.where(lane == head_dim, 1.0, 0.0)

    def rope(vec, rows):
        ahead = pltpu.roll(vec, pair - head_dim // 2, 1)
        behind = pltpu.roll(vec, head_dim // 2, 1)
        return vec * cos_ref[rows, :] + jnp.where(first_half, ahead, behind) * sin_ref[rows, :]

    q_cols = group_size * head_dim
    q_top = jnp.zeros((Q_TILE, 1), jnp.float32)
    k_top = jnp.zeros((Q_TILE, 1), jnp.float32)
    for start in range(0, seq_len, Q_TILE):
        rows = pl.ds(start, Q_TILE)
        kv = qkv_ref[0, rows, q_cols:q_cols + pair].astype(jnp.float32)
        k_rot = rope(kv, rows)
        key_id = start + lax.broadcasted_iota(jnp.int32, (Q_TILE, pair), 0)
        bias = jnp.where(key_id < length, 0.0, MASK_VALUE)
        kl_scr[rows, :] = jnp.where(low_lane, k_rot, bias * one_high).astype(jnp.bfloat16)
        kr_scr[rows, :] = jnp.where(low_lane, bias * one_low, pltpu.roll(k_rot, head_dim, 1)).astype(jnp.bfloat16)
        vl_scr[rows, :] = jnp.where(low_lane, pltpu.roll(kv, head_dim, 1), 0.0).astype(jnp.bfloat16)
        vr_scr[rows, :] = jnp.where(low_lane, 0.0, kv).astype(jnp.bfloat16)
        k_top = jnp.maximum(k_top, jnp.sum(jnp.where(low_lane, k_rot * k_rot, 0.0), axis=1, keepdims=True))
        for col in range(0, q_cols, pair):
            query = qkv_ref[0, rows, col:col + pair].astype(jnp.float32)
            q_top = jnp.maximum(q_top, jnp.sum(query * query, axis=1, keepdims=True))
    small = jnp.max(q_top) * jnp.max(k_top) < head_dim * SCORE_LIMIT ** 2

    def attend(keep_top, unroll):
        for start in range(0, seq_len, Q_TILE):
            rows = pl.ds(start, Q_TILE)
            keys = start + Q_TILE
            causal = lax.broadcasted_iota(jnp.int32, (Q_TILE, Q_TILE), 1) <= lax.broadcasted_iota(jnp.int32, (Q_TILE, Q_TILE), 0)

            def weights(query, k_scr):
                scores = lax.dot_general(query, k_scr[:keys, :], NT_DIMS, preferred_element_type=jnp.float32)
                parts = [scores[:, block:block + Q_TILE] for block in range(0, keys, Q_TILE)]
                parts[-1] = jnp.where(causal, parts[-1], MASK_VALUE)
                if keep_top:
                    top = parts[0]
                    for part in parts[1:]:
                        top = jnp.maximum(top, part)
                    top = jnp.max(top, axis=1, keepdims=True)
                    parts = [part - top for part in parts]
                parts = [jnp.exp(part) for part in parts]
                total = parts[0]
                for part in parts[1:]:
                    total = total + part
                scale = 1.0 / jnp.sum(total, axis=1, keepdims=True)
                return jnp.concatenate([(part * scale).astype(jnp.bfloat16) for part in parts], axis=1)

            def head_pair(index, carry):
                cols = pl.ds(pl.multiple_of(index * pair, pair), pair)
                query = rope(qkv_ref[0, rows, cols].astype(jnp.float32), rows).astype(jnp.bfloat16).astype(jnp.float32) * head_dim ** -0.5
                left = weights(jnp.where(low_lane, query, one_high).astype(jnp.bfloat16), kl_scr)
                right = weights(jnp.where(low_lane, one_low, query).astype(jnp.bfloat16), kr_scr)
                acc = jnp.dot(left, vl_scr[:keys, :], preferred_element_type=jnp.float32)
                acc = acc + jnp.dot(right, vr_scr[:keys, :], preferred_element_type=jnp.float32)
                out_ref[0, rows, cols] = acc.astype(jnp.bfloat16)
                return carry

            lax.fori_loop(0, group_size // 2, head_pair, 0, unroll=unroll)

    @pl.when(small)
    def _():
        attend(False, 2)

    @pl.when(jnp.logical_not(small))
    def _():
        attend(True, 1)


def attention(qkv_act, lengths, cos_tab, sin_tab, kv_heads, head_dim):
    batch, seq_len, qkv_cols = qkv_act.shape
    group_cols = qkv_cols // kv_heads
    group_size = group_cols // head_dim - 2
    out_cols = group_size * head_dim
    pair = 2 * head_dim
    cos_pair = jnp.tile(cos_tab, (1, 4))
    sin_pair = jnp.tile(jnp.concatenate([-sin_tab, sin_tab], axis=1), (1, 2))
    flops = 2 * 2 * batch * kv_heads * group_size * seq_len * seq_len * head_dim
    return pl.pallas_call(
        functools.partial(attention_kernel, head_dim, group_size),
        out_shape=jax.ShapeDtypeStruct((batch, seq_len, kv_heads * out_cols), jnp.bfloat16),
        grid_spec=pltpu.PrefetchScalarGridSpec(
            num_scalar_prefetch=1,
            grid=(batch, kv_heads),
            in_specs=[
                pl.BlockSpec((1, seq_len, group_cols), lambda b, g, _: (b, 0, g)),
                pl.BlockSpec((seq_len, pair), lambda b, g, _: (0, 0)),
                pl.BlockSpec((seq_len, pair), lambda b, g, _: (0, 0)),
            ],
            out_specs=pl.BlockSpec((1, seq_len, out_cols), lambda b, g, _: (b, 0, g)),
            scratch_shapes=[pltpu.VMEM((seq_len, pair), jnp.bfloat16)] * 4,
        ),
        compiler_params=pltpu.CompilerParams(dimension_semantics=('arbitrary', 'arbitrary'), vmem_limit_bytes=48 * 1024 * 1024),
        cost_estimate=pl.CostEstimate(flops=4 * flops, bytes_accessed=2 * batch * seq_len * (qkv_cols + kv_heads * out_cols), transcendentals=batch * kv_heads * group_size * seq_len * seq_len),
        name='prefill_attention',
    )(lengths, qkv_act, cos_pair, sin_pair)


def empty(shape, dtype):
    return pl.pallas_call(lambda out_ref: None, out_shape=jax.ShapeDtypeStruct(shape, dtype), out_specs=pl.BlockSpec(memory_space=pl.ANY), name='output_buffer')()


def normalise(src, gain, dst, rows):
    def step(index, carry):
        part = pl.ds(pl.multiple_of(index * 64, 64), 64)
        wide = src[part, :].astype(jnp.float32)
        mean_sq = jnp.mean(wide * wide, axis=1, keepdims=True)
        dst[part, :] = (wide * lax.rsqrt(mean_sq + NORM_EPS) * gain).astype(jnp.bfloat16)
        return carry

    lax.fori_loop(0, rows // 64, step, 0)


def gate_up_kernel(slot, start, h_ref, gain_ref, w_ref, mid_ref, h_scr, u_scr, act_scr, mid_scr, w_buf, w_sem, h_sem, out_sem):
    rows, _ = h_scr.shape
    depth, _, tile, _ = w_buf.shape
    steps = w_ref.shape[1] // tile

    def w_copy(step):
        return pltpu.make_async_copy(w_ref.at[:, pl.ds(pl.multiple_of(step * tile, tile), tile), :], w_buf.at[lax.rem(step, depth)], w_sem.at[lax.rem(step, depth)])

    def out_copy(step):
        return pltpu.make_async_copy(mid_scr.at[lax.rem(step, 2)], mid_ref.at[:, pl.ds(pl.multiple_of(step * tile, tile), tile)], out_sem.at[lax.rem(step, 2)])

    h_copy = pltpu.make_async_copy(h_ref.at[slot, pl.ds(start, rows), :], h_scr, h_sem)
    h_copy.start()
    for step in range(min(depth - 1, steps)):
        w_copy(step).start()
    h_copy.wait()
    normalise(h_scr, gain_ref[...].astype(jnp.float32), u_scr, rows)

    def finish(step):
        gate = act_scr[0].astype(jnp.float32)
        up = act_scr[1].astype(jnp.float32)
        mid_scr[lax.rem(step, 2)] = (jax.nn.silu(gate) * up).astype(jnp.bfloat16)

    def body(step, carry):
        @pl.when(step + depth - 1 < steps)
        def _():
            w_copy(step + depth - 1).start()

        @pl.when(step >= 3)
        def _():
            out_copy(step - 3).wait()

        w_copy(step).wait()
        index = lax.rem(step, depth)
        gate = lax.dot_general(u_scr[...], w_buf[index, 0], NT_DIMS, preferred_element_type=jnp.float32)
        up = lax.dot_general(u_scr[...], w_buf[index, 1], NT_DIMS, preferred_element_type=jnp.float32)
        finish(step + 1)
        act_scr[0] = gate.astype(jnp.bfloat16)
        act_scr[1] = up.astype(jnp.bfloat16)

        @pl.when(step >= 1)
        def _():
            out_copy(step - 1).start()

        return carry

    act_scr[...] = jnp.zeros_like(act_scr)
    lax.fori_loop(0, steps, body, 0)
    if steps >= 3:
        out_copy(steps - 3).wait()
    finish(steps - 1)
    out_copy(steps - 1).start()
    if steps >= 2:
        out_copy(steps - 2).wait()
    out_copy(steps - 1).wait()


def gate_up(hidden, gain, weights, slot, start, rows):
    dim = hidden.shape[2]
    ff = weights.shape[1]
    tile = min(FF_TILE, ff)
    depth = 3
    anywhere = pl.BlockSpec(memory_space=pl.ANY)
    return pl.pallas_call(
        functools.partial(gate_up_kernel, slot, start),
        out_shape=jax.ShapeDtypeStruct((rows, ff), jnp.bfloat16),
        in_specs=[anywhere, pl.BlockSpec(memory_space=pltpu.VMEM), anywhere],
        out_specs=anywhere,
        scratch_shapes=[
            pltpu.VMEM((rows, dim), jnp.bfloat16),
            pltpu.VMEM((rows, dim), jnp.bfloat16),
            pltpu.VMEM((2, rows, tile), jnp.bfloat16),
            pltpu.VMEM((2, rows, tile), jnp.bfloat16),
            pltpu.VMEM((depth, 2, tile, dim), jnp.bfloat16),
            pltpu.SemaphoreType.DMA((depth,)),
            pltpu.SemaphoreType.DMA,
            pltpu.SemaphoreType.DMA((2,)),
        ],
        compiler_params=pltpu.CompilerParams(vmem_limit_bytes=58 * 1024 * 1024),
        cost_estimate=pl.CostEstimate(flops=4 * rows * dim * ff, bytes_accessed=4 * dim * ff + 2 * rows * (dim + ff), transcendentals=rows * ff),
        name='gate_up',
    )(hidden, gain[None, :], weights)


def down_kernel(slot, start, first, row_ref, h_ref, mid_ref, w_ref, y_in, y_ref, part_ref, h_scr, mid_scr, acc_scr, w_buf, w_sem, mid_sem, h_sem, out_sem):
    rows, dim = h_scr.shape
    depth, tile, _ = w_buf.shape
    steps = w_ref.shape[0] // tile
    out_tile = min(OUT_TILE, dim)

    def w_copy(step):
        return pltpu.make_async_copy(w_ref.at[pl.ds(pl.multiple_of(step * tile, tile), tile), :], w_buf.at[lax.rem(step, depth)], w_sem.at[lax.rem(step, depth)])

    def mid_copy(step):
        return pltpu.make_async_copy(mid_ref.at[pl.ds(first, rows), pl.ds(pl.multiple_of(step * tile, tile), tile)], mid_scr.at[lax.rem(step, depth)], mid_sem.at[lax.rem(step, depth)])

    h_copy = pltpu.make_async_copy(h_ref.at[slot, pl.ds(start, rows), :], h_scr, h_sem)
    h_copy.start()
    for step in range(min(depth - 1, steps)):
        w_copy(step).start()
        mid_copy(step).start()
    h_copy.wait()

    def widen(index, carry):
        part = pl.ds(pl.multiple_of(index * 64, 64), 64)
        acc_scr[part, :] = h_scr[part, :].astype(jnp.float32)
        return carry

    lax.fori_loop(0, rows // 64, widen, 0)

    def body(step, carry):
        @pl.when(step + depth - 1 < steps)
        def _():
            w_copy(step + depth - 1).start()
            mid_copy(step + depth - 1).start()

        w_copy(step).wait()
        mid_copy(step).wait()
        index = lax.rem(step, depth)
        mid = mid_scr[index]
        for col in range(0, dim, out_tile):
            cols = slice(col, col + out_tile)
            acc_scr[:, cols] += jnp.dot(mid, w_buf[index, :, cols], preferred_element_type=jnp.float32)
        return carry

    lax.fori_loop(0, steps, body, 0)

    def narrow(index, carry):
        part = pl.ds(pl.multiple_of(index * 64, 64), 64)
        h_scr[part, :] = acc_scr[part, :].astype(jnp.bfloat16)
        return carry

    lax.fori_loop(0, rows // 64, narrow, 0)
    part_out = pltpu.make_async_copy(h_scr, part_ref, out_sem.at[0])
    y_out = pltpu.make_async_copy(h_scr, y_ref.at[slot, row_ref[0], pl.ds(start, rows), :], out_sem.at[1])
    part_out.start()
    y_out.start()
    part_out.wait()
    y_out.wait()


def down_proj(row, hidden, mid, weights, y_all, slot, start, first, rows):
    dim = hidden.shape[2]
    ff = mid.shape[1]
    tile = min(FF_TILE, ff)
    depth = 4
    anywhere = pl.BlockSpec(memory_space=pl.ANY)
    return pl.pallas_call(
        functools.partial(down_kernel, slot, start, first),
        out_shape=(jax.ShapeDtypeStruct(y_all.shape, jnp.bfloat16), jax.ShapeDtypeStruct((rows, dim), jnp.bfloat16)),
        in_specs=[pl.BlockSpec(memory_space=pltpu.SMEM), anywhere, anywhere, anywhere, anywhere],
        out_specs=(anywhere, anywhere),
        scratch_shapes=[
            pltpu.VMEM((rows, dim), jnp.bfloat16),
            pltpu.VMEM((depth, rows, tile), jnp.bfloat16),
            pltpu.VMEM((rows, dim), jnp.float32),
            pltpu.VMEM((depth, tile, dim), jnp.bfloat16),
            pltpu.SemaphoreType.DMA((depth,)),
            pltpu.SemaphoreType.DMA((depth,)),
            pltpu.SemaphoreType.DMA,
            pltpu.SemaphoreType.DMA((2,)),
        ],
        input_output_aliases={4: 0},
        compiler_params=pltpu.CompilerParams(vmem_limit_bytes=58 * 1024 * 1024),
        cost_estimate=pl.CostEstimate(flops=2 * rows * dim * ff, bytes_accessed=2 * dim * ff + 2 * rows * (4 * dim + ff), transcendentals=0),
        name='down_proj',
    )(row, hidden, mid, weights, y_all)


def place_kernel(spots, n_rows, row_ref, y_in, *refs):
    pieces, (y_ref, buf, in_sem, out_sem) = refs[:len(spots)], refs[len(spots):]
    block = buf.shape[1]
    loads, stores = [], []
    for piece, (slot, offset, start, rows) in zip(pieces, spots):
        owner = lax.rem(row_ref[0] + offset, n_rows)
        for first in range(0, rows, block):
            at = len(loads)
            loads.append(pltpu.make_async_copy(piece.at[pl.ds(first, block), :], buf.at[at], in_sem.at[at]))
            stores.append(pltpu.make_async_copy(buf.at[at], y_ref.at[slot, owner, pl.ds(start + first, block), :], out_sem.at[at]))
    for load in loads:
        load.start()
    for load, store in zip(loads, stores):
        load.wait()
        store.start()
    for store in stores:
        store.wait()


def place(row, y_all, pieces):
    arrays = [piece for piece, _ in pieces]
    spots = [spot for _, spot in pieces]
    block = min(256, *(spot[3] for spot in spots))
    count = sum(spot[3] for spot in spots) // block
    dim = y_all.shape[3]
    anywhere = pl.BlockSpec(memory_space=pl.ANY)
    moved = 2 * dim * sum(spot[3] for spot in spots)
    return pl.pallas_call(
        functools.partial(place_kernel, spots, y_all.shape[1]),
        out_shape=jax.ShapeDtypeStruct(y_all.shape, y_all.dtype),
        in_specs=[pl.BlockSpec(memory_space=pltpu.SMEM)] + [anywhere] * (1 + len(arrays)),
        out_specs=anywhere,
        scratch_shapes=[pltpu.VMEM((count, block, dim), jnp.bfloat16), pltpu.SemaphoreType.DMA((count,)), pltpu.SemaphoreType.DMA((count,))],
        input_output_aliases={1: 0},
        compiler_params=pltpu.CompilerParams(vmem_limit_bytes=40 * 1024 * 1024),
        cost_estimate=pl.CostEstimate(flops=moved * 100, bytes_accessed=2 * moved, transcendentals=0),
        name='place_rows',
    )(row, y_all, *arrays)


def relayout_kernel(row_ref, gu_ref, d_ref, gate_ref, up_ref, down_ref):
    gate_ref[...] = jnp.transpose(gu_ref[0].astype(jnp.float32)).astype(jnp.bfloat16)
    up_ref[...] = jnp.transpose(gu_ref[1].astype(jnp.float32)).astype(jnp.bfloat16)
    down_ref[...] = d_ref[...]


def relayout(row, gu_full, down_full, n_rows):
    _, ff, dim = gu_full.shape
    own = ff // n_rows
    tile = min(128, own)
    steps = own // tile
    column = pl.BlockSpec((dim, tile), lambda j, _: (0, j))
    return pl.pallas_call(
        relayout_kernel,
        out_shape=(jax.ShapeDtypeStruct((dim, own), jnp.bfloat16), jax.ShapeDtypeStruct((dim, own), jnp.bfloat16), jax.ShapeDtypeStruct((own, dim), jnp.bfloat16)),
        grid_spec=pltpu.PrefetchScalarGridSpec(
            num_scalar_prefetch=1,
            grid=(steps,),
            in_specs=[
                pl.BlockSpec((2, tile, dim), lambda j, at: (0, at[0] * steps + j, 0)),
                pl.BlockSpec((tile, dim), lambda j, at: (at[0] * steps + j, 0)),
            ],
            out_specs=(column, column, pl.BlockSpec((tile, dim), lambda j, _: (j, 0))),
        ),
        compiler_params=pltpu.CompilerParams(dimension_semantics=('arbitrary',), vmem_limit_bytes=40 * 1024 * 1024),
        cost_estimate=pl.CostEstimate(flops=600 * own * dim, bytes_accessed=12 * own * dim, transcendentals=0),
        name='relayout',
    )(row, gu_full, down_full)


def gather_attn_kernel(ring, kv_rows, x_ref, gain_ref, wq_ref, wo_ref, q_ref, o_ref, kv_ref, q_scr, o_scr, x_scr, u_scr, kv_scr, send_sem, recv_sem, local_sem, x_sem, out_sem, q_sem):
    n_row, n_col = ring
    row = lax.axis_index('tpa')
    col = lax.axis_index('tpb')
    core = lax.rem(col, 2)
    chip = col // 2
    n_chip = n_col // 2
    far = n_row // 2
    mate = col + 1 - 2 * core

    def at_row(offset):
        return lax.rem(row + offset + n_row, n_row)

    def at_col(offset):
        return 2 * lax.rem(chip + offset + n_chip, n_chip) + core

    def peer(axis, step):
        return {'tpa': at_row(step)} if axis == 'y' else {'tpb': at_col(step)}

    barrier = pltpu.get_barrier_semaphore()
    for axis in 'xy':
        for step in (1, -1):
            pl.semaphore_signal(barrier, inc=1, device_id=peer(axis, step), device_id_type=MESH)
    pl.semaphore_signal(barrier, inc=1, device_id={'tpb': mate}, device_id_type=MESH)

    offsets = (0, -1, 1, far)
    tensors = (('q', q_scr, wq_ref, 'xy'), ('o', o_scr, wo_ref, 'yx'))
    started = []
    index_of = {}

    def sem_at(key):
        return index_of.setdefault(key, len(index_of))

    def slot(order, first, second):
        dx, dy = (first, second) if order == 'xy' else (second, first)
        return at_row(dy), at_col(dx)

    def halves(scr):
        rows = scr.shape[2]
        split = (rows // 32) * 16
        return {1: slice(0, split), -1: slice(split, rows), 0: slice(0, rows)}

    def descriptor(scr, where, part, target, key):
        ref = scr.at[where[0], where[1], halves(scr)[part], :]
        return pltpu.make_async_remote_copy(src_ref=ref, dst_ref=ref, send_sem=send_sem.at[sem_at(key)], recv_sem=recv_sem.at[sem_at(key)], device_id=target, device_id_type=MESH)

    def send(name, scr, order, first, second, part, axis, step):
        key = (name, first, second, part, axis, step)
        target = {'tpb': mate} if axis == 'm' else peer(axis, step)
        copy = descriptor(scr, slot(order, first, second), part, target, key)
        copy.start()
        started.append(copy)

    def receive(scr, order, first, second, part, key):
        where = slot(order, first, second)
        descriptor(scr, where, part, {'tpb': mate}, key).wait_recv()

    own_batch, _, seq_len, dim = x_ref.shape
    rows = x_scr.shape[1]
    per = seq_len // rows
    tiles = own_batch * n_row * per

    def fetch_x(tile):
        slot, where = tile // (n_row * per), lax.rem(tile // per, n_row)
        return pltpu.make_async_copy(x_ref.at[slot, where, pl.ds(pl.multiple_of(lax.rem(tile, per) * rows, rows), rows), :], x_scr.at[lax.rem(tile, 2)], x_sem.at[lax.rem(tile, 2)])

    def store_kv(tile):
        return pltpu.make_async_copy(kv_scr.at[lax.rem(tile, 2)], kv_ref.at[tile // per, :, pl.ds(pl.multiple_of(lax.rem(tile, per) * rows, rows), rows)], out_sem.at[lax.rem(tile, 2)])

    own = [pltpu.make_async_copy(ref, scr.at[row, col], local_sem.at[k]) for k, (_, scr, ref, _) in enumerate(tensors)]
    for copy in own:
        copy.start()
    for tile in range(min(2, tiles)):
        fetch_x(jnp.int32(tile)).start()
    for copy in own:
        copy.wait()
    pl.semaphore_wait(barrier, 5)

    def spread(name, scr, order, first):
        for step in (1, -1):
            send(name, scr, order, first, 0, 0, order[1], step)
        send(name, scr, order, first, 0, 0, 'm', 0)

    for name, scr, _, order in tensors:
        for step in (1, -1):
            send(name, scr, order, 0, 0, 0, order[0], step)
    for name, scr, _, order in tensors:
        spread(name, scr, order, 0)
    gain = gain_ref[...].astype(jnp.float32)
    for step in (1, -1):
        for name, scr, _, order in tensors:
            receive(scr, order, -step, 0, 0, (name, 0, 0, 0, order[0], step))
            send(name, scr, order, -step, 0, step, order[0], step)
            spread(name, scr, order, -step)
    for name, scr, _, order in tensors:
        for step in (1, -1):
            receive(scr, order, far, 0, step, (name, -step, 0, step, order[0], step))
        spread(name, scr, order, far)

    def mate_wait(name, scr, order, first, second):
        dx, dy = (first, second) if order == 'xy' else (second, first)
        ref = scr.at[at_row(dy), 2 * lax.rem(chip + dx + n_chip, n_chip) + 1 - core]
        key = sem_at((name, first, second, 0, 'm', 0))
        pltpu.make_async_remote_copy(src_ref=ref, dst_ref=ref, send_sem=send_sem.at[key], recv_sem=recv_sem.at[key], device_id={'tpb': mate}, device_id_type=MESH).wait_recv()

    cols = q_scr.shape[1] * q_scr.shape[2]

    def kv_tiles(first, last):
        def body(tile, carry):
            fetch_x(tile).wait()
            normalise(x_scr.at[lax.rem(tile, 2)], gain, u_scr, rows)

            @pl.when(tile + 2 < tiles)
            def _():
                fetch_x(tile + 2).start()

            @pl.when(tile >= 2)
            def _():
                store_kv(tile - 2).wait()

            weight = q_scr[row].reshape(cols, dim)[cols - kv_rows:]
            kv_scr[lax.rem(tile, 2)] = lax.dot_general(weight, u_scr[...], NT_DIMS, preferred_element_type=jnp.float32).astype(jnp.bfloat16)
            store_kv(tile).start()
            return carry

        lax.fori_loop(first, last, body, 0)

    def store_q(offset, at):
        return pltpu.make_async_copy(q_scr.at[at_row(offset)], q_ref.at[at_row(offset)], q_sem.at[at])

    def second_hop(name, scr, order, first):
        for step in (1, -1):
            receive(scr, order, first, -step, 0, (name, first, 0, 0, order[1], step))
            send(name, scr, order, first, -step, step, order[1], step)
            send(name, scr, order, first, -step, 0, 'm', 0)

    for first in offsets[:2]:
        for name, scr, _, order in tensors:
            second_hop(name, scr, order, first)
    for first in offsets:
        mate_wait('q', q_scr, 'xy', first, 0)
    store_q(0, 0).start()
    kv_tiles(0, tiles // 4)
    for first in offsets[2:]:
        for name, scr, _, order in tensors:
            second_hop(name, scr, order, first)
    kv_tiles(tiles // 4, tiles // 2)

    def last_hop(name, scr, order):
        for first in offsets:
            for step in (1, -1):
                receive(scr, order, first, far, step, (name, first, -step, step, order[1], step))
            send(name, scr, order, first, far, 0, 'm', 0)

    for second in offsets[1:3]:
        for first in offsets:
            mate_wait('q', q_scr, 'xy', first, second)
        store_q(second, offsets.index(second)).start()
    last_hop('q', q_scr, 'xy')
    last_hop('o', o_scr, 'yx')
    kv_tiles(tiles // 2, tiles)
    for first in offsets:
        mate_wait('q', q_scr, 'xy', first, far)
    store_q(far, 3).start()
    for second in offsets:
        for first in offsets:
            mate_wait('o', o_scr, 'yx', first, second)
    o_out = pltpu.make_async_copy(o_scr, o_ref, local_sem.at[0])
    o_out.start()
    for copy in started:
        copy.wait_send()
    for tile in range(max(0, tiles - 2), tiles):
        store_kv(jnp.int32(tile)).wait()
    for at, offset in enumerate(offsets):
        store_q(offset, at).wait()
    o_out.wait()


def gather_attn(x_rows, gain, w_qkv_t, w_o, n_row, n_col, kv_rows):
    own_batch, _, seq_len, dim = x_rows.shape
    q_rows, o_rows = w_qkv_t.shape[0], w_o.shape[0]
    rows = min(512, seq_len)
    tokens = own_batch * n_row * seq_len
    moves = 2 * (4 + 9 * n_row)
    anywhere = pl.BlockSpec(memory_space=pl.ANY)
    return pl.pallas_call(
        functools.partial(gather_attn_kernel, (n_row, n_col), kv_rows),
        out_shape=(
            jax.ShapeDtypeStruct((n_row, n_col, q_rows, dim), jnp.bfloat16),
            jax.ShapeDtypeStruct((n_row, n_col, o_rows, dim), jnp.bfloat16),
            jax.ShapeDtypeStruct((own_batch * n_row, kv_rows, seq_len), jnp.bfloat16),
        ),
        in_specs=[anywhere, pl.BlockSpec(memory_space=pltpu.VMEM), anywhere, anywhere],
        out_specs=(anywhere, anywhere, anywhere),
        scratch_shapes=[
            pltpu.VMEM((n_row, n_col, q_rows, dim), jnp.bfloat16),
            pltpu.VMEM((n_row, n_col, o_rows, dim), jnp.bfloat16),
            pltpu.VMEM((2, rows, dim), jnp.bfloat16),
            pltpu.VMEM((rows, dim), jnp.bfloat16),
            pltpu.VMEM((2, kv_rows, rows), jnp.bfloat16),
            pltpu.SemaphoreType.DMA((moves,)),
            pltpu.SemaphoreType.DMA((moves,)),
            pltpu.SemaphoreType.DMA((2,)),
            pltpu.SemaphoreType.DMA((2,)),
            pltpu.SemaphoreType.DMA((2,)),
            pltpu.SemaphoreType.DMA((4,)),
        ],
        compiler_params=pltpu.CompilerParams(collective_id=0, has_side_effects=True, vmem_limit_bytes=58 * 1024 * 1024),
        cost_estimate=pl.CostEstimate(flops=2 * tokens * dim * kv_rows, bytes_accessed=2 * dim * n_row * n_col * (q_rows + o_rows), transcendentals=0),
        name='gather_attn',
    )(x_rows, gain[None, :], w_qkv_t, w_o)


def qkv_kernel(row_ref, x_ref, gain_ref, w_ref, out_ref, u_scr):
    piece, tile = pl.program_id(0), pl.program_id(1)

    @pl.when(piece == 0)
    def _():
        normalise(x_ref.at[0, 0], gain_ref[...].astype(jnp.float32), u_scr.at[tile], x_ref.shape[2])

    out_ref[0] = lax.dot_general(u_scr[tile], w_ref[...], NT_DIMS, preferred_element_type=jnp.float32).astype(jnp.bfloat16)


def qkv_proj(row, x_rows, gain, qkv_t, pieces):
    own_batch, _, seq_len, dim = x_rows.shape
    cols = qkv_t.shape[0] // pieces
    rows = min(512, seq_len)
    per = seq_len // rows
    tiles = own_batch * per

    def x_index(piece, tile, own):
        at = jnp.where(piece == 0, tile, tiles - 1)
        return (at // per, own[0], at % per, 0)

    return pl.pallas_call(
        qkv_kernel,
        out_shape=jax.ShapeDtypeStruct((own_batch, seq_len, pieces * cols), jnp.bfloat16),
        grid_spec=pltpu.PrefetchScalarGridSpec(
            num_scalar_prefetch=1,
            grid=(pieces, tiles),
            in_specs=[
                pl.BlockSpec((1, 1, rows, dim), x_index),
                pl.BlockSpec((1, dim), lambda p, t, _: (0, 0)),
                pl.BlockSpec((cols, dim), lambda p, t, _: (p, 0)),
            ],
            out_specs=pl.BlockSpec((1, rows, cols), lambda p, t, _: (t // per, t % per, p)),
            scratch_shapes=[pltpu.VMEM((tiles, rows, dim), jnp.bfloat16)],
        ),
        compiler_params=pltpu.CompilerParams(dimension_semantics=('arbitrary', 'arbitrary'), vmem_limit_bytes=60 * 1024 * 1024),
        cost_estimate=pl.CostEstimate(flops=2 * own_batch * seq_len * dim * pieces * cols, bytes_accessed=2 * dim * (pieces * cols + 2 * own_batch * seq_len), transcendentals=0),
        name='qkv_proj',
    )(row, x_rows, gain[None, :], qkv_t)


def out_kernel(row_ref, a_ref, x_ref, w_ref, h_ref, w_scr, sem):
    @pl.when(pl.program_id(0) == 0)
    def _():
        copy = pltpu.make_async_copy(w_ref, w_scr, sem)
        copy.start()
        copy.wait()

    dim = h_ref.shape[2]
    out_tile = min(OUT_TILE, dim)
    for col in range(0, dim, out_tile):
        cols = slice(col, col + out_tile)
        acc = jnp.dot(a_ref[0], w_scr[:, cols], preferred_element_type=jnp.float32)
        h_ref[0, :, cols] = (x_ref[0, 0, :, cols].astype(jnp.float32) + acc).astype(jnp.bfloat16)


def out_proj(row, attn, x_rows, w_o):
    own_batch, seq_len, depth = attn.shape
    dim = x_rows.shape[3]
    rows = min(256, seq_len)
    per = seq_len // rows
    return pl.pallas_call(
        out_kernel,
        out_shape=jax.ShapeDtypeStruct((own_batch, seq_len, dim), jnp.bfloat16),
        grid_spec=pltpu.PrefetchScalarGridSpec(
            num_scalar_prefetch=1,
            grid=(own_batch * per,),
            in_specs=[
                pl.BlockSpec((1, rows, depth), lambda t, _: (t // per, t % per, 0)),
                pl.BlockSpec((1, 1, rows, dim), lambda t, own: (t // per, own[0], t % per, 0)),
                pl.BlockSpec(memory_space=pl.ANY),
            ],
            out_specs=pl.BlockSpec((1, rows, dim), lambda t, _: (t // per, t % per, 0)),
            scratch_shapes=[pltpu.VMEM((depth, dim), jnp.bfloat16), pltpu.SemaphoreType.DMA],
        ),
        compiler_params=pltpu.CompilerParams(dimension_semantics=('arbitrary',), vmem_limit_bytes=56 * 1024 * 1024),
        cost_estimate=pl.CostEstimate(flops=2 * own_batch * seq_len * dim * depth, bytes_accessed=2 * dim * (depth + 3 * own_batch * seq_len), transcendentals=0),
        name='out_proj',
    )(row, attn, x_rows, w_o)


def solution(mesh):
    n_tpa = mesh.shape['tpa']
    n_tpb = mesh.shape['tpb']
    up_ring = [(i, (i + 1) % n_tpa) for i in range(n_tpa)]
    down_ring = [(i, (i - 1) % n_tpa) for i in range(n_tpa)]
    both = ('tpa', 'tpb')

    def layer_step(x_loc, len_loc, k_buf, v_buf, w_qkv, w_o, w_gate_up, w_down, g_attn, g_mlp):
        row = lax.axis_index('tpa')
        batch_loc, seq_len, model_dim = x_loc.shape
        head_dim = k_buf.shape[3]
        own_batch = batch_loc // n_tpa
        ff_block = w_gate_up.shape[1] // 2
        qkv_row = w_qkv.shape[1] * n_tpb
        o_row = w_o.shape[0] * n_tpb

        row_arg = row.astype(jnp.int32)[None]
        cos_tab, sin_tab = rope_tables(seq_len, head_dim)
        x_rows = x_loc.reshape(own_batch, n_tpa, seq_len, model_dim)
        len_own = lax.dynamic_index_in_dim(len_loc.reshape(own_batch, n_tpa), row, 1, keepdims=False)

        kv_cols = k_buf.shape[2] * head_dim
        q_full, o_full, kv_new = gather_attn(x_rows, g_attn, w_qkv.T, w_o, n_tpa, n_tpb, 2 * kv_cols)
        q_full, o_full, kv_new, gu_block, down_block = lax.optimization_barrier((q_full, o_full, kv_new, w_gate_up.T, w_down))
        gu_full = lax.all_gather(gu_block.reshape(2, ff_block, model_dim), both, axis=1, tiled=True)
        down_full = lax.all_gather(down_block, both, axis=0, tiled=True)
        qkv_act = qkv_proj(row_arg, x_rows, g_attn, q_full.reshape(-1, model_dim), 4)
        attn_out = attention(qkv_act, len_own, cos_tab, sin_tab, n_tpa * k_buf.shape[2], head_dim)
        hidden = out_proj(row_arg, attn_out, x_rows, o_full.reshape(-1, model_dim))

        y_all = empty((own_batch, n_tpa, seq_len, model_dim), jnp.bfloat16)

        gate_rows = seq_len // GATES_PER_PROMPT
        gates = [(slot, start) for slot in range(own_batch) for start in range(0, seq_len, gate_rows)]
        chunks = []
        for index, (slot, start) in enumerate(gates):
            parts = 2 if index in (0, len(gates) - 1) else 1
            for part in range(parts):
                chunks.append((index, part * gate_rows // parts, gate_rows // parts))
        spots = [(gates[index][0], gates[index][1] + offset, rows) for index, offset, rows in chunks]
        mids = []
        for slot, start in gates:
            mids.append(gate_up(hidden, g_mlp, gu_full, slot, start, gate_rows))
        fars = []
        near = []
        for index, (gate, offset, rows) in enumerate(chunks):
            slot, start, _ = spots[index]
            y_all, part = down_proj(row_arg, hidden, mids[gate], down_full, y_all, slot, start, offset, rows)
            near.append((lax.ppermute(part, 'tpa', up_ring), lax.ppermute(part, 'tpa', down_ring)))

        y_all, kv_late, o_late, q_late, gu_late, down_late = lax.optimization_barrier((y_all, kv_new, o_full, q_full, gu_full, down_full))
        q_cols = qkv_row - 2 * kv_cols
        qkv_own = lax.dynamic_index_in_dim(q_late, row, 0, keepdims=False).reshape(qkv_row, model_dim)
        o_rows = lax.dynamic_index_in_dim(o_late, row, 0, keepdims=False).reshape(o_row, model_dim)
        w_query = qkv_own[:q_cols].T
        w_key = qkv_own[q_cols:q_cols + kv_cols].T
        w_value = qkv_own[q_cols + kv_cols:].T
        kv_new = kv_late.transpose(0, 2, 1)
        half_dim = head_dim // 2
        k_first = kv_new[..., :half_dim].astype(jnp.float32)
        k_second = kv_new[..., half_dim:head_dim].astype(jnp.float32)
        k_rot = jnp.concatenate([k_first * cos_tab - k_second * sin_tab, k_second * cos_tab + k_first * sin_tab], axis=-1).astype(jnp.bfloat16)
        valid_pos = (jnp.arange(seq_len)[None, :] < len_loc[:, None])[:, :, None, None]
        k_cache = jnp.where(valid_pos, k_rot[:, :, None, :], k_buf)
        v_cache = jnp.where(valid_pos, kv_new[:, :, None, head_dim:], v_buf)
        w_gate, w_up, down_rows = relayout(row_arg, gu_late, down_late, n_tpa)
        cache_outs = (k_cache, v_cache, w_query, w_key, w_value, o_rows)
        near[-2], cache_outs = lax.optimization_barrier((near[-2], cache_outs))
        k_cache, v_cache, w_query, w_key, w_value, o_rows = cache_outs
        near[-1], (w_gate, w_up, down_rows) = lax.optimization_barrier((near[-1], (w_gate, w_up, down_rows)))
        for index, ((from_below, from_above), (slot, start, rows)) in enumerate(zip(near, spots)):
            if index % 2 == 0:
                far = lax.ppermute(from_below, 'tpa', up_ring)
            else:
                far = lax.ppermute(from_above, 'tpa', down_ring)
            fars.append(far)

        def near_pieces(first, last):
            for (from_below, from_above), (slot, start, rows) in list(zip(near, spots))[first:last]:
                yield from_below, (slot, n_tpa - 1, start, rows)
                yield from_above, (slot, 1, start, rows)

        def far_pieces(first, last):
            for far, (slot, start, rows) in list(zip(fars, spots))[first:last]:
                yield far, (slot, n_tpa - 2, start, rows)

        n_first = len(spots) // 2
        y_all = place(row_arg, y_all, [*near_pieces(0, n_first), *far_pieces(0, 2)])
        y_all = place(row_arg, y_all, [*near_pieces(n_first, len(spots)), *far_pieces(2, n_first)])
        for index in range(n_first, len(spots)):
            y_all = place(row_arg, y_all, [*far_pieces(index, index + 1)])
        layer_out = y_all.reshape(batch_loc, seq_len, model_dim)
        return (layer_out, k_cache, v_cache, w_query, w_key, w_value, o_rows, w_gate, w_up, down_rows)

    batch_spec = P(('part', 'tpb'), None, None)
    len_spec = P(('part', 'tpb'))
    cache_spec = P(('part', 'tpb'), None, 'tpa', None)
    train_cols = P('part', ('tpa', 'tpb'))
    train_rows = P(('part', 'tpa', 'tpb'), None)
    gain_spec = P('part')
    gen_cols = P('part', 'tpa')
    gen_rows = P(('part', 'tpa'), None)
    return jax.shard_map(layer_step, mesh=mesh, in_specs=(batch_spec, len_spec, cache_spec, cache_spec, train_cols, train_rows, train_cols, train_rows, gain_spec, gain_spec), out_specs=(batch_spec, cache_spec, cache_spec, gen_cols, gen_cols, gen_cols, gen_rows, gen_cols, gen_cols, gen_rows), check_vma=False)
```

```python
import functools
import math
import jax
import jax.numpy as jnp
from jax import lax
from jax.experimental import pallas as pl
from jax.experimental.pallas import tpu as pltpu
from jax.sharding import PartitionSpec as P

ROPE_BASE = 500000.0
ROPE_FACTOR = 8.0
LOW_FREQ = 1.0
HIGH_FREQ = 4.0
ORIG_CONTEXT = 8192.0
NORM_EPS = 1e-5
MASK_VALUE = -1e30
Q_TILE = 256
SCORE_LIMIT = 64.0
FF_TILE = 512
OUT_TILE = 512
NT_DIMS = (((1,), (1,)), ((), ()))
MESH = pl.DeviceIdType.MESH
GATE_TILE = 512


def rope_tables(seq_len, head_dim):
    exponent = jnp.arange(head_dim // 2, dtype=jnp.float32) * (2.0 / head_dim)
    inv_freq = 1.0 / jnp.power(ROPE_BASE, exponent)
    wavelen = 2.0 * math.pi / inv_freq
    smooth = (ORIG_CONTEXT / wavelen - LOW_FREQ) / (HIGH_FREQ - LOW_FREQ)
    blended = (1.0 - smooth) * inv_freq / ROPE_FACTOR + smooth * inv_freq
    rope_freq = jnp.where(wavelen < ORIG_CONTEXT / HIGH_FREQ, inv_freq, jnp.where(wavelen > ORIG_CONTEXT / LOW_FREQ, inv_freq / ROPE_FACTOR, blended))
    angles = jnp.arange(seq_len, dtype=jnp.float32)[:, None] * rope_freq[None, :]
    return jnp.cos(angles), jnp.sin(angles)


def attention_kernel(head_dim, group_size, len_ref, qkv_ref, cos_ref, sin_ref, out_ref, kl_scr, kr_scr, vl_scr, vr_scr):
    seq_len = qkv_ref.shape[1]
    pair = 2 * head_dim
    length = len_ref[pl.program_id(0)]
    lane = lax.broadcasted_iota(jnp.int32, (1, pair), 1)
    low_lane = lane < head_dim
    first_half = lax.rem(lane, head_dim) < head_dim // 2
    one_low = jnp.where(lane == 0, 1.0, 0.0)
    one_high = jnp.where(lane == head_dim, 1.0, 0.0)

    def rope(vec, rows):
        ahead = pltpu.roll(vec, pair - head_dim // 2, 1)
        behind = pltpu.roll(vec, head_dim // 2, 1)
        return vec * cos_ref[rows, :] + jnp.where(first_half, ahead, behind) * sin_ref[rows, :]

    q_cols = group_size * head_dim
    same_head = lax.broadcasted_iota(jnp.int32, (pair, pair), 0) // head_dim == lax.broadcasted_iota(jnp.int32, (pair, pair), 1) // head_dim
    head_sum = jnp.where(same_head, 1.0, 0.0).astype(jnp.bfloat16)
    q_top = jnp.zeros((Q_TILE, pair), jnp.float32)
    k_top = jnp.zeros((Q_TILE, pair), jnp.float32)
    for start in range(0, seq_len, Q_TILE):
        rows = pl.ds(start, Q_TILE)
        kv = qkv_ref[0, rows, q_cols:q_cols + pair].astype(jnp.float32)
        k_rot = rope(kv, rows)
        key_id = start + lax.broadcasted_iota(jnp.int32, (Q_TILE, pair), 0)
        bias = jnp.where(key_id < length, 0.0, MASK_VALUE)
        kl_scr[rows, :] = jnp.where(low_lane, k_rot, bias * one_high).astype(jnp.bfloat16)
        kr_scr[rows, :] = jnp.where(low_lane, bias * one_low, pltpu.roll(k_rot, head_dim, 1)).astype(jnp.bfloat16)
        vl_scr[rows, :] = jnp.where(low_lane, pltpu.roll(kv, head_dim, 1), 0.0).astype(jnp.bfloat16)
        vr_scr[rows, :] = jnp.where(low_lane, 0.0, kv).astype(jnp.bfloat16)
        squares = jnp.where(low_lane, k_rot * k_rot, 0.0).astype(jnp.bfloat16)
        k_top = jnp.maximum(k_top, jnp.dot(squares, head_sum, preferred_element_type=jnp.float32))
        for col in range(0, q_cols, pair):
            query = qkv_ref[0, rows, col:col + pair].astype(jnp.float32)
            squares = (query * query).astype(jnp.bfloat16)
            q_top = jnp.maximum(q_top, jnp.dot(squares, head_sum, preferred_element_type=jnp.float32))
    small = jnp.max(q_top) * jnp.max(k_top) < head_dim * SCORE_LIMIT ** 2

    def attend(start, keys, keep_top, unroll):
        rows = pl.ds(start, Q_TILE)
        row_id = start + lax.broadcasted_iota(jnp.int32, (Q_TILE, Q_TILE), 0)
        col_id = lax.broadcasted_iota(jnp.int32, (Q_TILE, Q_TILE), 1)

        def weights(query, k_scr):
            scores = lax.dot_general(query, k_scr[:keys, :], NT_DIMS, preferred_element_type=jnp.float32)
            parts = [scores[:, block:block + Q_TILE] for block in range(0, keys, Q_TILE)]
            if keep_top:
                parts = [jnp.where(block * Q_TILE + col_id <= row_id, part, MASK_VALUE) for block, part in enumerate(parts)]
                top = parts[0]
                for part in parts[1:]:
                    top = jnp.maximum(top, part)
                top = jnp.max(top, axis=1, keepdims=True)
                parts = [part - top for part in parts]
            else:
                parts[-1] = jnp.where(start + col_id <= row_id, parts[-1], MASK_VALUE)
            parts = [jnp.exp(part) for part in parts]
            total = parts[0]
            for part in parts[1:]:
                total = total + part
            scale = 1.0 / jnp.sum(total, axis=1, keepdims=True)
            return jnp.concatenate([(part * scale).astype(jnp.bfloat16) for part in parts], axis=1)

        def head_pair(index, carry):
            cols = pl.ds(pl.multiple_of(index * pair, pair), pair)
            query = rope(qkv_ref[0, rows, cols].astype(jnp.float32), rows).astype(jnp.bfloat16).astype(jnp.float32) * head_dim ** -0.5
            left = weights(jnp.where(low_lane, query, one_high).astype(jnp.bfloat16), kl_scr)
            right = weights(jnp.where(low_lane, one_low, query).astype(jnp.bfloat16), kr_scr)
            acc = jnp.dot(left, vl_scr[:keys, :], preferred_element_type=jnp.float32)
            acc = acc + jnp.dot(right, vr_scr[:keys, :], preferred_element_type=jnp.float32)
            out_ref[0, rows, cols] = acc.astype(jnp.bfloat16)
            return carry

        lax.fori_loop(0, group_size // 2, head_pair, 0, unroll=unroll)

    @pl.when(small)
    def _():
        for start in range(0, seq_len, Q_TILE):
            attend(start, start + Q_TILE, False, 2)

    @pl.when(jnp.logical_not(small))
    def _():
        def tile(index, carry):
            attend(pl.multiple_of(index * Q_TILE, Q_TILE), seq_len, True, 1)
            return carry

        lax.fori_loop(0, seq_len // Q_TILE, tile, 0)


def attention(qkv_act, lengths, cos_tab, sin_tab, kv_heads, head_dim):
    batch, seq_len, qkv_cols = qkv_act.shape
    group_cols = qkv_cols // kv_heads
    group_size = group_cols // head_dim - 2
    out_cols = group_size * head_dim
    pair = 2 * head_dim
    cos_pair = jnp.tile(cos_tab, (1, 4))
    sin_pair = jnp.tile(jnp.concatenate([-sin_tab, sin_tab], axis=1), (1, 2))
    flops = 2 * 2 * batch * kv_heads * group_size * seq_len * seq_len * head_dim
    return pl.pallas_call(
        functools.partial(attention_kernel, head_dim, group_size),
        out_shape=jax.ShapeDtypeStruct((batch, seq_len, kv_heads * out_cols), jnp.bfloat16),
        grid_spec=pltpu.PrefetchScalarGridSpec(
            num_scalar_prefetch=1,
            grid=(batch, kv_heads),
            in_specs=[
                pl.BlockSpec((1, seq_len, group_cols), lambda b, g, _: (b, 0, g)),
                pl.BlockSpec((seq_len, pair), lambda b, g, _: (0, 0)),
                pl.BlockSpec((seq_len, pair), lambda b, g, _: (0, 0)),
            ],
            out_specs=pl.BlockSpec((1, seq_len, out_cols), lambda b, g, _: (b, 0, g)),
            scratch_shapes=[pltpu.VMEM((seq_len, pair), jnp.bfloat16)] * 4,
        ),
        compiler_params=pltpu.CompilerParams(dimension_semantics=('arbitrary', 'arbitrary'), vmem_limit_bytes=48 * 1024 * 1024),
        cost_estimate=pl.CostEstimate(flops=4 * flops, bytes_accessed=2 * batch * seq_len * (qkv_cols + kv_heads * out_cols), transcendentals=batch * kv_heads * group_size * seq_len * seq_len),
        name='prefill_attention',
    )(lengths, qkv_act, cos_pair, sin_pair)


def empty(shape, dtype):
    return pl.pallas_call(lambda out_ref: None, out_shape=jax.ShapeDtypeStruct(shape, dtype), out_specs=pl.BlockSpec(memory_space=pl.ANY), name='output_buffer')()


def normalise(src, gain, dst, rows):
    def step(index, carry):
        part = pl.ds(pl.multiple_of(index * 64, 64), 64)
        wide = src[part, :].astype(jnp.float32)
        mean_sq = jnp.mean(wide * wide, axis=1, keepdims=True)
        dst[part, :] = (wide * lax.rsqrt(mean_sq + NORM_EPS) * gain).astype(jnp.bfloat16)
        return carry

    lax.fori_loop(0, rows // 64, step, 0)


def gate_up_kernel(slot, start, h_ref, gain_ref, w_ref, mid_ref, h_scr, u_scr, act_scr, mid_scr, w_buf, w_sem, h_sem, out_sem):
    rows, _ = h_scr.shape
    depth, _, tile, _ = w_buf.shape
    steps = w_ref.shape[1] // tile

    def w_copy(step):
        return pltpu.make_async_copy(w_ref.at[:, pl.ds(pl.multiple_of(step * tile, tile), tile), :], w_buf.at[lax.rem(step, depth)], w_sem.at[lax.rem(step, depth)])

    def out_copy(step):
        return pltpu.make_async_copy(mid_scr.at[lax.rem(step, 2)], mid_ref.at[:, pl.ds(pl.multiple_of(step * tile, tile), tile)], out_sem.at[lax.rem(step, 2)])

    h_copy = pltpu.make_async_copy(h_ref.at[slot, pl.ds(start, rows), :], h_scr, h_sem)
    h_copy.start()
    for step in range(min(depth - 1, steps)):
        w_copy(step).start()
    h_copy.wait()
    normalise(h_scr, gain_ref[...].astype(jnp.float32), u_scr, rows)

    part_rows = min(GATE_TILE, rows)
    parts = rows // part_rows

    def span(part):
        return pl.ds(pl.multiple_of(part * part_rows, part_rows), part_rows)

    def finish(step, part):
        gate = act_scr[0, span(part), :].astype(jnp.float32)
        up = act_scr[1, span(part), :].astype(jnp.float32)
        mid_scr[lax.rem(step, 2), span(part), :] = (jax.nn.silu(gate) * up).astype(jnp.bfloat16)

    def body(step, carry):
        @pl.when(step + depth - 1 < steps)
        def _():
            w_copy(step + depth - 1).start()

        @pl.when(step >= 3)
        def _():
            out_copy(step - 3).wait()

        w_copy(step).wait()
        index = lax.rem(step, depth)

        def rows_body(part, carry):
            normed = u_scr[span(part), :]
            gate = lax.dot_general(normed, w_buf[index, 0], NT_DIMS, preferred_element_type=jnp.float32)
            up = lax.dot_general(normed, w_buf[index, 1], NT_DIMS, preferred_element_type=jnp.float32)
            finish(step + 1, part)
            act_scr[0, span(part), :] = gate.astype(jnp.bfloat16)
            act_scr[1, span(part), :] = up.astype(jnp.bfloat16)
            return carry

        lax.fori_loop(0, parts, rows_body, 0)

        @pl.when(step >= 1)
        def _():
            out_copy(step - 1).start()

        return carry

    lax.fori_loop(0, steps, body, 0)
    if steps >= 3:
        out_copy(steps - 3).wait()

    def last_rows(part, carry):
        finish(steps - 1, part)
        return carry

    lax.fori_loop(0, parts, last_rows, 0)
    out_copy(steps - 1).start()
    if steps >= 2:
        out_copy(steps - 2).wait()
    out_copy(steps - 1).wait()


def gate_up(hidden, gain, weights, slot, start, rows):
    dim = hidden.shape[2]
    ff = weights.shape[1]
    tile = min(FF_TILE, ff)
    depth = 3
    anywhere = pl.BlockSpec(memory_space=pl.ANY)
    return pl.pallas_call(
        functools.partial(gate_up_kernel, slot, start),
        out_shape=jax.ShapeDtypeStruct((rows, ff), jnp.bfloat16),
        in_specs=[anywhere, pl.BlockSpec(memory_space=pltpu.VMEM), anywhere],
        out_specs=anywhere,
        scratch_shapes=[
            pltpu.VMEM((rows, dim), jnp.bfloat16),
            pltpu.VMEM((rows, dim), jnp.bfloat16),
            pltpu.VMEM((2, rows, tile), jnp.bfloat16),
            pltpu.VMEM((2, rows, tile), jnp.bfloat16),
            pltpu.VMEM((depth, 2, tile, dim), jnp.bfloat16),
            pltpu.SemaphoreType.DMA((depth,)),
            pltpu.SemaphoreType.DMA,
            pltpu.SemaphoreType.DMA((2,)),
        ],
        compiler_params=pltpu.CompilerParams(vmem_limit_bytes=58 * 1024 * 1024),
        cost_estimate=pl.CostEstimate(flops=4 * rows * dim * ff, bytes_accessed=4 * dim * ff + 2 * rows * (dim + ff), transcendentals=rows * ff),
        name='gate_up',
    )(hidden, gain[None, :], weights)


def down_kernel(slot, start, first, row_ref, h_ref, mid_ref, w_ref, y_in, y_ref, part_ref, h_scr, mid_scr, acc_scr, w_buf, w_sem, mid_sem, h_sem, out_sem):
    rows, dim = h_scr.shape
    depth, tile, _ = w_buf.shape
    steps = w_ref.shape[0] // tile
    out_tile = min(OUT_TILE, dim)

    def w_copy(step):
        return pltpu.make_async_copy(w_ref.at[pl.ds(pl.multiple_of(step * tile, tile), tile), :], w_buf.at[lax.rem(step, depth)], w_sem.at[lax.rem(step, depth)])

    def mid_copy(step):
        return pltpu.make_async_copy(mid_ref.at[pl.ds(first, rows), pl.ds(pl.multiple_of(step * tile, tile), tile)], mid_scr.at[lax.rem(step, depth)], mid_sem.at[lax.rem(step, depth)])

    h_copy = pltpu.make_async_copy(h_ref.at[slot, pl.ds(start, rows), :], h_scr, h_sem)
    h_copy.start()
    for step in range(min(depth - 1, steps)):
        w_copy(step).start()
        mid_copy(step).start()
    h_copy.wait()

    def widen(index, carry):
        part = pl.ds(pl.multiple_of(index * 64, 64), 64)
        acc_scr[part, :] = h_scr[part, :].astype(jnp.float32)
        return carry

    lax.fori_loop(0, rows // 64, widen, 0)

    def body(step, carry):
        @pl.when(step + depth - 1 < steps)
        def _():
            w_copy(step + depth - 1).start()
            mid_copy(step + depth - 1).start()

        w_copy(step).wait()
        mid_copy(step).wait()
        index = lax.rem(step, depth)
        mid = mid_scr[index]
        for col in range(0, dim, out_tile):
            cols = slice(col, col + out_tile)
            acc_scr[:, cols] += jnp.dot(mid, w_buf[index, :, cols], preferred_element_type=jnp.float32)
        return carry

    lax.fori_loop(0, steps, body, 0)

    def narrow(index, carry):
        part = pl.ds(pl.multiple_of(index * 64, 64), 64)
        h_scr[part, :] = acc_scr[part, :].astype(jnp.bfloat16)
        return carry

    lax.fori_loop(0, rows // 64, narrow, 0)
    part_out = pltpu.make_async_copy(h_scr, part_ref, out_sem.at[0])
    y_out = pltpu.make_async_copy(h_scr, y_ref.at[slot, row_ref[0], pl.ds(start, rows), :], out_sem.at[1])
    part_out.start()
    y_out.start()
    part_out.wait()
    y_out.wait()


def down_proj(row, hidden, mid, weights, y_all, slot, start, first, rows):
    dim = hidden.shape[2]
    ff = mid.shape[1]
    tile = min(FF_TILE, ff)
    depth = 4
    anywhere = pl.BlockSpec(memory_space=pl.ANY)
    return pl.pallas_call(
        functools.partial(down_kernel, slot, start, first),
        out_shape=(jax.ShapeDtypeStruct(y_all.shape, jnp.bfloat16), jax.ShapeDtypeStruct((rows, dim), jnp.bfloat16)),
        in_specs=[pl.BlockSpec(memory_space=pltpu.SMEM), anywhere, anywhere, anywhere, anywhere],
        out_specs=(anywhere, anywhere),
        scratch_shapes=[
            pltpu.VMEM((rows, dim), jnp.bfloat16),
            pltpu.VMEM((depth, rows, tile), jnp.bfloat16),
            pltpu.VMEM((rows, dim), jnp.float32),
            pltpu.VMEM((depth, tile, dim), jnp.bfloat16),
            pltpu.SemaphoreType.DMA((depth,)),
            pltpu.SemaphoreType.DMA((depth,)),
            pltpu.SemaphoreType.DMA,
            pltpu.SemaphoreType.DMA((2,)),
        ],
        input_output_aliases={4: 0},
        compiler_params=pltpu.CompilerParams(vmem_limit_bytes=58 * 1024 * 1024),
        cost_estimate=pl.CostEstimate(flops=2 * rows * dim * ff, bytes_accessed=2 * dim * ff + 2 * rows * (4 * dim + ff), transcendentals=0),
        name='down_proj',
    )(row, hidden, mid, weights, y_all)


def place_kernel(spots, n_rows, row_ref, y_in, *refs):
    pieces, (y_ref, buf, in_sem, out_sem) = refs[:len(spots)], refs[len(spots):]
    block = buf.shape[1]
    loads, stores = [], []
    for piece, (slot, offset, start, rows) in zip(pieces, spots):
        owner = lax.rem(row_ref[0] + offset, n_rows)
        for first in range(0, rows, block):
            at = len(loads)
            loads.append(pltpu.make_async_copy(piece.at[pl.ds(first, block), :], buf.at[at], in_sem.at[at]))
            stores.append(pltpu.make_async_copy(buf.at[at], y_ref.at[slot, owner, pl.ds(start + first, block), :], out_sem.at[at]))
    for load in loads:
        load.start()
    for load, store in zip(loads, stores):
        load.wait()
        store.start()
    for store in stores:
        store.wait()


def place(row, y_all, pieces):
    arrays = [piece for piece, _ in pieces]
    spots = [spot for _, spot in pieces]
    block = min(256, *(spot[3] for spot in spots))
    count = sum(spot[3] for spot in spots) // block
    dim = y_all.shape[3]
    anywhere = pl.BlockSpec(memory_space=pl.ANY)
    moved = 2 * dim * sum(spot[3] for spot in spots)
    return pl.pallas_call(
        functools.partial(place_kernel, spots, y_all.shape[1]),
        out_shape=jax.ShapeDtypeStruct(y_all.shape, y_all.dtype),
        in_specs=[pl.BlockSpec(memory_space=pltpu.SMEM)] + [anywhere] * (1 + len(arrays)),
        out_specs=anywhere,
        scratch_shapes=[pltpu.VMEM((count, block, dim), jnp.bfloat16), pltpu.SemaphoreType.DMA((count,)), pltpu.SemaphoreType.DMA((count,))],
        input_output_aliases={1: 0},
        compiler_params=pltpu.CompilerParams(vmem_limit_bytes=40 * 1024 * 1024),
        cost_estimate=pl.CostEstimate(flops=moved * 100, bytes_accessed=2 * moved, transcendentals=0),
        name='place_rows',
    )(row, y_all, *arrays)


def relayout_kernel(row_ref, gu_ref, d_ref, gate_ref, up_ref, down_ref):
    gate_ref[...] = jnp.transpose(gu_ref[0].astype(jnp.float32)).astype(jnp.bfloat16)
    up_ref[...] = jnp.transpose(gu_ref[1].astype(jnp.float32)).astype(jnp.bfloat16)
    down_ref[...] = d_ref[...]


def relayout(row, gu_full, down_full, n_rows):
    _, ff, dim = gu_full.shape
    own = ff // n_rows
    tile = min(128, own)
    steps = own // tile
    column = pl.BlockSpec((dim, tile), lambda j, _: (0, j))
    return pl.pallas_call(
        relayout_kernel,
        out_shape=(jax.ShapeDtypeStruct((dim, own), jnp.bfloat16), jax.ShapeDtypeStruct((dim, own), jnp.bfloat16), jax.ShapeDtypeStruct((own, dim), jnp.bfloat16)),
        grid_spec=pltpu.PrefetchScalarGridSpec(
            num_scalar_prefetch=1,
            grid=(steps,),
            in_specs=[
                pl.BlockSpec((2, tile, dim), lambda j, at: (0, at[0] * steps + j, 0)),
                pl.BlockSpec((tile, dim), lambda j, at: (at[0] * steps + j, 0)),
            ],
            out_specs=(column, column, pl.BlockSpec((tile, dim), lambda j, _: (j, 0))),
        ),
        compiler_params=pltpu.CompilerParams(dimension_semantics=('arbitrary',), vmem_limit_bytes=40 * 1024 * 1024),
        cost_estimate=pl.CostEstimate(flops=600 * own * dim, bytes_accessed=12 * own * dim, transcendentals=0),
        name='relayout',
    )(row, gu_full, down_full)


def gather_attn_kernel(ring, kv_rows, x_ref, gain_ref, wq_ref, wo_ref, q_ref, o_ref, kv_ref, q_scr, o_scr, x_scr, u_scr, kv_scr, send_sem, recv_sem, local_sem, x_sem, out_sem, q_sem):
    n_row, n_col = ring
    row = lax.axis_index('tpa')
    col = lax.axis_index('tpb')
    core = lax.rem(col, 2)
    chip = col // 2
    n_chip = n_col // 2
    far = n_row // 2
    mate = col + 1 - 2 * core

    def at_row(offset):
        return lax.rem(row + offset + n_row, n_row)

    def at_col(offset):
        return 2 * lax.rem(chip + offset + n_chip, n_chip) + core

    def peer(axis, step):
        return {'tpa': at_row(step)} if axis == 'y' else {'tpb': at_col(step)}

    barrier = pltpu.get_barrier_semaphore()
    for axis in 'xy':
        for step in (1, -1):
            pl.semaphore_signal(barrier, inc=1, device_id=peer(axis, step), device_id_type=MESH)
    pl.semaphore_signal(barrier, inc=1, device_id={'tpb': mate}, device_id_type=MESH)

    offsets = (0, -1, 1, far)
    tensors = (('q', q_scr, wq_ref, 'xy'), ('o', o_scr, wo_ref, 'yx'))
    started = []
    index_of = {}

    def sem_at(key):
        return index_of.setdefault(key, len(index_of))

    def slot(order, first, second):
        dx, dy = (first, second) if order == 'xy' else (second, first)
        return at_row(dy), at_col(dx)

    def halves(scr):
        rows = scr.shape[2]
        split = (rows // 32) * 16
        return {1: slice(0, split), -1: slice(split, rows), 0: slice(0, rows)}

    def descriptor(scr, where, part, target, key):
        ref = scr.at[where[0], where[1], halves(scr)[part], :]
        return pltpu.make_async_remote_copy(src_ref=ref, dst_ref=ref, send_sem=send_sem.at[sem_at(key)], recv_sem=recv_sem.at[sem_at(key)], device_id=target, device_id_type=MESH)

    def send(name, scr, order, first, second, part, axis, step):
        key = (name, first, second, part, axis, step)
        target = {'tpb': mate} if axis == 'm' else peer(axis, step)
        copy = descriptor(scr, slot(order, first, second), part, target, key)
        copy.start()
        started.append(copy)

    def receive(scr, order, first, second, part, key):
        where = slot(order, first, second)
        descriptor(scr, where, part, {'tpb': mate}, key).wait_recv()

    own_batch, _, seq_len, dim = x_ref.shape
    rows = x_scr.shape[1]
    per = seq_len // rows
    tiles = own_batch * n_row * per

    def fetch_x(tile):
        slot, where = tile // (n_row * per), lax.rem(tile // per, n_row)
        return pltpu.make_async_copy(x_ref.at[slot, where, pl.ds(pl.multiple_of(lax.rem(tile, per) * rows, rows), rows), :], x_scr.at[lax.rem(tile, 2)], x_sem.at[lax.rem(tile, 2)])

    def store_kv(tile):
        return pltpu.make_async_copy(kv_scr.at[lax.rem(tile, 2)], kv_ref.at[tile // per, :, pl.ds(pl.multiple_of(lax.rem(tile, per) * rows, rows), rows)], out_sem.at[lax.rem(tile, 2)])

    own = [pltpu.make_async_copy(ref, scr.at[row, col], local_sem.at[k]) for k, (_, scr, ref, _) in enumerate(tensors)]
    for copy in own:
        copy.start()
    for tile in range(min(2, tiles)):
        fetch_x(jnp.int32(tile)).start()
    for copy in own:
        copy.wait()
    pl.semaphore_wait(barrier, 5)

    def spread(name, scr, order, first):
        for step in (1, -1):
            send(name, scr, order, first, 0, 0, order[1], step)
        send(name, scr, order, first, 0, 0, 'm', 0)

    for name, scr, _, order in tensors:
        for step in (1, -1):
            send(name, scr, order, 0, 0, 0, order[0], step)
    for name, scr, _, order in tensors:
        spread(name, scr, order, 0)
    gain = gain_ref[...].astype(jnp.float32)
    for step in (1, -1):
        for name, scr, _, order in tensors:
            receive(scr, order, -step, 0, 0, (name, 0, 0, 0, order[0], step))
            send(name, scr, order, -step, 0, step, order[0], step)
            spread(name, scr, order, -step)
    for name, scr, _, order in tensors:
        for step in (1, -1):
            receive(scr, order, far, 0, step, (name, -step, 0, step, order[0], step))
        spread(name, scr, order, far)

    def mate_wait(name, scr, order, first, second):
        dx, dy = (first, second) if order == 'xy' else (second, first)
        ref = scr.at[at_row(dy), 2 * lax.rem(chip + dx + n_chip, n_chip) + 1 - core]
        key = sem_at((name, first, second, 0, 'm', 0))
        pltpu.make_async_remote_copy(src_ref=ref, dst_ref=ref, send_sem=send_sem.at[key], recv_sem=recv_sem.at[key], device_id={'tpb': mate}, device_id_type=MESH).wait_recv()

    cols = q_scr.shape[1] * q_scr.shape[2]

    def kv_tiles(first, last):
        def body(tile, carry):
            fetch_x(tile).wait()
            normalise(x_scr.at[lax.rem(tile, 2)], gain, u_scr, rows)

            @pl.when(tile + 2 < tiles)
            def _():
                fetch_x(tile + 2).start()

            @pl.when(tile >= 2)
            def _():
                store_kv(tile - 2).wait()

            weight = q_scr[row].reshape(cols, dim)[cols - kv_rows:]
            kv_scr[lax.rem(tile, 2)] = lax.dot_general(weight, u_scr[...], NT_DIMS, preferred_element_type=jnp.float32).astype(jnp.bfloat16)
            store_kv(tile).start()
            return carry

        lax.fori_loop(first, last, body, 0)

    def store_q(offset, at):
        return pltpu.make_async_copy(q_scr.at[at_row(offset)], q_ref.at[at_row(offset)], q_sem.at[at])

    def second_hop(name, scr, order, first):
        for step in (1, -1):
            receive(scr, order, first, -step, 0, (name, first, 0, 0, order[1], step))
            send(name, scr, order, first, -step, step, order[1], step)
            send(name, scr, order, first, -step, 0, 'm', 0)

    for first in offsets[:2]:
        for name, scr, _, order in tensors:
            second_hop(name, scr, order, first)
    for first in offsets:
        mate_wait('q', q_scr, 'xy', first, 0)
    store_q(0, 0).start()
    kv_tiles(0, tiles // 4)
    for first in offsets[2:]:
        for name, scr, _, order in tensors:
            second_hop(name, scr, order, first)
    kv_tiles(tiles // 4, 13 * tiles // 16)

    def last_hop(name, scr, order):
        for first in offsets:
            for step in (1, -1):
                receive(scr, order, first, far, step, (name, first, -step, step, order[1], step))
            send(name, scr, order, first, far, 0, 'm', 0)

    for second in offsets[1:3]:
        for first in offsets:
            mate_wait('q', q_scr, 'xy', first, second)
        store_q(second, offsets.index(second)).start()
    last_hop('q', q_scr, 'xy')
    last_hop('o', o_scr, 'yx')
    kv_tiles(13 * tiles // 16, tiles)
    for first in offsets:
        mate_wait('q', q_scr, 'xy', first, far)
    store_q(far, 3).start()
    for second in offsets:
        for first in offsets:
            mate_wait('o', o_scr, 'yx', first, second)
    o_out = pltpu.make_async_copy(o_scr, o_ref, local_sem.at[0])
    o_out.start()
    for copy in started:
        copy.wait_send()
    for tile in range(max(0, tiles - 2), tiles):
        store_kv(jnp.int32(tile)).wait()
    for at, offset in enumerate(offsets):
        store_q(offset, at).wait()
    o_out.wait()


def gather_attn(x_rows, gain, w_qkv_t, w_o, n_row, n_col, kv_rows):
    own_batch, _, seq_len, dim = x_rows.shape
    q_rows, o_rows = w_qkv_t.shape[0], w_o.shape[0]
    rows = min(512, seq_len)
    tokens = own_batch * n_row * seq_len
    moves = 2 * (4 + 9 * n_row)
    anywhere = pl.BlockSpec(memory_space=pl.ANY)
    return pl.pallas_call(
        functools.partial(gather_attn_kernel, (n_row, n_col), kv_rows),
        out_shape=(
            jax.ShapeDtypeStruct((n_row, n_col, q_rows, dim), jnp.bfloat16),
            jax.ShapeDtypeStruct((n_row, n_col, o_rows, dim), jnp.bfloat16),
            jax.ShapeDtypeStruct((own_batch * n_row, kv_rows, seq_len), jnp.bfloat16),
        ),
        in_specs=[anywhere, pl.BlockSpec(memory_space=pltpu.VMEM), anywhere, anywhere],
        out_specs=(anywhere, anywhere, anywhere),
        scratch_shapes=[
            pltpu.VMEM((n_row, n_col, q_rows, dim), jnp.bfloat16),
            pltpu.VMEM((n_row, n_col, o_rows, dim), jnp.bfloat16),
            pltpu.VMEM((2, rows, dim), jnp.bfloat16),
            pltpu.VMEM((rows, dim), jnp.bfloat16),
            pltpu.VMEM((2, kv_rows, rows), jnp.bfloat16),
            pltpu.SemaphoreType.DMA((moves,)),
            pltpu.SemaphoreType.DMA((moves,)),
            pltpu.SemaphoreType.DMA((2,)),
            pltpu.SemaphoreType.DMA((2,)),
            pltpu.SemaphoreType.DMA((2,)),
            pltpu.SemaphoreType.DMA((4,)),
        ],
        compiler_params=pltpu.CompilerParams(collective_id=0, has_side_effects=True, vmem_limit_bytes=58 * 1024 * 1024),
        cost_estimate=pl.CostEstimate(flops=2 * tokens * dim * kv_rows, bytes_accessed=2 * dim * n_row * n_col * (q_rows + o_rows), transcendentals=0),
        name='gather_attn',
    )(x_rows, gain[None, :], w_qkv_t, w_o)


def qkv_kernel(row_ref, x_ref, gain_ref, w_ref, out_ref, u_scr):
    piece, tile = pl.program_id(0), pl.program_id(1)

    @pl.when(piece == 0)
    def _():
        normalise(x_ref.at[0, 0], gain_ref[...].astype(jnp.float32), u_scr.at[tile], x_ref.shape[2])

    out_ref[0] = lax.dot_general(u_scr[tile], w_ref[...], NT_DIMS, preferred_element_type=jnp.float32).astype(jnp.bfloat16)


def qkv_proj(row, x_rows, gain, qkv_t, pieces):
    own_batch, _, seq_len, dim = x_rows.shape
    cols = qkv_t.shape[0] // pieces
    rows = min(512, seq_len)
    per = seq_len // rows
    tiles = own_batch * per

    def x_index(piece, tile, own):
        at = jnp.where(piece == 0, tile, tiles - 1)
        return (at // per, own[0], at % per, 0)

    return pl.pallas_call(
        qkv_kernel,
        out_shape=jax.ShapeDtypeStruct((own_batch, seq_len, pieces * cols), jnp.bfloat16),
        grid_spec=pltpu.PrefetchScalarGridSpec(
            num_scalar_prefetch=1,
            grid=(pieces, tiles),
            in_specs=[
                pl.BlockSpec((1, 1, rows, dim), x_index),
                pl.BlockSpec((1, dim), lambda p, t, _: (0, 0)),
                pl.BlockSpec((cols, dim), lambda p, t, _: (p, 0)),
            ],
            out_specs=pl.BlockSpec((1, rows, cols), lambda p, t, _: (t // per, t % per, p)),
            scratch_shapes=[pltpu.VMEM((tiles, rows, dim), jnp.bfloat16)],
        ),
        compiler_params=pltpu.CompilerParams(dimension_semantics=('arbitrary', 'arbitrary'), vmem_limit_bytes=60 * 1024 * 1024),
        cost_estimate=pl.CostEstimate(flops=2 * own_batch * seq_len * dim * pieces * cols, bytes_accessed=2 * dim * (pieces * cols + 2 * own_batch * seq_len), transcendentals=0),
        name='qkv_proj',
    )(row, x_rows, gain[None, :], qkv_t)


def out_kernel(row_ref, a_ref, x_ref, w_ref, h_ref, w_scr, sem):
    @pl.when(pl.program_id(0) == 0)
    def _():
        copy = pltpu.make_async_copy(w_ref, w_scr, sem)
        copy.start()
        copy.wait()

    dim = h_ref.shape[2]
    out_tile = min(OUT_TILE, dim)
    for col in range(0, dim, out_tile):
        cols = slice(col, col + out_tile)
        acc = jnp.dot(a_ref[0], w_scr[:, cols], preferred_element_type=jnp.float32)
        h_ref[0, :, cols] = (x_ref[0, 0, :, cols].astype(jnp.float32) + acc).astype(jnp.bfloat16)


def out_proj(row, attn, x_rows, w_o):
    own_batch, seq_len, depth = attn.shape
    dim = x_rows.shape[3]
    rows = min(256, seq_len)
    per = seq_len // rows
    return pl.pallas_call(
        out_kernel,
        out_shape=jax.ShapeDtypeStruct((own_batch, seq_len, dim), jnp.bfloat16),
        grid_spec=pltpu.PrefetchScalarGridSpec(
            num_scalar_prefetch=1,
            grid=(own_batch * per,),
            in_specs=[
                pl.BlockSpec((1, rows, depth), lambda t, _: (t // per, t % per, 0)),
                pl.BlockSpec((1, 1, rows, dim), lambda t, own: (t // per, own[0], t % per, 0)),
                pl.BlockSpec(memory_space=pl.ANY),
            ],
            out_specs=pl.BlockSpec((1, rows, dim), lambda t, _: (t // per, t % per, 0)),
            scratch_shapes=[pltpu.VMEM((depth, dim), jnp.bfloat16), pltpu.SemaphoreType.DMA],
        ),
        compiler_params=pltpu.CompilerParams(dimension_semantics=('arbitrary',), vmem_limit_bytes=56 * 1024 * 1024),
        cost_estimate=pl.CostEstimate(flops=2 * own_batch * seq_len * dim * depth, bytes_accessed=2 * dim * (depth + 3 * own_batch * seq_len), transcendentals=0),
        name='out_proj',
    )(row, attn, x_rows, w_o)


def solution(mesh):
    n_tpa = mesh.shape['tpa']
    n_tpb = mesh.shape['tpb']
    up_ring = [(i, (i + 1) % n_tpa) for i in range(n_tpa)]
    down_ring = [(i, (i - 1) % n_tpa) for i in range(n_tpa)]
    both = ('tpa', 'tpb')

    def layer_step(x_loc, len_loc, k_buf, v_buf, w_qkv, w_o, w_gate_up, w_down, g_attn, g_mlp):
        row = lax.axis_index('tpa')
        batch_loc, seq_len, model_dim = x_loc.shape
        head_dim = k_buf.shape[3]
        own_batch = batch_loc // n_tpa
        ff_block = w_gate_up.shape[1] // 2
        qkv_row = w_qkv.shape[1] * n_tpb
        o_row = w_o.shape[0] * n_tpb

        row_arg = row.astype(jnp.int32)[None]
        cos_tab, sin_tab = rope_tables(seq_len, head_dim)
        x_rows = x_loc.reshape(own_batch, n_tpa, seq_len, model_dim)
        len_own = lax.dynamic_index_in_dim(len_loc.reshape(own_batch, n_tpa), row, 1, keepdims=False)

        kv_cols = k_buf.shape[2] * head_dim
        q_full, o_full, kv_new = gather_attn(x_rows, g_attn, w_qkv.T, w_o, n_tpa, n_tpb, 2 * kv_cols)
        q_full, o_full, kv_new, gu_block, down_block = lax.optimization_barrier((q_full, o_full, kv_new, w_gate_up.T, w_down))
        gu_full = lax.all_gather(gu_block.reshape(2, ff_block, model_dim), both, axis=1, tiled=True)
        down_full = lax.all_gather(down_block, both, axis=0, tiled=True)
        qkv_act = qkv_proj(row_arg, x_rows, g_attn, q_full.reshape(-1, model_dim), 2)
        attn_out = attention(qkv_act, len_own, cos_tab, sin_tab, n_tpa * k_buf.shape[2], head_dim)
        hidden = out_proj(row_arg, attn_out, x_rows, o_full.reshape(-1, model_dim))

        y_all = empty((own_batch, n_tpa, seq_len, model_dim), jnp.bfloat16)

        half = seq_len // 2
        gates = [(0, 0, seq_len, (half // 2, half // 2, half)), (1, 0, half, (half,)), (1, half, half, (half // 2, half // 2))]
        chunks = []
        spots = []
        mids = []
        for index, (slot, start, gate_rows, parts) in enumerate(gates):
            mids.append(gate_up(hidden, g_mlp, gu_full, slot, start, gate_rows))
            for part, rows in enumerate(parts):
                offset = sum(parts[:part])
                chunks.append((index, offset, rows))
                spots.append((slot, start + offset, rows))
        fars = []
        near = []
        for index, (gate, offset, rows) in enumerate(chunks):
            slot, start, _ = spots[index]
            y_all, part = down_proj(row_arg, hidden, mids[gate], down_full, y_all, slot, start, offset, rows)
            near.append((lax.ppermute(part, 'tpa', up_ring), lax.ppermute(part, 'tpa', down_ring)))

        y_all, kv_late, o_late, q_late, gu_late, down_late = lax.optimization_barrier((y_all, kv_new, o_full, q_full, gu_full, down_full))
        q_cols = qkv_row - 2 * kv_cols
        qkv_own = lax.dynamic_index_in_dim(q_late, row, 0, keepdims=False).reshape(qkv_row, model_dim)
        o_rows = lax.dynamic_index_in_dim(o_late, row, 0, keepdims=False).reshape(o_row, model_dim)
        w_query = qkv_own[:q_cols].T
        w_key = qkv_own[q_cols:q_cols + kv_cols].T
        w_value = qkv_own[q_cols + kv_cols:].T
        kv_new = kv_late.transpose(0, 2, 1)
        half_dim = head_dim // 2
        k_first = kv_new[..., :half_dim].astype(jnp.float32)
        k_second = kv_new[..., half_dim:head_dim].astype(jnp.float32)
        k_rot = jnp.concatenate([k_first * cos_tab - k_second * sin_tab, k_second * cos_tab + k_first * sin_tab], axis=-1).astype(jnp.bfloat16)
        valid_pos = (jnp.arange(seq_len)[None, :] < len_loc[:, None])[:, :, None, None]
        k_cache = jnp.where(valid_pos, k_rot[:, :, None, :], k_buf)
        v_cache = jnp.where(valid_pos, kv_new[:, :, None, head_dim:], v_buf)
        w_gate, w_up, down_rows = relayout(row_arg, gu_late, down_late, n_tpa)
        cache_outs = (k_cache, v_cache, w_query, w_key, w_value, o_rows)
        near[-2], cache_outs = lax.optimization_barrier((near[-2], cache_outs))
        k_cache, v_cache, w_query, w_key, w_value, o_rows = cache_outs
        near[-1], (w_gate, w_up, down_rows) = lax.optimization_barrier((near[-1], (w_gate, w_up, down_rows)))
        for index, ((from_below, from_above), (slot, start, rows)) in enumerate(zip(near, spots)):
            if index % 2 == 0:
                far = lax.ppermute(from_below, 'tpa', up_ring)
            else:
                far = lax.ppermute(from_above, 'tpa', down_ring)
            fars.append(far)

        def near_pieces(first, last):
            for (from_below, from_above), (slot, start, rows) in list(zip(near, spots))[first:last]:
                yield from_below, (slot, n_tpa - 1, start, rows)
                yield from_above, (slot, 1, start, rows)

        def far_pieces(first, last):
            for far, (slot, start, rows) in list(zip(fars, spots))[first:last]:
                yield far, (slot, n_tpa - 2, start, rows)

        n_first = len(spots) // 2
        y_all = place(row_arg, y_all, [*near_pieces(0, n_first), *far_pieces(0, 2)])
        y_all = place(row_arg, y_all, [*near_pieces(n_first, len(spots)), *far_pieces(2, n_first)])
        for index in range(n_first, len(spots)):
            y_all = place(row_arg, y_all, [*far_pieces(index, index + 1)])
        layer_out = y_all.reshape(batch_loc, seq_len, model_dim)
        return (layer_out, k_cache, v_cache, w_query, w_key, w_value, o_rows, w_gate, w_up, down_rows)

    batch_spec = P(('part', 'tpb'), None, None)
    len_spec = P(('part', 'tpb'))
    cache_spec = P(('part', 'tpb'), None, 'tpa', None)
    train_cols = P('part', ('tpa', 'tpb'))
    train_rows = P(('part', 'tpa', 'tpb'), None)
    gain_spec = P('part')
    gen_cols = P('part', 'tpa')
    gen_rows = P(('part', 'tpa'), None)
    return jax.shard_map(layer_step, mesh=mesh, in_specs=(batch_spec, len_spec, cache_spec, cache_spec, train_cols, train_rows, train_cols, train_rows, gain_spec, gain_spec), out_specs=(batch_spec, cache_spec, cache_spec, gen_cols, gen_cols, gen_cols, gen_rows, gen_cols, gen_cols, gen_rows), check_vma=False)
```
